8 devices in a mesh: dp: 1 (over z), yz: 2 (over y), x: 4 (over x, core).
Axes of the slice: x: 2, y: 2, z: 1, core: 2. Of those that a mesh axis runs over, the one named last changes fastest.
Arguments:
- h_in: bfloat16 [256, 1024], P('dp', ('x', 'yz'))
- seq_lens: int32 [256], P('dp')
- k_cache: bfloat16 [2, 256, 16, 512, 64], P(None, 'dp', ('yz', 'x'))
- v_cache: bfloat16 [2, 256, 16, 512, 64], P(None, 'dp', ('yz', 'x'))
- g_attn: bfloat16 [2, 1024], P(None, ('x', 'yz'))
- w_q: bfloat16 [2, 1024, 1024], P(None, 'x', 'yz')
- w_k: bfloat16 [2, 1024, 1024], P(None, 'x', 'yz')
- w_v: bfloat16 [2, 1024, 1024], P(None, 'x', 'yz')
- w_o: bfloat16 [2, 1024, 1024], P(None, 'yz', 'x')
- g_mlp: bfloat16 [2, 1024], P(None, ('x', 'yz'))
- w_in: bfloat16 [2, 1024, 2816], P(None, 'x', 'yz')
- w_out: bfloat16 [2, 2816, 1024], P(None, 'yz', 'x')
- g_final: bfloat16 [1024], P(('x', 'yz'))
- w_unemb: bfloat16 [1024, 32128], P('x', 'yz')
Outputs:
- output 1: bfloat16 [256, 1024], P('dp', ('x', 'yz'))
- output 2: float32 [256, 32128], P('dp', ('yz', 'x'))
- output 3: bfloat16 [2, 256, 16, 64], P(None, 'dp', ('yz', 'x'))
- output 4: bfloat16 [2, 256, 16, 64], P(None, 'dp', ('yz', 'x'))
All inputs are finite; a program needn't handle non-finite values.
Results may differ from the reference program's by a relative error of at most 0.0186626.
Values are sent between devices in bfloat16 or wider.
A program may use at most 1 GiB of HBM per device.

```python
import jax
import jax.numpy as jnp
from jax import lax

MODEL_DIM = 1024
NUM_HEADS = 16
HEAD_DIM = 64
FFN_DIM = 2816
VOCAB_SIZE = 32128
BATCH_SEQS = 256
CACHE_LEN = 512
NUM_LAYERS = 2
ATTN_WIDTH = NUM_HEADS * HEAD_DIM
NORM_EPS = 1e-6


def setup_inputs(seed: int = 0, part: int = 0) -> dict:
    shared_keys = jax.random.split(jax.random.key(seed), 10)
    part_keys = jax.random.split(jax.random.fold_in(jax.random.key(seed + 1), part), 6)

    def weight(key_w, fan_in, fan_out):
        normal_draw = jax.random.normal(key_w, (NUM_LAYERS, fan_in, fan_out), jnp.float32)
        return (normal_draw * fan_in ** -0.5).astype(jnp.bfloat16)

    def gain(key_g, gain_shape):
        return jax.random.uniform(key_g, gain_shape, jnp.float32, 0.5, 1.5).astype(jnp.bfloat16)

    col_pos = (jnp.arange(MODEL_DIM, dtype=jnp.float32) + 0.5) / MODEL_DIM
    col_scale = 0.25 + 1.5 * col_pos
    row_scale = jax.random.uniform(part_keys[1], (BATCH_SEQS, 1), jnp.float32, 0.5, 2.0)
    h_draw = jax.random.normal(part_keys[0], (BATCH_SEQS, MODEL_DIM), jnp.float32)
    h_in = (h_draw * col_scale * row_scale).astype(jnp.bfloat16)
    seq_lens = jax.random.randint(part_keys[2], (BATCH_SEQS,), 1, CACHE_LEN, jnp.int32)
    seq_lens = seq_lens.at[0].set(CACHE_LEN - 1).at[1].set(1)
    cache_shape = (NUM_LAYERS, BATCH_SEQS, NUM_HEADS, CACHE_LEN, HEAD_DIM)
    k_cache = (1.5 * jax.random.normal(part_keys[3], cache_shape, jnp.float32)).astype(jnp.bfloat16)
    v_mean = jax.random.normal(part_keys[4], (NUM_LAYERS, BATCH_SEQS, NUM_HEADS, 1, HEAD_DIM), jnp.float32)
    v_cache = (jax.random.normal(part_keys[5], cache_shape, jnp.float32) + v_mean).astype(jnp.bfloat16)
    unemb_draw = jax.random.normal(shared_keys[9], (MODEL_DIM, VOCAB_SIZE), jnp.float32)
    return {
        'h_in': h_in,
        'seq_lens': seq_lens,
        'k_cache': k_cache,
        'v_cache': v_cache,
        'g_attn': gain(shared_keys[0], (NUM_LAYERS, MODEL_DIM)),
        'w_q': weight(shared_keys[1], MODEL_DIM, ATTN_WIDTH),
        'w_k': weight(shared_keys[2], MODEL_DIM, ATTN_WIDTH),
        'w_v': weight(shared_keys[3], MODEL_DIM, ATTN_WIDTH),
        'w_o': weight(shared_keys[4], ATTN_WIDTH, MODEL_DIM),
        'g_mlp': gain(shared_keys[5], (NUM_LAYERS, MODEL_DIM)),
        'w_in': weight(shared_keys[6], MODEL_DIM, FFN_DIM),
        'w_out': weight(shared_keys[7], FFN_DIM, MODEL_DIM),
        'g_final': gain(shared_keys[8], (MODEL_DIM,)),
        'w_unemb': (unemb_draw * MODEL_DIM ** -0.5).astype(jnp.bfloat16),
    }


def rms_norm(h_act, gain_vec):
    h_f32 = h_act.astype(jnp.float32)
    inv_rms = lax.rsqrt(jnp.mean(h_f32 * h_f32, axis=-1, keepdims=True) + NORM_EPS)
    return (h_f32 * inv_rms * gain_vec.astype(jnp.float32)).astype(jnp.bfloat16)


def attend(q_heads, k_new, v_new, k_cache, v_cache, seq_lens):
    inv_sqrt = HEAD_DIM ** -0.5
    q_f32 = q_heads.astype(jnp.float32)
    s_cache = jnp.einsum('bhd,bhsd->bhs', q_f32, k_cache.astype(jnp.float32)) * inv_sqrt
    s_new = jnp.sum(q_f32 * k_new.astype(jnp.float32), axis=-1) * inv_sqrt
    valid_pos = jnp.arange(CACHE_LEN)[None, None, :] < seq_lens[:, None, None]
    s_cache = jnp.where(valid_pos, s_cache, -1e30)
    score_max = jnp.maximum(jnp.max(s_cache, axis=-1), s_new)
    p_cache = jnp.exp(s_cache - score_max[:, :, None])
    p_new = jnp.exp(s_new - score_max)
    prob_sum = jnp.sum(p_cache, axis=-1) + p_new
    p_cache = (p_cache / prob_sum[:, :, None]).astype(jnp.bfloat16)
    p_new = (p_new / prob_sum).astype(jnp.bfloat16)
    mixed_out = jnp.einsum('bhs,bhsd->bhd', p_cache.astype(jnp.float32), v_cache.astype(jnp.float32))
    mixed_out = mixed_out + p_new.astype(jnp.float32)[:, :, None] * v_new.astype(jnp.float32)
    return mixed_out.astype(jnp.bfloat16)


def decoder_layer(h_act, layer_args, seq_lens):
    k_cache, v_cache, g_attn, w_q, w_k, w_v, w_o, g_mlp, w_in, w_out = layer_args
    head_shape = (BATCH_SEQS, NUM_HEADS, HEAD_DIM)
    normed = rms_norm(h_act, g_attn)
    q_heads = jnp.dot(normed, w_q, preferred_element_type=jnp.float32).astype(jnp.bfloat16).reshape(head_shape)
    k_new = jnp.dot(normed, w_k, preferred_element_type=jnp.float32).astype(jnp.bfloat16).reshape(head_shape)
    v_new = jnp.dot(normed, w_v, preferred_element_type=jnp.float32).astype(jnp.bfloat16).reshape(head_shape)
    attn_heads = attend(q_heads, k_new, v_new, k_cache, v_cache, seq_lens).reshape(BATCH_SEQS, ATTN_WIDTH)
    attn_sum = jnp.dot(attn_heads, w_o, preferred_element_type=jnp.float32)
    h_act = (h_act.astype(jnp.float32) + attn_sum).astype(jnp.bfloat16)
    normed = rms_norm(h_act, g_mlp)
    hidden = jax.nn.gelu(jnp.dot(normed, w_in, preferred_element_type=jnp.float32)).astype(jnp.bfloat16)
    mlp_sum = jnp.dot(hidden, w_out, preferred_element_type=jnp.float32)
    h_act = (h_act.astype(jnp.float32) + mlp_sum).astype(jnp.bfloat16)
    return h_act, (k_new, v_new)


def reference(h_in, seq_lens, k_cache, v_cache, g_attn, w_q, w_k, w_v, w_o, g_mlp, w_in, w_out, g_final, w_unemb):
    def scan_body(h_act, layer_args):
        return decoder_layer(h_act, layer_args, seq_lens)

    layer_stack = (k_cache, v_cache, g_attn, w_q, w_k, w_v, w_o, g_mlp, w_in, w_out)
    h_out, new_entries = lax.scan(scan_body, h_in, layer_stack)
    logits = jnp.dot(rms_norm(h_out, g_final), w_unemb, preferred_element_type=jnp.float32)
    return (h_out, logits, new_entries[0], new_entries[1])
```

```python
import functools

import jax
import jax.numpy as jnp
from jax import lax
from jax.experimental import pallas as pl
from jax.experimental.pallas import tpu as pltpu
from jax.sharding import PartitionSpec as P

NORM_EPS = 1e-6
MESH = pl.DeviceIdType.MESH
BF = jnp.bfloat16
F32 = jnp.float32
ANY = pl.BlockSpec(memory_space=pl.ANY)
VM = pl.BlockSpec(memory_space=pltpu.VMEM)
SEQ_STEP = 16
SLOTS = 3
CHUNK = 128


def tdot(w, act):
    return lax.dot_general(w, act, (((0,), (0,)), ((), ())), preferred_element_type=F32)


def attn_kernel(layer, lens_ref, q_ref, k_ref, v_ref, kc_ref, vc_ref, o_ref, kbuf, vbuf, sems):
    batch, width = q_ref.shape
    dh = kc_ref.shape[3]
    cache_len = kc_ref.shape[4]
    steps = batch // SEQ_STEP

    def copies(step, slot, s):
        b = step * SEQ_STEP + s
        size = (lens_ref[b] + (CHUNK - 1)) // CHUNK * CHUNK
        size = pl.multiple_of(jnp.where(step < SLOTS, cache_len, size), CHUNK)
        span = pl.ds(0, size)
        return [
            pltpu.make_async_copy(c.at[layer, b, :, :, span], buf.at[slot, s, :, :, span], sems.at[slot, n, s])
            for n, (c, buf) in enumerate(((kc_ref, kbuf), (vc_ref, vbuf)))
        ]

    def issue(step, slot):
        for s in range(SEQ_STEP):
            for c in copies(step, slot, s):
                c.start()

    def fetched(step, slot):
        for s in range(SEQ_STEP):
            for c in copies(step, slot, s):
                c.wait()

    for n in range(SLOTS - 1):
        issue(n, n)

    row = lax.broadcasted_iota(jnp.int32, (16, width), 0) % 8
    lane = lax.broadcasted_iota(jnp.int32, (8, width), 1)
    pos = lax.broadcasted_iota(jnp.int32, (16, cache_len), 1)
    row8 = lax.broadcasted_iota(jnp.int32, (8, width), 0)
    first_head = lane < dh

    def body(step, carry):
        slot = lax.rem(step, SLOTS)
        nxt = step + SLOTS - 1

        @pl.when(nxt < steps)
        def _():
            issue(nxt, lax.rem(nxt, SLOTS))

        fetched(step, slot)
        groups = range(SEQ_STEP // 8)
        base = [pl.multiple_of(step * SEQ_STEP + 8 * g, 8) for g in groups]
        q2s, scores = [], []
        for g in groups:
            q8 = q_ref[pl.ds(base[g], 8), :]
            q2 = jnp.concatenate([jnp.where(first_head, q8, 0.0), jnp.where(first_head, 0.0, q8)], axis=0)
            qbd = jnp.concatenate([jnp.where(row == n, q2, 0.0) for n in range(8)], axis=1).astype(BF)
            kb = kbuf[slot, 8 * g:8 * g + 8].reshape(8 * width, cache_len)
            scores.append(jnp.dot(qbd, kb, preferred_element_type=F32))
            q2s.append(q2)
        probs, p_news = [], []
        for g in groups:
            k8 = k_ref[pl.ds(base[g], 8), :]
            k2 = jnp.concatenate([k8, k8], axis=0)
            s_new = jnp.sum(q2s[g] * k2, axis=1, keepdims=True) * (dh ** -0.5)
            lens8 = jnp.zeros((8, width), jnp.int32)
            for n in range(8):
                lens8 = jnp.where(row8 == n, lens_ref[base[g] + n], lens8)
            lens16 = jnp.concatenate([lens8, lens8], axis=0)
            lens_full = jnp.concatenate([lens16] * (cache_len // width), axis=1)
            s = jnp.where(pos < lens_full, scores[g] * (dh ** -0.5), -1e30)
            top = jnp.maximum(jnp.max(s, axis=1, keepdims=True), s_new)
            e = jnp.exp(s - top)
            e_new = jnp.exp(s_new - top)
            inv = 1.0 / (jnp.sum(e, axis=1, keepdims=True) + e_new)
            probs.append((e * inv).astype(BF))
            p_news.append((e_new * inv).astype(BF).astype(F32))
        for g in groups:
            vb = vbuf[slot, 8 * g:8 * g + 8].reshape(8 * width, cache_len)
            mixed = lax.dot_general(probs[g], vb, (((1,), (1,)), ((), ())), preferred_element_type=F32)
            o2 = jnp.zeros((16, width), F32)
            for n in range(8):
                o2 = jnp.where(row == n, mixed[:, n * width:(n + 1) * width], o2)
            v8 = v_ref[pl.ds(base[g], 8), :]
            o2 = o2 + p_news[g] * jnp.concatenate([v8, v8], axis=0)
            o_ref[pl.ds(base[g], 8), :] = jnp.where(first_head, o2[:8], o2[8:])
        return carry

    lax.fori_loop(0, steps, body, 0)


def attention(layer, seq_lens, q, k, v, kc, vc):
    batch, width = q.shape
    heads, dh, cache_len = kc.shape[2:]
    nbytes = kc.shape[1] * heads * dh * cache_len * 2 * 2
    return pl.pallas_call(
        functools.partial(attn_kernel, layer),
        name="attn",
        out_shape=jax.ShapeDtypeStruct((batch, width), F32),
        in_specs=[pl.BlockSpec(memory_space=pltpu.SMEM), VM, VM, VM, ANY, ANY],
        out_specs=VM,
        scratch_shapes=[
            pltpu.VMEM((SLOTS, SEQ_STEP, heads, dh, cache_len), BF),
            pltpu.VMEM((SLOTS, SEQ_STEP, heads, dh, cache_len), BF),
            pltpu.SemaphoreType.DMA((SLOTS, 2, SEQ_STEP)),
        ],
        compiler_params=pltpu.CompilerParams(vmem_limit_bytes=40 * 2**20),
        cost_estimate=pl.CostEstimate(flops=nbytes, bytes_accessed=nbytes, transcendentals=0),
    )(seq_lens, q, k, v, kc, vc)


class Net:
    def __init__(self, send, recv, local):
        self.i = lax.axis_index("x")
        self.j = lax.axis_index("yz")
        self.chip = self.i // 2
        self.core = lax.rem(self.i, 2)
        self.sib = {"x": 2 * self.chip + 1 - self.core}
        self.across = {"x": lax.rem(self.i + 2, 4)}
        self.yother = {"yz": 1 - self.j}
        self.send, self.recv, self.local = send, recv, local
        self.n = 0
        self.m = 0
        self.sent = []

    def greet(self):
        self.barrier = pltpu.get_barrier_semaphore()
        for dx in range(4):
            for dy in range(2):
                if dx or dy:
                    pl.semaphore_signal(self.barrier, inc=1, device_id=self.peer(dx, dy), device_id_type=MESH)

    def met(self):
        pl.semaphore_wait(self.barrier, 7)

    def peer(self, dx, dy):
        return {"x": lax.rem(self.i + dx, 4), "yz": lax.rem(self.j + dy, 2)}

    def put(self, src, dst, to):
        c = pltpu.make_async_remote_copy(
            src_ref=src, dst_ref=dst, send_sem=self.send.at[self.n], recv_sem=self.recv.at[self.n],
            device_id=to, device_id_type=MESH)
        self.n += 1
        c.start()
        self.sent.append(c)
        return c

    def fetch(self, src, dst):
        c = pltpu.make_async_copy(src, dst, self.local.at[self.m])
        self.m += 1
        c.start()
        return c

    def finish(self):
        for c in self.sent:
            c.wait_send()


def norm_send(net, h_own, hx, ssq):
    hf = h_own.astype(F32)
    me = 2 * net.i + net.j
    hx[net.j] = h_own
    ssq[me] = jnp.sum(hf * hf, axis=0, keepdims=True)
    waits = [net.put(hx.at[net.j], hx.at[net.j], net.yother)]
    for dx in range(4):
        for dy in range(2):
            if dx or dy:
                waits.append(net.put(ssq.at[me], ssq.at[me], net.peer(dx, dy)))
    return waits


def norm_finish(waits, hx, ssq, gain, model_dim):
    for c in waits:
        c.wait_recv()
    total = ssq[0]
    for n in range(1, 8):
        total = total + ssq[n]
    inv = lax.rsqrt(total / model_dim + NORM_EPS)
    rows = hx.shape[0] * hx.shape[1]
    hf = hx[...].reshape(rows, hx.shape[2]).astype(F32)
    return (hf * inv * gain).astype(BF)


def slot_of(d):
    return 2 * (d % 2) + d // 2


def rs_first(net, part, got):
    return net.put(part.at[pl.ds(2 * (1 - net.core), 2)], got, net.sib)


def rs_second(net, wait, part, got, out, back):
    wait.wait_recv()
    far = 1 - net.chip
    out[...] = (part[2 * net.core + far].astype(F32) + got[far].astype(F32)).astype(BF)
    return net.put(out, back, net.across)


def rs_last(net, wait, part, got, back):
    mine = part[2 * net.core + net.chip].astype(F32) + got[net.chip].astype(F32)
    wait.wait_recv()
    return mine + back[...].astype(F32)


def qkv_stage(net, xn, ws, bufs, outs, layer_out):
    part, got, out, back = bufs
    first = []
    for n in range(3):
        y = tdot(ws[n][...], xn).astype(BF)
        r = y.shape[0] // 4
        for d in range(4):
            part[n, slot_of(d)] = y[d * r:(d + 1) * r]
        first.append(rs_first(net, part.at[n], got.at[n]))
    second = [rs_second(net, first[n], part.at[n], got.at[n], out.at[n], back.at[n]) for n in range(3)]
    q_out, k_out, v_out, kt_out, vt_out = outs
    for n in range(3):
        y = rs_last(net, second[n], part.at[n], got.at[n], back.at[n]).astype(BF)
        if n:
            (kt_out, vt_out)[n - 1][...] = y
        (q_out, k_out, v_out)[n][...] = y.astype(F32).T


def kernel_a(model_dim, layer, h_ref, g_ref, wq, wk, wv, q_out, k_out, v_out, kt_out, vt_out, ht_out, gx_out,
             hx, ssq, gx, w_buf, part, got, out, back, send, recv, local):
    net = Net(send, recv, local)
    net.greet()
    loads = [net.fetch(w.at[layer], w_buf.at[n]) for n, w in enumerate((wq, wk, wv))]
    h_own = h_ref[...].astype(F32).T.astype(BF)
    ht_out[...] = h_own
    gx[net.j] = g_ref[...]
    net.met()
    waits = norm_send(net, h_own, hx, ssq)
    waits.append(net.put(gx.at[net.j], gx.at[net.j], net.yother))
    for c in loads:
        c.wait()
    waits[-1].wait_recv()
    gains = gx[...].reshape(2 * gx.shape[1], gx.shape[2])
    gx_out[...] = gains
    xn = norm_finish(waits[:-1], hx, ssq, gains[:, layer:layer + 1], model_dim)
    qkv_stage(net, xn, [w_buf.at[n] for n in range(3)], (part, got, out, back),
              (q_out, k_out, v_out, kt_out, vt_out), layer)
    net.finish()


def gather_x(net, buf):
    me = buf.at[net.i]
    across = net.put(me, me, net.across)
    sib = net.put(me, me, net.sib)
    return sib, across


def gather_forward(net, buf, across):
    across.wait_recv()
    far = buf.at[lax.rem(net.i + 2, 4)]
    return net.put(far, far, net.sib)


def sum_yz(net, y, part, got):
    r = y.shape[0] // 2
    part[0] = y[:r].astype(BF)
    part[1] = y[r:].astype(BF)
    c = net.put(part.at[1 - net.j], got, net.yother)
    c.wait_recv()
    return part[net.j].astype(F32) + got[...].astype(F32)


def post_attention(net, model_dim, o_ref, h_own, gain, wo, win, wout, s, wait_w):
    s["o"][net.i] = o_ref[...].T.astype(BF)
    net.met()
    sib, across = gather_x(net, s["o"])
    wait_w("wo")
    fwd = gather_forward(net, s["o"], across)
    sib.wait_recv()
    fwd.wait_recv()
    o_all = s["o"][...].reshape(-1, s["o"].shape[2])
    h1 = (h_own.astype(F32) + sum_yz(net, tdot(wo[...], o_all), s["ypart1"], s["ygot1"])).astype(BF)
    waits = norm_send(net, h1, s["hx1"], s["ssq1"])
    wait_w("win")
    xn = norm_finish(waits, s["hx1"], s["ssq1"], gain, model_dim)
    r = win.shape[1] // 4
    y = tdot(win[...], xn).astype(BF)
    for d in range(4):
        s["upart"][slot_of(d)] = y[d * r:(d + 1) * r]
    first = rs_first(net, s["upart"], s["ugot"])
    second = rs_second(net, first, s["upart"], s["ugot"], s["uout"], s["uback"])
    up = rs_last(net, second, s["upart"], s["ugot"], s["uback"]).astype(BF)
    s["u"][net.i] = jax.nn.gelu(up.astype(F32)).astype(BF)
    sib, across = gather_x(net, s["u"])
    wait_w("wout")
    fwd = gather_forward(net, s["u"], across)
    sib.wait_recv()
    fwd.wait_recv()
    u_all = s["u"][...].reshape(-1, s["u"].shape[2])
    return (h1.astype(F32) + sum_yz(net, tdot(wout[...], u_all), s["ypart2"], s["ygot2"])).astype(BF)


POST = ("o", "ypart1", "ygot1", "hx1", "ssq1", "upart", "ugot", "uout", "uback", "u", "ypart2", "ygot2", "hx2", "ssq2",
        "wo", "win", "wout")


def post_shapes(blk, batch, f_loc, k_o):
    r = f_loc // 4
    return [
        pltpu.VMEM((4, blk, batch), BF),
        pltpu.VMEM((2, blk, batch), BF), pltpu.VMEM((blk, batch), BF),
        pltpu.VMEM((2, blk, batch), BF), pltpu.VMEM((8, 1, batch), F32),
        pltpu.VMEM((4, r, batch), BF), pltpu.VMEM((2, r, batch), BF), pltpu.VMEM((r, batch), BF), pltpu.VMEM((r, batch), BF),
        pltpu.VMEM((4, r, batch), BF),
        pltpu.VMEM((2, blk, batch), BF), pltpu.VMEM((blk, batch), BF),
        pltpu.VMEM((2, blk, batch), BF), pltpu.VMEM((8, 1, batch), F32),
        pltpu.VMEM((k_o, 2 * blk), BF), pltpu.VMEM((2 * blk, f_loc), BF), pltpu.VMEM((f_loc, 2 * blk), BF),
    ]


def kernel_b(model_dim, layers, layer, o_ref, ht_ref, gx_ref, wo, win, wout, wq, wk, wv,
             q_out, k_out, v_out, kt_out, vt_out, ht_out, *rest):
    s = dict(zip(POST, rest))
    w_buf, part, got, out, back, send, recv, local = rest[len(POST):]
    net = Net(send, recv, local)
    net.greet()
    loads = {n: net.fetch(w.at[layer], s[n]) for n, w in (("wo", wo), ("win", win), ("wout", wout))}
    qkv_loads = [net.fetch(w.at[layer + 1], w_buf.at[n]) for n, w in enumerate((wq, wk, wv))]
    gains = gx_ref[...]
    h2 = post_attention(net, model_dim, o_ref, ht_ref[...], gains[:, layers + layer:layers + layer + 1],
                        s["wo"], s["win"], s["wout"], s, lambda n: loads[n].wait())
    ht_out[...] = h2
    waits = norm_send(net, h2, s["hx2"], s["ssq2"])
    for c in qkv_loads:
        c.wait()
    xn = norm_finish(waits, s["hx2"], s["ssq2"], gains[:, layer + 1:layer + 2], model_dim)
    qkv_stage(net, xn, [w_buf.at[n] for n in range(3)], (part, got, out, back),
              (q_out, k_out, v_out, kt_out, vt_out), layer + 1)
    net.finish()


def kernel_c(model_dim, layers, layer, o_ref, ht_ref, gx_ref, wo, win, wout, wu, h_out, logit_out, *rest):
    s = dict(zip(POST, rest))
    w_buf, send_a, got_a, send_b, got_b, stage, send, recv, local = rest[len(POST):]
    net = Net(send, recv, local)
    net.greet()
    loads = {n: net.fetch(w.at[layer], s[n]) for n, w in (("wo", wo), ("win", win), ("wout", wout))}
    wu_load = net.fetch(wu, w_buf)
    gains = gx_ref[...]
    h2 = post_attention(net, model_dim, o_ref, ht_ref[...], gains[:, layers + layer:layers + layer + 1],
                        s["wo"], s["win"], s["wout"], s, lambda n: loads[n].wait())
    waits = norm_send(net, h2, s["hx2"], s["ssq2"])
    h_out[...] = h2.astype(F32).T.astype(BF)
    wu_load.wait()
    xn = norm_finish(waits, s["hx2"], s["ssq2"], gains[:, 2 * layers:2 * layers + 1], model_dim)
    v_loc = got_b.shape[0]
    step = 512
    spans = [(a, min(step, v_loc - a)) for a in range(0, v_loc, step)]

    def product(chip, core, a, n):
        start = pl.multiple_of((2 * chip + core) * v_loc + a, 16)
        return jnp.dot(w_buf[pl.ds(start, n), :], xn, preferred_element_type=F32)

    first, second = [], []

    def stage1(a, n):
        for chip in range(2):
            send_a[chip, pl.ds(a, n)] = product(chip, 1 - net.core, a, n).astype(BF)
        first.append(net.put(send_a.at[:, pl.ds(a, n)], got_a.at[:, pl.ds(a, n)], net.sib))

    def stage2(r, a, n):
        far = 1 - net.chip
        y = product(far, net.core, a, n)
        first[r].wait_recv()
        send_b[pl.ds(a, n)] = (y + got_a[far, pl.ds(a, n)].astype(F32)).astype(BF)
        second.append(net.put(send_b.at[pl.ds(a, n)], got_b.at[pl.ds(a, n)], net.across))

    stage1(*spans[0])
    for r in range(len(spans)):
        if r + 1 < len(spans):
            stage1(*spans[r + 1])
        stage2(r, *spans[r])
    stores = []
    for r, (a, n) in enumerate(spans):
        y = product(net.chip, net.core, a, n) + got_a[net.chip, pl.ds(a, n)].astype(F32)
        second[r].wait_recv()
        stage[pl.ds(a, n)] = y + got_b[pl.ds(a, n)].astype(F32)
        stores.append(net.fetch(stage.at[pl.ds(a, n)], logit_out.at[pl.ds(a, n)]))
    for c in stores:
        c.wait()
    net.finish()


def sds(shape, dtype):
    return jax.ShapeDtypeStruct(shape, dtype)


def solution(mesh):
    def decode_step(h_loc, seq_lens, k_cache, v_cache, g_attn, w_q, w_k, w_v, w_o, g_mlp, w_in, w_out, g_final, w_unemb):
        batch, blk = h_loc.shape
        layers = w_q.shape[0]
        model_dim = 8 * blk
        heads, dh = k_cache.shape[2], k_cache.shape[4]
        k_in, n_qkv = w_q.shape[1:]
        f_loc = w_in.shape[2]
        v_all = w_unemb.shape[1]
        v_loc = v_all // 4
        width = heads * dh
        kc = jnp.swapaxes(k_cache, 3, 4)
        vc = jnp.swapaxes(v_cache, 3, 4)
        wu = w_unemb.T
        gains = jnp.concatenate([g_attn, g_mlp, g_final[None]], axis=0)
        gains = jnp.pad(gains, ((0, 128 - gains.shape[0]), (0, 0))).T.astype(F32)

        qkv_bufs = [
            pltpu.VMEM((3, k_in, n_qkv), BF),
            pltpu.VMEM((3, 4, width, batch), BF), pltpu.VMEM((3, 2, width, batch), BF),
            pltpu.VMEM((3, width, batch), BF), pltpu.VMEM((3, width, batch), BF),
        ]
        qkv_outs = [sds((batch, width), F32)] * 3 + [sds((width, batch), BF)] * 2 + [sds((blk, batch), BF)]

        def sems(remote, local):
            return [pltpu.SemaphoreType.DMA((remote,)), pltpu.SemaphoreType.DMA((remote,)), pltpu.SemaphoreType.DMA((local,))]

        def params(cid):
            return pltpu.CompilerParams(collective_id=cid, has_side_effects=True, vmem_limit_bytes=56 * 2**20)

        q, k, v, kt, vt, ht, gx = pl.pallas_call(
            functools.partial(kernel_a, model_dim, 0),
            name="stage_a",
            out_shape=qkv_outs + [sds((2 * blk, 128), F32)],
            in_specs=[VM, VM, ANY, ANY, ANY],
            out_specs=[VM] * 7,
            scratch_shapes=[pltpu.VMEM((2, blk, batch), BF), pltpu.VMEM((8, 1, batch), F32),
                            pltpu.VMEM((2, blk, 128), F32)] + qkv_bufs + sems(15, 3),
            compiler_params=params(0),
        )(h_loc, gains, w_q, w_k, w_v)
        kts, vts = [kt], [vt]
        for layer in range(layers - 1):
            o = attention(layer, seq_lens, q, k, v, kc, vc)
            q, k, v, kt, vt, ht = pl.pallas_call(
                functools.partial(kernel_b, model_dim, layers, layer),
                name="stage_b",
                out_shape=qkv_outs,
                in_specs=[VM, VM, VM] + [ANY] * 6,
                out_specs=[VM] * 6,
                scratch_shapes=post_shapes(blk, batch, f_loc, w_o.shape[1]) + qkv_bufs + sems(32, 6),
                compiler_params=params(1 + layer),
            )(o, ht, gx, w_o, w_in, w_out, w_q, w_k, w_v)
            kts.append(kt)
            vts.append(vt)
        layer = layers - 1
        o = attention(layer, seq_lens, q, k, v, kc, vc)
        h_out, logits_t = pl.pallas_call(
            functools.partial(kernel_c, model_dim, layers, layer),
            name="stage_c",
            out_shape=[sds((batch, blk), BF), sds((v_loc, batch), F32)],
            in_specs=[VM, VM, VM] + [ANY] * 4,
            out_specs=[VM, ANY],
            scratch_shapes=post_shapes(blk, batch, f_loc, w_o.shape[1]) + [
                pltpu.VMEM((v_all, 2 * blk), BF),
                pltpu.VMEM((2, v_loc, batch), BF), pltpu.VMEM((2, v_loc, batch), BF),
                pltpu.VMEM((v_loc, batch), BF), pltpu.VMEM((v_loc, batch), BF), pltpu.VMEM((v_loc, batch), F32),
            ] + sems(64, 16),
            compiler_params=params(layers),
        )(o, ht, gx, w_o, w_in, w_out, wu)

        def entries(parts):
            return jnp.transpose(jnp.stack(parts).reshape(layers, heads, dh, batch), (0, 3, 1, 2))

        return h_out, logits_t.T, entries(kts), entries(vts)

    emb_spec = P('dp', ('x', 'yz'))
    gain_spec = P(None, ('x', 'yz'))
    cache_spec = P(None, 'dp', ('yz', 'x'), None, None)
    in_rows = P(None, 'x', 'yz')
    out_rows = P(None, 'yz', 'x')
    new_spec = P(None, 'dp', ('yz', 'x'), None)
    in_specs = (emb_spec, P('dp'), cache_spec, cache_spec, gain_spec, in_rows, in_rows, in_rows, out_rows, gain_spec, in_rows, out_rows, P(('x', 'yz')), P('x', 'yz'))
    out_specs = (emb_spec, P('dp', ('yz', 'x')), new_spec, new_spec)
    return jax.shard_map(decode_step, mesh=mesh, in_specs=in_specs, out_specs=out_specs, check_vma=False)
```

```python
import functools

import jax
import jax.numpy as jnp
from jax import lax
from jax.experimental import pallas as pl
from jax.experimental.pallas import tpu as pltpu
from jax.sharding import PartitionSpec as P

NORM_EPS = 1e-6
MESH = pl.DeviceIdType.MESH
BF = jnp.bfloat16
F32 = jnp.float32
ANY = pl.BlockSpec(memory_space=pl.ANY)
VM = pl.BlockSpec(memory_space=pltpu.VMEM)
SEQ_STEP = 16
SLOTS = 5
WINDOWS = (768, 176, 208, 224, 240, 768, 176, 208, 224)
COPIES = 150


def tdot(w, act):
    return lax.dot_general(w, act, (((0,), (0,)), ((), ())), preferred_element_type=F32)


class Attention:
    def __init__(self, lens_ref, kc_ref, vc_ref, q_ref, k_ref, v_ref, o_ref, kbuf, vbuf, pbuf, pnew, sems):
        self.lens, self.kc, self.vc = lens_ref, kc_ref, vc_ref
        self.q, self.k, self.v, self.o = q_ref, k_ref, v_ref, o_ref
        self.kbuf, self.vbuf, self.pbuf, self.pnew, self.sems = kbuf, vbuf, pbuf, pnew, sems
        self.layers = kc_ref.shape[0]
        self.batch, self.width = q_ref.shape
        self.dh, self.cache_len = kc_ref.shape[3], kc_ref.shape[4]
        self.steps = self.batch // SEQ_STEP
        self.groups = range(SEQ_STEP // 8)
        self.row = lax.broadcasted_iota(jnp.int32, (16, self.width), 0) % 8
        self.pos = lax.broadcasted_iota(jnp.int32, (16, self.cache_len), 1)
        self.row8 = lax.broadcasted_iota(jnp.int32, (8, self.width), 0)
        self.first_head = lax.broadcasted_iota(jnp.int32, (8, self.width), 1) < self.dh

    def copy(self, g, n):
        slot = lax.rem(g, SLOTS)
        src, buf = ((self.kc, self.kbuf), (self.vc, self.vbuf))[n]
        block = src.at[g // self.steps, pl.ds(lax.rem(g, self.steps) * SEQ_STEP, SEQ_STEP)]
        return pltpu.make_async_copy(block, buf.at[slot], self.sems.at[slot, n])

    def issue(self, g):
        for n in range(2):
            self.copy(g, n).start()

    def start(self):
        for g in range(SLOTS):
            self.issue(jnp.int32(g))

    def base(self, step, g):
        return pl.multiple_of(step * SEQ_STEP + 8 * g, 8)

    def score(self, step, slot):
        q2s, scores = [], []
        for g in self.groups:
            q8 = self.q[pl.ds(self.base(step, g), 8), :]
            q2 = jnp.concatenate([jnp.where(self.first_head, q8, 0.0), jnp.where(self.first_head, 0.0, q8)], axis=0)
            qbd = jnp.concatenate([jnp.where(self.row == n, q2, 0.0) for n in range(8)], axis=1).astype(BF)
            kb = self.kbuf[slot, 8 * g:8 * g + 8].reshape(8 * self.width, self.cache_len)
            scores.append(jnp.dot(qbd, kb, preferred_element_type=F32))
            q2s.append(q2)
        return q2s, scores

    def softmax(self, step, q2s, scores):
        for g in self.groups:
            k8 = self.k[pl.ds(self.base(step, g), 8), :]
            k2 = jnp.concatenate([k8, k8], axis=0)
            s_new = jnp.sum(q2s[g] * k2, axis=1, keepdims=True) * (self.dh ** -0.5)
            lens8 = jnp.zeros((8, self.width), jnp.int32)
            for n in range(8):
                lens8 = jnp.where(self.row8 == n, self.lens[self.base(step, g) + n], lens8)
            lens16 = jnp.concatenate([lens8, lens8], axis=0)
            lens_full = jnp.concatenate([lens16] * (self.cache_len // self.width), axis=1)
            s = jnp.where(self.pos < lens_full, scores[g] * (self.dh ** -0.5), -1e30)
            top = jnp.maximum(jnp.max(s, axis=1, keepdims=True), s_new)
            e = jnp.exp(s - top)
            e_new = jnp.exp(s_new - top)
            inv = 1.0 / (jnp.sum(e, axis=1, keepdims=True) + e_new)
            self.pbuf[g] = (e * inv).astype(BF)
            self.pnew[g] = jnp.broadcast_to((e_new * inv).astype(BF).astype(F32), (16, self.width))

    def mix(self, step, slot):
        w = self.width
        for g in self.groups:
            vb = self.vbuf[slot, 8 * g:8 * g + 8].reshape(8 * w, self.cache_len)
            mixed = lax.dot_general(self.pbuf[g], vb, (((1,), (1,)), ((), ())), preferred_element_type=F32)
            o2 = jnp.zeros((16, w), F32)
            for n in range(8):
                o2 = jnp.where(self.row == n, mixed[:, n * w:(n + 1) * w], o2)
            v8 = self.v[pl.ds(self.base(step, g), 8), :]
            o2 = o2 + self.pnew[g] * jnp.concatenate([v8, v8], axis=0)
            self.o[pl.ds(self.base(step, g), 8), :] = jnp.where(self.first_head, o2[:8], o2[8:])

    def layer(self, layer):
        first = layer * self.steps
        last = self.layers * self.steps

        def fetched(step, n):
            self.copy(first + step, n).wait()
            return lax.rem(first + step, SLOTS)

        self.softmax(0, *self.score(0, fetched(jnp.int32(0), 0)))

        def body(step, carry):
            nxt = first + step - 2 + SLOTS

            @pl.when((step >= 2) & (nxt < last))
            def _():
                self.issue(nxt)

            k_slot = fetched(step, 0)
            v_slot = fetched(step - 1, 1)
            q2s, scores = self.score(step, k_slot)
            self.mix(step - 1, v_slot)
            self.softmax(step, q2s, scores)
            return carry

        lax.fori_loop(1, self.steps, body, 0)
        self.mix(self.steps - 1, fetched(jnp.int32(self.steps - 1), 1))
        for g in (first + self.steps - 2 + SLOTS, first + self.steps - 1 + SLOTS):
            if g < last:
                self.issue(jnp.int32(g))


class Net:
    def __init__(self, send, recv, local):
        self.i = lax.axis_index("x")
        self.j = lax.axis_index("yz")
        self.chip = self.i // 2
        self.core = lax.rem(self.i, 2)
        self.sib = {"x": 2 * self.chip + 1 - self.core}
        self.across = {"x": lax.rem(self.i + 2, 4)}
        self.yother = {"yz": 1 - self.j}
        self.send, self.recv, self.local = send, recv, local
        self.n = 0
        self.m = 0
        self.sent = []

    def greet(self):
        self.barrier = pltpu.get_barrier_semaphore()
        for dx in range(4):
            for dy in range(2):
                if dx or dy:
                    pl.semaphore_signal(self.barrier, inc=1, device_id=self.peer(dx, dy), device_id_type=MESH)

    def met(self):
        pl.semaphore_wait(self.barrier, 7)

    def peer(self, dx, dy):
        return {"x": lax.rem(self.i + dx, 4), "yz": lax.rem(self.j + dy, 2)}

    def put(self, src, dst, to):
        c = pltpu.make_async_remote_copy(
            src_ref=src, dst_ref=dst, send_sem=self.send.at[self.n], recv_sem=self.recv.at[self.n],
            device_id=to, device_id_type=MESH)
        self.n += 1
        c.start()
        self.sent.append(c)
        return c

    def fetch(self, src, dst):
        c = pltpu.make_async_copy(src, dst, self.local.at[self.m])
        self.m += 1
        c.start()
        return c

    def finish(self):
        for c in self.sent:
            c.wait_send()


def slot_of(d):
    return 2 * (d % 2) + d // 2


def rs_first(net, part, got):
    return net.put(part.at[pl.ds(2 * (1 - net.core), 2)], got, net.sib)


def rs_second(net, wait, part, got, out, back):
    wait.wait_recv()
    far = 1 - net.chip
    out[...] = (part[2 * net.core + far].astype(F32) + got[far].astype(F32)).astype(BF)
    return net.put(out, back, net.across)


def rs_last(net, wait, part, got, back):
    mine = part[2 * net.core + net.chip].astype(F32) + got[net.chip].astype(F32)
    wait.wait_recv()
    return mine + back[...].astype(F32)


def qkv_stage(net, xn, w, s, q_out, k_out, v_out, kt_out, vt_out):
    part, got, out, back = s["qkv_part"], s["qkv_got"], s["qkv_out"], s["qkv_back"]
    first = []
    for n in range(3):
        y = tdot(w[n], xn).astype(BF)
        r = y.shape[0] // 4
        for d in range(4):
            part[n, slot_of(d)] = y[d * r:(d + 1) * r]
        first.append(rs_first(net, part.at[n], got.at[n]))
    second = [rs_second(net, first[n], part.at[n], got.at[n], out.at[n], back.at[n]) for n in range(3)]
    for n in range(3):
        y = rs_last(net, second[n], part.at[n], got.at[n], back.at[n]).astype(BF)
        if n:
            (kt_out, vt_out)[n - 1][...] = y
        (q_out, k_out, v_out)[n][...] = y.astype(F32).T


def gather_x(net, buf):
    me = buf.at[net.i]
    across = net.put(me, me, net.across)
    sib = net.put(me, me, net.sib)
    return sib, across


def gather_forward(net, buf, across):
    across.wait_recv()
    far = buf.at[lax.rem(net.i + 2, 4)]
    return net.put(far, far, net.sib)


def sum_yz(net, y, part, got):
    r = y.shape[0] // 2
    part[0] = y[:r].astype(BF)
    part[1] = y[r:].astype(BF)
    c = net.put(part.at[1 - net.j], got, net.yother)
    c.wait_recv()
    return part[net.j].astype(F32) + got[...].astype(F32)


def norm_send(net, h_own, hx, ssq, far=False):
    hf = h_own.astype(F32)
    me = 2 * net.i + net.j
    hx[0, net.j] = h_own
    ssq[me] = jnp.sum(hf * hf, axis=0, keepdims=True)
    mine = hx.at[0, net.j]
    stats = []
    for dx in range(4):
        for dy in range(2):
            if dx or dy:
                stats.append(net.put(ssq.at[me], ssq.at[me], net.peer(dx, dy)))
    near = net.put(mine, hx.at[0, net.j], net.yother)
    fars = [net.put(mine, hx.at[1, net.j], to) for to in (net.across, net.peer(2, 1))] if far else []
    return stats, near, fars


def norm_scale(stats, ssq, model_dim):
    for c in stats:
        c.wait_recv()
    total = ssq[0]
    for n in range(1, 8):
        total = total + ssq[n]
    return lax.rsqrt(total / model_dim + NORM_EPS)


def normed(hx, inv, gain):
    rows = hx.shape[0] * hx.shape[1]
    return (hx[...].reshape(rows, hx.shape[2]).astype(F32) * inv * gain).astype(BF)


def columns(gx, n):
    return jnp.concatenate([gx[0].T[:, n:n + 1], gx[1].T[:, n:n + 1]], axis=0)


def kernel(names, model_dim, h_ref, lens_ref, kc, vc, g_ref, wq, wk, wv, wo, win, wout, wu, h_out, logit_out, kt_out, vt_out, *rest):
    s = dict(zip(names, rest))
    kv_sems, send, recv, local = rest[len(names):]
    layers = wq.shape[0]
    net = Net(send, recv, local)
    net.greet()
    mats = (("wo", wo), ("win", win), ("wout", wout))
    loads = {("qkv", 0): [net.fetch(w.at[0], s["wqkv0"].at[n]) for n, w in enumerate((wq, wk, wv))]}
    att = Attention(lens_ref, kc, vc, s["q"], s["k"], s["v"], s["att"], s["kbuf"], s["vbuf"], s["pbuf"], s["pnew"], kv_sems)
    for l in range(layers):
        if l:
            loads["qkv", l] = [net.fetch(w.at[l], s[f"wqkv{l}"].at[n]) for n, w in enumerate((wq, wk, wv))]
        for name, w in mats:
            loads[name, l] = [net.fetch(w.at[l], s[f"{name}{l}"])]
    att.start()

    def weight(name, l):
        for c in loads.pop((name, l)):
            c.wait()
        return s[f"{name}{l}"]

    v_loc = logit_out.shape[0]
    early = []
    far_chip = 1 - net.chip

    def window(n):
        a = sum(WINDOWS[:n])
        for core in range(2):
            src = wu.at[pl.ds(pl.multiple_of((2 * far_chip + core) * v_loc + a, 16), WINDOWS[n])]
            early.append(net.put(src, s["wm"].at[core, pl.ds(a, WINDOWS[n])], net.across))

    gx, gfar = s["gx"], s["gfar"]
    h_own = h_ref[...].astype(F32).T.astype(BF)
    gx[net.j] = g_ref[...]
    net.met()
    g_near = net.put(gx.at[net.j], gx.at[net.j], net.yother)
    stats, near, _ = norm_send(net, h_own, s["hx_a0"], s["ssq_a0"])
    g_fars = [net.put(gx.at[net.j], gfar.at[net.j], to) for to in (net.across, net.peer(2, 1))]
    g_near.wait_recv()
    wn = 0
    for l in range(layers):
        inv = norm_scale(stats, s[f"ssq_a{l}"], model_dim)
        near.wait_recv()
        xn = normed(s[f"hx_a{l}"].at[0], inv, columns(gx, l))
        sl = {k[:-1]: s[k] for k in s if k.endswith(str(l))}
        qkv_stage(net, xn, wait_qkv(loads, s, l), sl, s["q"], s["k"], s["v"], kt_out.at[l], vt_out.at[l])
        window(wn)
        wn += 1
        att.layer(l)
        if l == layers - 1:
            wu_load = net.fetch(wu, s["wu"])
        o = sl["o"]
        o[net.i] = s["att"][...].T.astype(BF)
        sib, across = gather_x(net, o)
        w = weight("wo", l)
        fwd = gather_forward(net, o, across)
        window(wn)
        wn += 1
        sib.wait_recv()
        fwd.wait_recv()
        delta = sum_yz(net, tdot(w[...], o[...].reshape(-1, o.shape[2])), sl["ypart1"], sl["ygot1"])
        h_own = (h_own.astype(F32) + delta).astype(BF)
        stats, near, _ = norm_send(net, h_own, sl["hx_m"], sl["ssq_m"])
        window(wn)
        wn += 1
        w = weight("win", l)
        inv = norm_scale(stats, sl["ssq_m"], model_dim)
        near.wait_recv()
        xn = normed(sl["hx_m"].at[0], inv, columns(gx, layers + l))
        r = w.shape[1] // 4
        y = tdot(w[...], xn).astype(BF)
        for d in range(4):
            sl["upart"][slot_of(d)] = y[d * r:(d + 1) * r]
        first = rs_first(net, sl["upart"], sl["ugot"])
        second = rs_second(net, first, sl["upart"], sl["ugot"], sl["uout"], sl["uback"])
        up = rs_last(net, second, sl["upart"], sl["ugot"], sl["uback"]).astype(BF)
        u = sl["u"]
        u[net.i] = jax.nn.gelu(up.astype(F32)).astype(BF)
        sib, across = gather_x(net, u)
        w = weight("wout", l)
        fwd = gather_forward(net, u, across)
        window(wn)
        wn += 1
        sib.wait_recv()
        fwd.wait_recv()
        delta = sum_yz(net, tdot(w[...], u[...].reshape(-1, u.shape[2])), sl["ypart2"], sl["ygot2"])
        h_own = (h_own.astype(F32) + delta).astype(BF)
        end = l == layers - 1
        stats, near, fars = norm_send(net, h_own, s[f"hx_a{l + 1}"], s[f"ssq_a{l + 1}"], far=end)
        if not end:
            window(wn)
            wn += 1
    h_out[...] = h_own.astype(F32).T.astype(BF)
    unembed(net, s, model_dim, 2 * layers, stats, near, fars, g_fars, early, wu_load, s[f"hx_a{layers}"], s[f"ssq_a{layers}"], logit_out)
    net.finish()


def wait_qkv(loads, s, l):
    for c in loads.pop(("qkv", l)):
        c.wait()
    return s[f"wqkv{l}"]


def unembed(net, s, model_dim, gain_row, stats, near, fars, g_fars, early, wu_load, hx, ssq, logit_out):
    v_loc = logit_out.shape[0]
    moved = sum(WINDOWS)
    left = v_loc - moved
    wu, wm, stage = s["wu"], s["wm"], s["stage"]
    inv = norm_scale(stats, ssq, model_dim)
    near.wait_recv()
    xn = normed(hx.at[0], inv, columns(s["gx"], gain_row))
    wu_load.wait()
    far_chip = 1 - net.chip
    send_a, got_a, send_b, got_b = s["send_a"], s["got_a"], s["send_b"], s["got_b"]

    def rows(chip, core, a, n):
        return wu[pl.ds(pl.multiple_of((2 * chip + core) * v_loc + a, 16), n), :]

    def product(chip, core, a, n):
        return jnp.dot(rows(chip, core, moved + a, n), xn, preferred_element_type=F32)

    spans = [(a, min(512, left - a)) for a in range(0, left, 512)]
    first, second = [], []

    def stage1(a, n):
        for chip in range(2):
            send_a[chip, pl.ds(a, n)] = product(chip, 1 - net.core, a, n).astype(BF)
        first.append(net.put(send_a.at[:, pl.ds(a, n)], got_a.at[:, pl.ds(a, n)], net.sib))

    def stage2(r, a, n):
        y = product(far_chip, net.core, a, n)
        first[r].wait_recv()
        send_b[pl.ds(a, n)] = (y + got_a[far_chip, pl.ds(a, n)].astype(F32)).astype(BF)
        second.append(net.put(send_b.at[pl.ds(a, n)], got_b.at[pl.ds(a, n)], net.across))

    stage1(*spans[0])
    for r in range(len(spans)):
        if r + 1 < len(spans):
            stage1(*spans[r + 1])
        stage2(r, *spans[r])

    stores = []

    def store(a, n):
        stores.append(net.fetch(stage.at[pl.ds(a, n)], logit_out.at[pl.ds(a, n)]))

    for c in fars + g_fars + early:
        c.wait_recv()
    xf = normed(hx.at[1], inv, columns(s["gfar"], gain_row))
    x2 = jnp.concatenate([xn, xf], axis=0)
    mspans = [(a, min(512, moved - a)) for a in range(0, moved, 512)]
    send_m, got_m = s["send_m"], s["got_m"]
    third = []

    def both(core, a, n):
        w2 = jnp.concatenate([rows(net.chip, core, a, n), wm[core, pl.ds(a, n), :]], axis=1)
        return jnp.dot(w2, x2, preferred_element_type=F32)

    for a, n in mspans:
        send_m[pl.ds(a, n)] = both(1 - net.core, a, n).astype(BF)
        third.append(net.put(send_m.at[pl.ds(a, n)], got_m.at[pl.ds(a, n)], net.sib))
    for r, (a, n) in enumerate(mspans):
        y = both(net.core, a, n)
        third[r].wait_recv()
        stage[pl.ds(a, n)] = y + got_m[pl.ds(a, n)].astype(F32)
        store(a, n)
    for r, (a, n) in enumerate(spans):
        y = product(net.chip, net.core, a, n) + got_a[net.chip, pl.ds(a, n)].astype(F32)
        second[r].wait_recv()
        stage[pl.ds(moved + a, n)] = y + got_b[pl.ds(a, n)].astype(F32)
        store(moved + a, n)
    for c in stores:
        c.wait()


def scratch(layers, blk, batch, k_o, f_loc, n_qkv, v_loc, width, heads, dh, cache_len):
    r = f_loc // 4
    moved = sum(WINDOWS)
    left = v_loc - moved
    t = {}
    for l in range(layers + 1):
        t[f"hx_a{l}"] = ((2 if l == layers else 1, 2, blk, batch), BF)
        t[f"ssq_a{l}"] = ((8, 1, batch), F32)
    for l in range(layers):
        t.update({
            f"wqkv{l}": ((3, 2 * blk, n_qkv), BF), f"wo{l}": ((k_o, 2 * blk), BF),
            f"win{l}": ((2 * blk, f_loc), BF), f"wout{l}": ((f_loc, 2 * blk), BF),
            f"qkv_part{l}": ((3, 4, width, batch), BF), f"qkv_got{l}": ((3, 2, width, batch), BF),
            f"qkv_out{l}": ((3, width, batch), BF), f"qkv_back{l}": ((3, width, batch), BF),
            f"o{l}": ((4, width, batch), BF),
            f"ypart1{l}": ((2, blk, batch), BF), f"ygot1{l}": ((blk, batch), BF),
            f"hx_m{l}": ((1, 2, blk, batch), BF), f"ssq_m{l}": ((8, 1, batch), F32),
            f"upart{l}": ((4, r, batch), BF), f"ugot{l}": ((2, r, batch), BF),
            f"uout{l}": ((r, batch), BF), f"uback{l}": ((r, batch), BF), f"u{l}": ((4, r, batch), BF),
            f"ypart2{l}": ((2, blk, batch), BF), f"ygot2{l}": ((blk, batch), BF),
        })
    t.update({
        "gx": ((2, 8, blk), F32), "gfar": ((2, 8, blk), F32),
        "q": ((batch, width), F32), "k": ((batch, width), F32), "v": ((batch, width), F32), "att": ((batch, width), F32),
        "kbuf": ((SLOTS, SEQ_STEP, heads, dh, cache_len), BF), "vbuf": ((SLOTS, SEQ_STEP, heads, dh, cache_len), BF),
        "pbuf": ((SEQ_STEP // 8, 16, cache_len), BF), "pnew": ((SEQ_STEP // 8, 16, width), F32),
        "wu": ((4 * v_loc, 2 * blk), BF), "wm": ((2, moved, 2 * blk), BF),
        "send_a": ((2, left, batch), BF), "got_a": ((2, left, batch), BF),
        "send_b": ((left, batch), BF), "got_b": ((left, batch), BF),
        "send_m": ((moved, batch), BF), "got_m": ((moved, batch), BF),
        "stage": ((v_loc, batch), F32),
    })
    return t


def sds(shape, dtype):
    return jax.ShapeDtypeStruct(shape, dtype)


def solution(mesh):
    def decode_step(h_loc, seq_lens, k_cache, v_cache, g_attn, w_q, w_k, w_v, w_o, g_mlp, w_in, w_out, g_final, w_unemb):
        batch, blk = h_loc.shape
        layers = w_q.shape[0]
        heads, dh, cache_len = k_cache.shape[2], k_cache.shape[4], k_cache.shape[3]
        v_loc = w_unemb.shape[1] // 4
        width = heads * dh
        kc = jnp.swapaxes(k_cache, 3, 4)
        vc = jnp.swapaxes(v_cache, 3, 4)
        gains = jnp.concatenate([g_attn, g_mlp, g_final[None]], axis=0).astype(F32)
        gains = jnp.pad(gains, ((0, 8 - gains.shape[0]), (0, 0)))
        names = scratch(layers, blk, batch, w_o.shape[1], w_in.shape[2], w_q.shape[2], v_loc, width, heads, dh, cache_len)
        h_out, logits_t, kt, vt = pl.pallas_call(
            functools.partial(kernel, tuple(names), 8 * blk),
            name="decode",
            out_shape=[sds((batch, blk), BF), sds((v_loc, batch), F32)] + [sds((layers, width, batch), BF)] * 2,
            in_specs=[VM, pl.BlockSpec(memory_space=pltpu.SMEM), ANY, ANY, VM] + [ANY] * 7,
            out_specs=[VM, ANY, VM, VM],
            scratch_shapes=[pltpu.VMEM(shape, dtype) for shape, dtype in names.values()] + [
                pltpu.SemaphoreType.DMA((SLOTS, 2)),
                pltpu.SemaphoreType.DMA((COPIES,)), pltpu.SemaphoreType.DMA((COPIES,)), pltpu.SemaphoreType.DMA((40,))],
            compiler_params=pltpu.CompilerParams(collective_id=0, has_side_effects=True, vmem_limit_bytes=67043328),
        )(h_loc, seq_lens, kc, vc, gains, w_q, w_k, w_v, w_o, w_in, w_out, w_unemb.T)

        def entries(t):
            return jnp.transpose(t.reshape(layers, heads, dh, batch), (0, 3, 1, 2))

        return h_out, logits_t.T, entries(kt), entries(vt)

    emb_spec = P('dp', ('x', 'yz'))
    gain_spec = P(None, ('x', 'yz'))
    cache_spec = P(None, 'dp', ('yz', 'x'), None, None)
    in_rows = P(None, 'x', 'yz')
    out_rows = P(None, 'yz', 'x')
    new_spec = P(None, 'dp', ('yz', 'x'), None)
    in_specs = (emb_spec, P('dp'), cache_spec, cache_spec, gain_spec, in_rows, in_rows, in_rows, out_rows, gain_spec, in_rows, out_rows, P(('x', 'yz')), P('x', 'yz'))
    out_specs = (emb_spec, P('dp', ('yz', 'x')), new_spec, new_spec)
    return jax.shard_map(decode_step, mesh=mesh, in_specs=in_specs, out_specs=out_specs, check_vma=False)
```

```python
import functools

import jax
import jax.numpy as jnp
from jax import lax
from jax.experimental import pallas as pl
from jax.experimental.pallas import tpu as pltpu
from jax.sharding import PartitionSpec as P

NORM_EPS = 1e-6
MESH = pl.DeviceIdType.MESH
BF = jnp.bfloat16
F32 = jnp.float32
ANY = pl.BlockSpec(memory_space=pl.ANY)
VM = pl.BlockSpec(memory_space=pltpu.VMEM)
SEQ_STEP = 16
SLOTS = 5
WINDOWS = (176, 768, 176, 240, 208, 288, 768, 176, 240, 208, 128)
COPIES = 170
OUT_ROWS = 512


def tdot(w, act):
    return lax.dot_general(w, act, (((0,), (0,)), ((), ())), preferred_element_type=F32)


class Attention:
    def __init__(self, lens_ref, kc_ref, vc_ref, q_ref, k_ref, v_ref, o_ref, kbuf, vbuf, pbuf, pnew, sems):
        self.lens, self.kc, self.vc = lens_ref, kc_ref, vc_ref
        self.q, self.k, self.v, self.o = q_ref, k_ref, v_ref, o_ref
        self.kbuf, self.vbuf, self.pbuf, self.pnew, self.sems = kbuf, vbuf, pbuf, pnew, sems
        self.layers = kc_ref.shape[0]
        self.batch, self.width = q_ref.shape
        self.dh, self.cache_len = kc_ref.shape[3], kc_ref.shape[4]
        self.steps = self.batch // SEQ_STEP
        self.groups = range(SEQ_STEP // 8)
        self.row = lax.broadcasted_iota(jnp.int32, (16, self.width), 0) % 8
        self.pos = lax.broadcasted_iota(jnp.int32, (16, self.cache_len), 1)
        self.row8 = lax.broadcasted_iota(jnp.int32, (8, self.width), 0)
        self.first_head = lax.broadcasted_iota(jnp.int32, (8, self.width), 1) < self.dh

    def copy(self, g, n):
        slot = lax.rem(g, SLOTS)
        src, buf = ((self.kc, self.kbuf), (self.vc, self.vbuf))[n]
        block = src.at[g // self.steps, pl.ds(lax.rem(g, self.steps) * SEQ_STEP, SEQ_STEP)]
        return pltpu.make_async_copy(block, buf.at[slot], self.sems.at[slot, n])

    def issue(self, g):
        for n in range(2):
            self.copy(g, n).start()

    def start(self):
        for g in range(SLOTS):
            self.issue(jnp.int32(g))

    def base(self, step, g):
        return pl.multiple_of(step * SEQ_STEP + 8 * g, 8)

    def score(self, step, slot):
        q2s, scores = [], []
        for g in self.groups:
            q8 = self.q[pl.ds(self.base(step, g), 8), :]
            q2 = jnp.concatenate([jnp.where(self.first_head, q8, 0.0), jnp.where(self.first_head, 0.0, q8)], axis=0)
            qbd = jnp.concatenate([jnp.where(self.row == n, q2, 0.0) for n in range(8)], axis=1).astype(BF)
            kb = self.kbuf[slot, 8 * g:8 * g + 8].reshape(8 * self.width, self.cache_len)
            scores.append(jnp.dot(qbd, kb, preferred_element_type=F32))
            q2s.append(q2)
        return q2s, scores

    def softmax(self, step, q2s, scores):
        for g in self.groups:
            k8 = self.k[pl.ds(self.base(step, g), 8), :]
            k2 = jnp.concatenate([k8, k8], axis=0)
            s_new = jnp.sum(q2s[g] * k2, axis=1, keepdims=True) * (self.dh ** -0.5)
            lens8 = jnp.zeros((8, self.width), jnp.int32)
            for n in range(8):
                lens8 = jnp.where(self.row8 == n, self.lens[self.base(step, g) + n], lens8)
            lens16 = jnp.concatenate([lens8, lens8], axis=0)
            lens_full = jnp.concatenate([lens16] * (self.cache_len // self.width), axis=1)
            s = jnp.where(self.pos < lens_full, scores[g] * (self.dh ** -0.5), -1e30)
            top = jnp.maximum(jnp.max(s, axis=1, keepdims=True), s_new)
            e = jnp.exp(s - top)
            e_new = jnp.exp(s_new - top)
            inv = 1.0 / (jnp.sum(e, axis=1, keepdims=True) + e_new)
            self.pbuf[g] = (e * inv).astype(BF)
            self.pnew[g] = jnp.broadcast_to((e_new * inv).astype(BF).astype(F32), (16, self.width))

    def mix(self, step, slot):
        w = self.width
        for g in self.groups:
            vb = self.vbuf[slot, 8 * g:8 * g + 8].reshape(8 * w, self.cache_len)
            mixed = lax.dot_general(self.pbuf[g], vb, (((1,), (1,)), ((), ())), preferred_element_type=F32)
            o2 = jnp.zeros((16, w), F32)
            for n in range(8):
                o2 = jnp.where(self.row == n, mixed[:, n * w:(n + 1) * w], o2)
            v8 = self.v[pl.ds(self.base(step, g), 8), :]
            o2 = o2 + self.pnew[g] * jnp.concatenate([v8, v8], axis=0)
            self.o[pl.ds(self.base(step, g), 8), :] = jnp.where(self.first_head, o2[:8], o2[8:])

    def layer(self, layer):
        first = layer * self.steps
        last = self.layers * self.steps

        def fetched(step, n):
            self.copy(first + step, n).wait()
            return lax.rem(first + step, SLOTS)

        self.softmax(0, *self.score(0, fetched(jnp.int32(0), 0)))

        def body(step, carry):
            nxt = first + step - 2 + SLOTS

            @pl.when((step >= 2) & (nxt < last))
            def _():
                self.issue(nxt)

            k_slot = fetched(step, 0)
            v_slot = fetched(step - 1, 1)
            q2s, scores = self.score(step, k_slot)
            self.mix(step - 1, v_slot)
            self.softmax(step, q2s, scores)
            return carry

        lax.fori_loop(1, self.steps, body, 0)
        self.mix(self.steps - 1, fetched(jnp.int32(self.steps - 1), 1))
        for g in (first + self.steps - 2 + SLOTS, first + self.steps - 1 + SLOTS):
            if g < last:
                self.issue(jnp.int32(g))


class Net:
    def __init__(self, send, recv, local):
        self.i = lax.axis_index("x")
        self.j = lax.axis_index("yz")
        self.chip = self.i // 2
        self.core = lax.rem(self.i, 2)
        self.sib = {"x": 2 * self.chip + 1 - self.core}
        self.across = {"x": lax.rem(self.i + 2, 4)}
        self.yother = {"yz": 1 - self.j}
        self.send, self.recv, self.local = send, recv, local
        self.n = 0
        self.m = 0
        self.sent = []

    def greet(self):
        self.barrier = pltpu.get_barrier_semaphore()
        for dx in range(4):
            for dy in range(2):
                if dx or dy:
                    pl.semaphore_signal(self.barrier, inc=1, device_id=self.peer(dx, dy), device_id_type=MESH)

    def met(self):
        pl.semaphore_wait(self.barrier, 7)

    def peer(self, dx, dy):
        return {"x": lax.rem(self.i + dx, 4), "yz": lax.rem(self.j + dy, 2)}

    def put(self, src, dst, to):
        c = pltpu.make_async_remote_copy(
            src_ref=src, dst_ref=dst, send_sem=self.send.at[self.n], recv_sem=self.recv.at[self.n],
            device_id=to, device_id_type=MESH)
        self.n += 1
        c.start()
        self.sent.append(c)
        return c

    def fetch(self, src, dst):
        c = pltpu.make_async_copy(src, dst, self.local.at[self.m])
        self.m += 1
        c.start()
        return c

    def finish(self):
        for c in self.sent:
            c.wait_send()


def slot_of(d):
    return 2 * (d % 2) + d // 2


def rs_first(net, part, got):
    return net.put(part.at[pl.ds(2 * (1 - net.core), 2)], got, net.sib)


def rs_second(net, wait, part, got, out, back):
    wait.wait_recv()
    far = 1 - net.chip
    out[...] = (part[2 * net.core + far].astype(F32) + got[far].astype(F32)).astype(BF)
    return net.put(out, back, net.across)


def rs_last(net, wait, part, got, back):
    mine = part[2 * net.core + net.chip].astype(F32) + got[net.chip].astype(F32)
    wait.wait_recv()
    return mine + back[...].astype(F32)


def qkv_stage(net, xn, w, s, q_out, k_out, v_out, kt_out, vt_out):
    part, got, out, back = s["qkv_part"], s["qkv_got"], s["qkv_out"], s["qkv_back"]
    first = []
    for n in range(3):
        y = tdot(w[n], xn).astype(BF)
        r = y.shape[0] // 4
        for d in range(4):
            part[n, slot_of(d)] = y[d * r:(d + 1) * r]
        first.append(rs_first(net, part.at[n], got.at[n]))
    second = [rs_second(net, first[n], part.at[n], got.at[n], out.at[n], back.at[n]) for n in range(3)]
    for n in range(3):
        y = rs_last(net, second[n], part.at[n], got.at[n], back.at[n]).astype(BF)
        if n:
            (kt_out, vt_out)[n - 1][...] = y
        (q_out, k_out, v_out)[n][...] = y.astype(F32).T


def gather_x(net, buf):
    me = buf.at[net.i]
    across = net.put(me, me, net.across)
    sib = net.put(me, me, net.sib)
    return sib, across


def gather_forward(net, buf, across):
    across.wait_recv()
    far = buf.at[lax.rem(net.i + 2, 4)]
    return net.put(far, far, net.sib)


def sum_yz(net, w, act, part, got):
    r = got.shape[0]
    part[...] = tdot(w[:, pl.ds(pl.multiple_of((1 - net.j) * r, r), r)], act).astype(BF)
    c = net.put(part, got, net.yother)
    mine = tdot(w[:, pl.ds(pl.multiple_of(net.j * r, r), r)], act)
    c.wait_recv()
    return mine + got[...].astype(F32)


def norm_send(net, h_own, hx, ssq, far=False):
    hf = h_own.astype(F32)
    me = 2 * net.i + net.j
    hx[0, net.j] = h_own
    ssq[me] = jnp.sum(hf * hf, axis=0, keepdims=True)
    mine = hx.at[0, net.j]
    stats = []
    for dx in range(4):
        for dy in range(2):
            if dx or dy:
                stats.append(net.put(ssq.at[me], ssq.at[me], net.peer(dx, dy)))
    near = net.put(mine, hx.at[0, net.j], net.yother)
    fars = [net.put(mine, hx.at[1, net.j], to) for to in (net.across, net.peer(2, 1))] if far else []
    return stats, near, fars


def norm_scale(stats, ssq, model_dim):
    for c in stats:
        c.wait_recv()
    total = ssq[0]
    for n in range(1, 8):
        total = total + ssq[n]
    return lax.rsqrt(total / model_dim + NORM_EPS)


def normed(hx, inv, gain):
    rows = hx.shape[0] * hx.shape[1]
    return (hx[...].reshape(rows, hx.shape[2]).astype(F32) * inv * gain).astype(BF)


def columns(gx, n):
    return jnp.concatenate([gx[0].T[:, n:n + 1], gx[1].T[:, n:n + 1]], axis=0)


def kernel(names, model_dim, h_ref, lens_ref, kc, vc, ga, gm, gf, wq, wk, wv, wo, win, wout, wu, h_out, p_own, p_other, kt_out, vt_out, *rest):
    s = dict(zip(names, rest))
    kv_sems, send, recv, local = rest[len(names):]
    layers = wq.shape[0]
    net = Net(send, recv, local)
    net.greet()
    mats = (("wo", wo), ("win", win), ("wout", wout))
    loads = {("qkv", 0): [net.fetch(w.at[0], s["wqkv0"].at[n]) for n, w in enumerate((wq, wk, wv))]}
    att = Attention(lens_ref, kc, vc, s["q"], s["k"], s["v"], s["att"], s["kbuf"], s["vbuf"], s["pbuf"], s["pnew"], kv_sems)
    for l in range(layers):
        if l:
            loads["qkv", l] = [net.fetch(w.at[l], s[f"wqkv{l}"].at[n]) for n, w in enumerate((wq, wk, wv))]
        for name, w in mats:
            loads[name, l] = [net.fetch(w.at[l], s[f"{name}{l}"])]
    att.start()

    def weight(name, l):
        for c in loads.pop((name, l)):
            c.wait()
        return s[f"{name}{l}"]

    v_loc = p_own.shape[0]
    early = []
    far_chip = 1 - net.chip

    def window(n):
        a = sum(WINDOWS[:n])
        for core in range(2):
            src = wu.at[pl.ds(pl.multiple_of((2 * far_chip + core) * v_loc + a, 16), WINDOWS[n])]
            early.append(net.put(src, s["wm"].at[core, pl.ds(a, WINDOWS[n])], net.across))

    gx, gfar = s["gx"], s["gfar"]
    h_own = h_ref[...].astype(F32).T.astype(BF)
    for n, g in enumerate((ga, gm, gf)):
        gx[net.j, pl.ds(n * layers, g.shape[0])] = g[...].astype(F32)
    rest_rows = gx.shape[1] - 2 * layers - 1
    gx[net.j, pl.ds(2 * layers + 1, rest_rows)] = jnp.zeros((rest_rows, gx.shape[2]), F32)
    net.met()
    g_near = net.put(gx.at[net.j], gx.at[net.j], net.yother)
    stats, near, _ = norm_send(net, h_own, s["hx_a0"], s["ssq_a0"])
    g_fars = [net.put(gx.at[net.j], gfar.at[net.j], to) for to in (net.across, net.peer(2, 1))]
    window(0)
    g_near.wait_recv()
    wn = 1
    stores = []
    for l in range(layers):
        inv = norm_scale(stats, s[f"ssq_a{l}"], model_dim)
        near.wait_recv()
        xn = normed(s[f"hx_a{l}"].at[0], inv, columns(gx, l))
        sl = {k[:-1]: s[k] for k in s if k.endswith(str(l))}
        qkv_stage(net, xn, wait_qkv(loads, s, l), sl, s["q"], s["k"], s["v"], s["kt"].at[l], s["vt"].at[l])
        stores += [net.fetch(s["kt"].at[l], kt_out.at[l]), net.fetch(s["vt"].at[l], vt_out.at[l])]
        window(wn)
        wn += 1
        att.layer(l)
        if l == layers - 1:
            wu_load = net.fetch(wu, s["wu"])
        o = sl["o"]
        o[net.i] = s["att"][...].T.astype(BF)
        sib, across = gather_x(net, o)
        w = weight("wo", l)
        fwd = gather_forward(net, o, across)
        window(wn)
        wn += 1
        sib.wait_recv()
        fwd.wait_recv()
        delta = sum_yz(net, w, o[...].reshape(-1, o.shape[2]), sl["ypart1"], sl["ygot1"])
        h_own = (h_own.astype(F32) + delta).astype(BF)
        stats, near, _ = norm_send(net, h_own, sl["hx_m"], sl["ssq_m"])
        window(wn)
        wn += 1
        w = weight("win", l)
        inv = norm_scale(stats, sl["ssq_m"], model_dim)
        near.wait_recv()
        xn = normed(sl["hx_m"].at[0], inv, columns(gx, layers + l))
        r = w.shape[1] // 4
        y = tdot(w[...], xn).astype(BF)
        for d in range(4):
            sl["upart"][slot_of(d)] = y[d * r:(d + 1) * r]
        u = sl["u"]
        half = [pl.ds(n * (r // 2), r // 2) for n in range(2)]
        pieces = [[sl[k].at[:, h] for k in ("upart", "ugot")] + [sl[k].at[h] for k in ("uout", "uback")] for h in half]
        first = [rs_first(net, part, got) for part, got, out, back in pieces]
        second = [rs_second(net, first[n], *p) for n, p in enumerate(pieces)]
        sent = []
        for n, (part, got, out, back) in enumerate(pieces):
            up = rs_last(net, second[n], part, got, back).astype(BF)
            u[net.i, half[n]] = jax.nn.gelu(up.astype(F32)).astype(BF)
            sent.append(gather_x(net, u.at[:, half[n]]))
        window(wn)
        wn += 1
        w = weight("wout", l)
        fwd = [gather_forward(net, u.at[:, half[n]], sent[n][1]) for n in range(2)]
        for n in range(2):
            sent[n][0].wait_recv()
            fwd[n].wait_recv()
        delta = sum_yz(net, w, u[...].reshape(-1, u.shape[2]), sl["ypart2"], sl["ygot2"])
        h_own = (h_own.astype(F32) + delta).astype(BF)
        end = l == layers - 1
        stats, near, fars = norm_send(net, h_own, s[f"hx_a{l + 1}"], s[f"ssq_a{l + 1}"], far=end)
        window(wn)
        wn += 1
    s["h"][...] = h_own.astype(F32).T.astype(BF)
    stores.append(net.fetch(s["h"], h_out))
    unembed(net, s, model_dim, 2 * layers, stats, near, fars, g_fars, early, wu_load, s[f"hx_a{layers}"], s[f"ssq_a{layers}"], p_own, p_other, stores)
    for c in stores:
        c.wait()
    net.finish()


def wait_qkv(loads, s, l):
    for c in loads.pop(("qkv", l)):
        c.wait()
    return s[f"wqkv{l}"]


def unembed(net, s, model_dim, gain_row, stats, near, fars, g_fars, early, wu_load, hx, ssq, p_own, p_other, stores):
    v_loc = p_own.shape[0]
    moved = sum(WINDOWS)
    left = v_loc - moved
    wu, wm, own = s["wu"], s["wm"], s["own"]
    inv = norm_scale(stats, ssq, model_dim)
    near.wait_recv()
    xn = normed(hx.at[0], inv, columns(s["gx"], gain_row))
    wu_load.wait()
    far_chip = 1 - net.chip
    send_a, got_a, send_b = s["send_a"], s["got_a"], s["send_b"]

    def rows(chip, core, a, n):
        return wu[pl.ds(pl.multiple_of((2 * chip + core) * v_loc + a, 16), n), :]

    def product(chip, core, a, n):
        return jnp.dot(rows(chip, core, moved + a, n), xn, preferred_element_type=F32)

    spans = [(a, min(512, left - a)) for a in range(0, left, 512)]
    first, arrivals = [], []

    def stage1(a, n):
        for chip in range(2):
            send_a[chip, pl.ds(a, n)] = product(chip, 1 - net.core, a, n).astype(BF)
        first.append(net.put(send_a.at[:, pl.ds(a, n)], got_a.at[:, pl.ds(a, n)], net.sib))

    def stage2(r, a, n):
        y = product(far_chip, net.core, a, n)
        first[r].wait_recv()
        send_b[pl.ds(a, n)] = (y + got_a[far_chip, pl.ds(a, n)].astype(F32)).astype(BF)
        arrivals.append(net.put(send_b.at[pl.ds(a, n)], p_other.at[pl.ds(moved + a, n)], net.across))

    stage1(*spans[0])
    for r in range(len(spans)):
        if r + 1 < len(spans):
            stage1(*spans[r + 1])
        stage2(r, *spans[r])

    def store(a, n):
        stores.append(net.fetch(own.at[pl.ds(a, n)], p_own.at[pl.ds(a, n)]))

    for c in fars + g_fars + early:
        c.wait_recv()
    xf = normed(hx.at[1], inv, columns(s["gfar"], gain_row))
    x2 = jnp.concatenate([xn, xf], axis=0)
    mspans = [(a, min(512, moved - a)) for a in range(0, moved, 512)]
    send_m = s["send_m"]

    def both(core, a, n):
        w2 = jnp.concatenate([rows(net.chip, core, a, n), wm[core, pl.ds(a, n), :]], axis=1)
        return jnp.dot(w2, x2, preferred_element_type=F32)

    for a, n in mspans:
        send_m[pl.ds(a, n)] = both(1 - net.core, a, n).astype(BF)
        arrivals.append(net.put(send_m.at[pl.ds(a, n)], p_other.at[pl.ds(a, n)], net.sib))
    for a, n in mspans:
        own[pl.ds(a, n)] = both(net.core, a, n).astype(BF)
        store(a, n)
    for a, n in spans:
        y = product(net.chip, net.core, a, n) + got_a[net.chip, pl.ds(a, n)].astype(F32)
        own[pl.ds(moved + a, n)] = y.astype(BF)
        store(moved + a, n)
    for c in arrivals:
        c.wait_recv()


def output_kernel(p_own, p_other, h, kt, vt, logits, h_out, kt_out, vt_out, own, other, total, hb, kb, vb, in_sems, out_sems):
    small = [(h, hb, h_out), (kt, kb, kt_out), (vt, vb, vt_out)]
    spans = [pl.ds(a, min(OUT_ROWS, total.shape[0] - a)) for a in range(0, total.shape[0], OUT_ROWS)]
    ins = [[pltpu.make_async_copy(p.at[d], buf.at[d], in_sems.at[2 * n + m]) for m, (p, buf) in enumerate(((p_own, own), (p_other, other)))]
           for n, d in enumerate(spans)]
    ins += [[pltpu.make_async_copy(src, buf, in_sems.at[2 * len(spans) + n])] for n, (src, buf, dst) in enumerate(small)]
    outs = [pltpu.make_async_copy(total.at[d], logits.at[d], out_sems.at[n]) for n, d in enumerate(spans)]
    outs += [pltpu.make_async_copy(buf, dst, out_sems.at[len(spans) + n]) for n, (src, buf, dst) in enumerate(small)]
    for group in ins:
        for c in group:
            c.start()
    for n, d in enumerate(spans):
        for c in ins[n]:
            c.wait()
        total[d] = own[d].astype(F32) + other[d].astype(F32)
        outs[n].start()
    for n in range(len(small)):
        ins[len(spans) + n][0].wait()
        outs[len(spans) + n].start()
    for c in outs:
        c.wait()


def scratch(layers, blk, batch, k_o, f_loc, n_qkv, v_loc, width, heads, dh, cache_len):
    r = f_loc // 4
    moved = sum(WINDOWS)
    left = v_loc - moved
    t = {}
    for l in range(layers + 1):
        t[f"hx_a{l}"] = ((2 if l == layers else 1, 2, blk, batch), BF)
        t[f"ssq_a{l}"] = ((8, 1, batch), F32)
    for l in range(layers):
        t.update({
            f"wqkv{l}": ((3, 2 * blk, n_qkv), BF), f"wo{l}": ((k_o, 2 * blk), BF),
            f"win{l}": ((2 * blk, f_loc), BF), f"wout{l}": ((f_loc, 2 * blk), BF),
            f"qkv_part{l}": ((3, 4, width, batch), BF), f"qkv_got{l}": ((3, 2, width, batch), BF),
            f"qkv_out{l}": ((3, width, batch), BF), f"qkv_back{l}": ((3, width, batch), BF),
            f"o{l}": ((4, width, batch), BF),
            f"ypart1{l}": ((blk, batch), BF), f"ygot1{l}": ((blk, batch), BF),
            f"hx_m{l}": ((1, 2, blk, batch), BF), f"ssq_m{l}": ((8, 1, batch), F32),
            f"upart{l}": ((4, r, batch), BF), f"ugot{l}": ((2, r, batch), BF),
            f"uout{l}": ((r, batch), BF), f"uback{l}": ((r, batch), BF), f"u{l}": ((4, r, batch), BF),
            f"ypart2{l}": ((blk, batch), BF), f"ygot2{l}": ((blk, batch), BF),
        })
    t.update({
        "gx": ((2, 8, blk), F32), "gfar": ((2, 8, blk), F32),
        "q": ((batch, width), F32), "k": ((batch, width), F32), "v": ((batch, width), F32), "att": ((batch, width), F32),
        "kbuf": ((SLOTS, SEQ_STEP, heads, dh, cache_len), BF), "vbuf": ((SLOTS, SEQ_STEP, heads, dh, cache_len), BF),
        "pbuf": ((SEQ_STEP // 8, 16, cache_len), BF), "pnew": ((SEQ_STEP // 8, 16, width), F32),
        "wu": ((4 * v_loc, 2 * blk), BF), "wm": ((2, moved, 2 * blk), BF),
        "send_a": ((2, left, batch), BF), "got_a": ((2, left, batch), BF),
        "send_b": ((left, batch), BF), "send_m": ((moved, batch), BF), "own": ((v_loc, batch), BF),
        "kt": ((layers, width, batch), BF), "vt": ((layers, width, batch), BF), "h": ((batch, blk), BF),
    })
    return t


def sds(shape, dtype):
    return jax.ShapeDtypeStruct(shape, dtype)


def solution(mesh):
    def decode_step(h_loc, seq_lens, k_cache, v_cache, g_attn, w_q, w_k, w_v, w_o, g_mlp, w_in, w_out, g_final, w_unemb):
        batch, blk = h_loc.shape
        layers = w_q.shape[0]
        heads, dh, cache_len = k_cache.shape[2], k_cache.shape[4], k_cache.shape[3]
        v_loc = w_unemb.shape[1] // 4
        width = heads * dh
        kc = jnp.swapaxes(k_cache, 3, 4)
        vc = jnp.swapaxes(v_cache, 3, 4)
        names = scratch(layers, blk, batch, w_o.shape[1], w_in.shape[2], w_q.shape[2], v_loc, width, heads, dh, cache_len)
        h_out, p_own, p_other, kt, vt = pl.pallas_call(
            functools.partial(kernel, tuple(names), 8 * blk),
            name="decode",
            out_shape=[sds((batch, blk), BF), sds((v_loc, batch), BF), sds((v_loc, batch), BF)] + [sds((layers, width, batch), BF)] * 2,
            in_specs=[VM, pl.BlockSpec(memory_space=pltpu.SMEM), ANY, ANY, VM, VM, VM] + [ANY] * 7,
            out_specs=[ANY] * 5,
            scratch_shapes=[pltpu.VMEM(shape, dtype) for shape, dtype in names.values()] + [
                pltpu.SemaphoreType.DMA((SLOTS, 2)),
                pltpu.SemaphoreType.DMA((COPIES,)), pltpu.SemaphoreType.DMA((COPIES,)), pltpu.SemaphoreType.DMA((40,))],
            compiler_params=pltpu.CompilerParams(collective_id=0, has_side_effects=True, vmem_limit_bytes=67043328),
        )(h_loc, seq_lens, kc, vc, g_attn, g_mlp, g_final[None], w_q, w_k, w_v, w_o, w_in, w_out, w_unemb.T)

        parts = -(-v_loc // OUT_ROWS)
        logits_t, h_out, kt, vt = pl.pallas_call(
            output_kernel,
            name="outputs",
            out_shape=[sds((v_loc, batch), F32), sds(h_out.shape, BF), sds(kt.shape, BF), sds(vt.shape, BF)],
            in_specs=[ANY] * 5,
            out_specs=[ANY] * 4,
            scratch_shapes=[pltpu.VMEM((v_loc, batch), BF), pltpu.VMEM((v_loc, batch), BF), pltpu.VMEM((v_loc, batch), F32),
                            pltpu.VMEM(h_out.shape, BF), pltpu.VMEM(kt.shape, BF), pltpu.VMEM(vt.shape, BF),
                            pltpu.SemaphoreType.DMA((2 * parts + 3,)), pltpu.SemaphoreType.DMA((parts + 3,))],
            compiler_params=pltpu.CompilerParams(vmem_limit_bytes=56 * 2**20),
        )(p_own, p_other, h_out, kt, vt)

        def entries(t):
            return jnp.transpose(t.reshape(layers, heads, dh, batch), (0, 3, 1, 2))

        return h_out, logits_t.T, entries(kt), entries(vt)

    emb_spec = P('dp', ('x', 'yz'))
    gain_spec = P(None, ('x', 'yz'))
    cache_spec = P(None, 'dp', ('yz', 'x'), None, None)
    in_rows = P(None, 'x', 'yz')
    out_rows = P(None, 'yz', 'x')
    new_spec = P(None, 'dp', ('yz', 'x'), None)
    in_specs = (emb_spec, P('dp'), cache_spec, cache_spec, gain_spec, in_rows, in_rows, in_rows, out_rows, gain_spec, in_rows, out_rows, P(('x', 'yz')), P('x', 'yz'))
    out_specs = (emb_spec, P('dp', ('yz', 'x')), new_spec, new_spec)
    return jax.shard_map(decode_step, mesh=mesh, in_specs=in_specs, out_specs=out_specs, check_vma=False)
```

```python
import functools

import jax
import jax.numpy as jnp
from jax import lax
from jax.experimental import pallas as pl
from jax.experimental.pallas import tpu as pltpu
from jax.sharding import PartitionSpec as P

NORM_EPS = 1e-6
MESH = pl.DeviceIdType.MESH
BF = jnp.bfloat16
F32 = jnp.float32
ANY = pl.BlockSpec(memory_space=pl.ANY)
VM = pl.BlockSpec(memory_space=pltpu.VMEM)
SEQ_STEP = 16
SLOTS = 5
HALVES = 2
PARTS = 4
MOVED = 3168
PIECE = 96
COPIES = 250
OUT_ROWS = 512


def tdot(w, act):
    return lax.dot_general(w, act, (((0,), (0,)), ((), ())), preferred_element_type=F32)


class Attention:
    def __init__(self, lens_ref, kc_ref, vc_ref, q_ref, k_ref, v_ref, o_ref, kbuf, vbuf, pbuf, pnew, sems):
        self.lens, self.kc, self.vc = lens_ref, kc_ref, vc_ref
        self.q, self.k, self.v, self.o = q_ref, k_ref, v_ref, o_ref
        self.kbuf, self.vbuf, self.pbuf, self.pnew, self.sems = kbuf, vbuf, pbuf, pnew, sems
        self.layers = kc_ref.shape[0]
        self.batch, self.width = q_ref.shape
        self.dh, self.cache_len = kc_ref.shape[3], kc_ref.shape[4]
        self.steps = self.batch // SEQ_STEP
        self.groups = range(SEQ_STEP // 8)
        self.row = lax.broadcasted_iota(jnp.int32, (16, self.width), 0) % 8
        self.pos = lax.broadcasted_iota(jnp.int32, (16, self.cache_len), 1)
        self.row8 = lax.broadcasted_iota(jnp.int32, (8, self.width), 0)
        self.first_head = lax.broadcasted_iota(jnp.int32, (8, self.width), 1) < self.dh

    def copy(self, g, n):
        slot = lax.rem(g, SLOTS)
        src, buf = ((self.kc, self.kbuf), (self.vc, self.vbuf))[n]
        block = src.at[g // self.steps, pl.ds(lax.rem(g, self.steps) * SEQ_STEP, SEQ_STEP)]
        return pltpu.make_async_copy(block, buf.at[slot], self.sems.at[slot, n])

    def issue(self, g):
        for n in range(2):
            self.copy(g, n).start()

    def start(self):
        for g in range(SLOTS):
            self.issue(jnp.int32(g))

    def base(self, step, g):
        return pl.multiple_of(step * SEQ_STEP + 8 * g, 8)

    def score(self, step, slot):
        q2s, scores = [], []
        for g in self.groups:
            q8 = self.q[pl.ds(self.base(step, g), 8), :]
            q2 = jnp.concatenate([jnp.where(self.first_head, q8, 0.0), jnp.where(self.first_head, 0.0, q8)], axis=0)
            qbd = jnp.concatenate([jnp.where(self.row == n, q2, 0.0) for n in range(8)], axis=1).astype(BF)
            kb = self.kbuf[slot, 8 * g:8 * g + 8].reshape(8 * self.width, self.cache_len)
            scores.append(jnp.dot(qbd, kb, preferred_element_type=F32))
            q2s.append(q2)
        return q2s, scores

    def softmax(self, step, q2s, scores):
        for g in self.groups:
            k8 = self.k[pl.ds(self.base(step, g), 8), :]
            k2 = jnp.concatenate([k8, k8], axis=0)
            s_new = jnp.sum(q2s[g] * k2, axis=1, keepdims=True) * (self.dh ** -0.5)
            lens8 = jnp.zeros((8, self.width), jnp.int32)
            for n in range(8):
                lens8 = jnp.where(self.row8 == n, self.lens[self.base(step, g) + n], lens8)
            lens16 = jnp.concatenate([lens8, lens8], axis=0)
            lens_full = jnp.concatenate([lens16] * (self.cache_len // self.width), axis=1)
            s = jnp.where(self.pos < lens_full, scores[g] * (self.dh ** -0.5), -1e30)
            top = jnp.maximum(jnp.max(s, axis=1, keepdims=True), s_new)
            e = jnp.exp(s - top)
            e_new = jnp.exp(s_new - top)
            inv = 1.0 / (jnp.sum(e, axis=1, keepdims=True) + e_new)
            self.pbuf[g] = (e * inv).astype(BF)
            self.pnew[g] = jnp.broadcast_to((e_new * inv).astype(BF).astype(F32), (16, self.width))

    def mix(self, step, slot):
        w = self.width
        for g in self.groups:
            vb = self.vbuf[slot, 8 * g:8 * g + 8].reshape(8 * w, self.cache_len)
            mixed = lax.dot_general(self.pbuf[g], vb, (((1,), (1,)), ((), ())), preferred_element_type=F32)
            o2 = jnp.zeros((16, w), F32)
            for n in range(8):
                o2 = jnp.where(self.row == n, mixed[:, n * w:(n + 1) * w], o2)
            v8 = self.v[pl.ds(self.base(step, g), 8), :]
            o2 = o2 + self.pnew[g] * jnp.concatenate([v8, v8], axis=0)
            self.o[pl.ds(self.base(step, g), 8), :] = jnp.where(self.first_head, o2[:8], o2[8:])

    def fetched(self, g, n):
        self.copy(g, n).wait()
        return lax.rem(g, SLOTS)

    def refill(self, g):
        nxt = g - 2 + SLOTS

        @pl.when((g >= 2) & (nxt < self.layers * self.steps))
        def _():
            self.issue(nxt)

    def piece(self, layer, half, n, count):
        first = layer * self.steps
        per = self.steps // HALVES
        lo = half * per
        begin, end = lo + n * per // count, lo + (n + 1) * per // count

        def body(step, carry):
            self.refill(first + step)
            k_slot = self.fetched(first + step, 0)
            v_slot = self.fetched(first + step - 1, 1)
            q2s, scores = self.score(step, k_slot)
            self.mix(step - 1, v_slot)
            self.softmax(step, q2s, scores)
            return carry

        if n == 0:
            self.refill(jnp.int32(first + begin))
            self.softmax(begin, *self.score(begin, self.fetched(jnp.int32(first + begin), 0)))
            begin += 1
        lax.fori_loop(begin, end, body, 0)
        if n == count - 1:
            self.mix(end - 1, self.fetched(jnp.int32(first + end - 1), 1))


class Message:
    def __init__(self, copy, arrives):
        self.copy, self.arrives = copy, arrives

    def wait_recv(self):
        self.copy.wait_recv()


class Net:
    def __init__(self, send, recv, local):
        self.i = lax.axis_index("x")
        self.j = lax.axis_index("yz")
        self.chip = self.i // 2
        self.core = lax.rem(self.i, 2)
        self.sib = {"x": 2 * self.chip + 1 - self.core}
        self.across = {"x": lax.rem(self.i + 2, 4)}
        self.yother = {"yz": 1 - self.j}
        self.send, self.recv, self.local = send, recv, local
        self.n = 0
        self.m = 0
        self.sent = []
        self.now = 0.0
        self.free = {"x": 0.0, "y": 0.0, "d": 0.0}

    def greet(self):
        self.barrier = pltpu.get_barrier_semaphore()
        for dx in range(4):
            for dy in range(2):
                if dx or dy:
                    pl.semaphore_signal(self.barrier, inc=1, device_id=self.peer(dx, dy), device_id_type=MESH)

    def met(self):
        pl.semaphore_wait(self.barrier, 7)

    def peer(self, dx, dy):
        return {"x": lax.rem(self.i + dx, 4), "yz": lax.rem(self.j + dy, 2)}

    def put(self, src, dst, to):
        c = pltpu.make_async_remote_copy(
            src_ref=src, dst_ref=dst, send_sem=self.send.at[self.n], recv_sem=self.recv.at[self.n],
            device_id=to, device_id_type=MESH)
        self.n += 1
        c.start()
        self.sent.append(c)
        size = src.dtype.itemsize
        for d in src.shape:
            size *= d
        if to is self.sib:
            link, rate, latency = "d", 600e3, 1.0
        elif to is self.yother:
            link, rate, latency = "y", 46e3, 1.8
        else:
            link, rate, latency = "x", 46e3, 1.8
        begin = max(self.now, self.free[link])
        self.free[link] = begin + size / rate
        return Message(c, self.free[link] + latency)

    def fetch(self, src, dst):
        c = pltpu.make_async_copy(src, dst, self.local.at[self.m])
        self.m += 1
        c.start()
        return c

    def finish(self):
        for c in self.sent:
            c.wait_send()


def interleave(net, chains, fill):
    state = []
    for c in chains:
        state.append([net.now, 0.0, [], c, None])
    turn = 0
    while state:
        best = min((e for e in state if e[4] in (None, turn)), key=lambda e: (max(net.now, e[0]), e[0]))
        turn += best[4] is not None
        begin = max(net.now, best[0])
        fill(begin + best[1])
        for m in best[2]:
            m.wait_recv()
        net.now = begin + best[1]
        try:
            best[2], best[1], *tail = next(best[3])
            best[4] = tail[0] if tail else None
            best[0] = max([net.now] + [m.arrives for m in best[2]])
        except StopIteration:
            state.remove(best)


def slot_of(d):
    return 2 * (d % 2) + d // 2


def rs_first(net, part, got):
    return net.put(part.at[pl.ds(2 * (1 - net.core), 2)], got, net.sib)


def rs_second(net, part, got, out, back):
    far = 1 - net.chip
    out[...] = (part[2 * net.core + far].astype(F32) + got[far].astype(F32)).astype(BF)
    return net.put(out, back, net.across)


def rs_last(net, part, got, back):
    return part[2 * net.core + net.chip].astype(F32) + got[net.chip].astype(F32) + back[...].astype(F32)


def gather_x(net, buf):
    me = buf.at[net.i]
    across = net.put(me, me, net.across)
    sib = net.put(me, me, net.sib)
    return sib, across


def gather_forward(net, buf):
    far = buf.at[lax.rem(net.i + 2, 4)]
    return net.put(far, far, net.sib)


def send_half(net, w, act, part, got):
    r = got.shape[0]
    part[...] = tdot(w[:, pl.ds(pl.multiple_of((1 - net.j) * r, r), r)], act).astype(BF)
    return net.put(part, got, net.yother)


def own_half(net, w, act, r):
    return tdot(w[:, pl.ds(pl.multiple_of(net.j * r, r), r)], act)


def norm_send(net, h_own, hx, ssq, far=False):
    hf = h_own.astype(F32)
    me = 2 * net.i + net.j
    hx[0, net.j] = h_own
    ssq[me] = jnp.sum(hf * hf, axis=0, keepdims=True)
    mine = hx.at[0, net.j]
    stats = []
    for dx in range(4):
        for dy in range(2):
            if dx or dy:
                stats.append(net.put(ssq.at[me], ssq.at[me], net.peer(dx, dy)))
    near = net.put(mine, hx.at[0, net.j], net.yother)
    fars = [net.put(mine, hx.at[1, net.j], to) for to in (net.across, net.peer(2, 1))] if far else []
    return stats, near, fars


def norm_scale(ssq, model_dim):
    total = ssq[0]
    for n in range(1, 8):
        total = total + ssq[n]
    return lax.rsqrt(total / model_dim + NORM_EPS)


def normed(hx, inv, gain):
    rows = hx.shape[0] * hx.shape[1]
    return (hx[...].reshape(rows, hx.shape[2]).astype(F32) * inv * gain).astype(BF)


def columns(gx, n):
    return jnp.concatenate([gx[0].T[:, n:n + 1], gx[1].T[:, n:n + 1]], axis=0)


def kernel(names, model_dim, h_ref, lens_ref, kc, vc, ga, gm, gf, wq, wk, wv, wo, win, wout, wu, h_out, p_own, p_other, kt_out, vt_out, *rest):
    s = dict(zip(names, rest))
    kv_sems, send, recv, local = rest[len(names):]
    layers = wq.shape[0]
    net = Net(send, recv, local)
    net.greet()
    mats = (("wo", wo), ("win", win), ("wout", wout))
    loads = {("wqkv", 0): [net.fetch(w.at[0], s["wqkv0"].at[n]) for n, w in enumerate((wq, wk, wv))]}
    att = Attention(lens_ref, kc, vc, s["q"], s["k"], s["v"], s["att"], s["kbuf"], s["vbuf"], s["pbuf"], s["pnew"], kv_sems)
    for l in range(layers):
        if l:
            loads["wqkv", l] = [net.fetch(w.at[l], s[f"wqkv{l}"].at[n]) for n, w in enumerate((wq, wk, wv))]
        for name, w in mats:
            loads[name, l] = [net.fetch(w.at[l], s[f"{name}{l}"])]
    att.start()

    v_loc = p_own.shape[0]
    early = []
    far_chip = 1 - net.chip

    def cross():
        core, a = len(early) % 2, len(early) // 2 * PIECE
        src = wu.at[pl.ds(pl.multiple_of((2 * far_chip + core) * v_loc + a, 16), PIECE)]
        early.append(net.put(src, s["wm"].at[core, pl.ds(a, PIECE)], net.across))

    cost = PIECE * 512 / 46e3

    def fill(until):
        while len(early) < 2 * MOVED // PIECE and net.free["x"] + cost <= until:
            net.free["x"] = max(net.free["x"], net.now)
            if net.free["x"] + cost > until:
                break
            cross()

    gx, gfar = s["gx"], s["gfar"]
    for n, g in enumerate((ga, gm, gf)):
        gx[net.j, pl.ds(n * layers, g.shape[0])] = g[...].astype(F32)
    rest_rows = gx.shape[1] - 2 * layers - 1
    gx[net.j, pl.ds(2 * layers + 1, rest_rows)] = jnp.zeros((rest_rows, gx.shape[2]), F32)
    h_in = h_ref[...].astype(F32).T.astype(BF)
    net.met()
    g_near = net.put(gx.at[net.j], gx.at[net.j], net.yother)
    g_fars = []
    stores = []
    h_last = [None] * HALVES
    final = []
    hb = s["ssq_a00"].shape[2]
    blk = h_in.shape[0]
    width = s["q"].shape[1]
    waited = {}

    def once(name, l):
        if (name, l) not in waited:
            for c in loads[name, l]:
                c.wait()
            waited[name, l] = s[f"{name}{l}"]
        return waited[name, l]

    def chain(h):
        lanes = slice(h * hb, (h + 1) * hb)
        seqs = pl.ds(h * hb, hb)
        h_own = h_in[:, lanes]
        stats, near, _ = norm_send(net, h_own, s[f"hx_a0{h}"], s[f"ssq_a0{h}"])
        head = [g_near] if h == 0 else []
        if h == 0:
            g_fars.extend([net.put(gx.at[net.j], gfar.at[net.j], to) for to in (net.across, net.peer(2, 1))])
        for l in range(layers):
            sl = {k[:-2]: s[k] for k in s if k.endswith(f"{l}{h}")}
            yield stats + [near] + head, 0.9
            head = []
            inv = norm_scale(sl["ssq_a"], model_dim)
            xn = normed(sl["hx_a"].at[0], inv, columns(gx, l))
            w = once("wqkv", l)
            part, got, back = sl["qkv_part"], sl["qkv_got"], sl["qkv_back"]
            for n in range(3):
                y = tdot(w[n], xn).astype(BF)
                for d in range(4):
                    part[slot_of(d), n * width:(n + 1) * width] = y[d * width:(d + 1) * width]
            first = rs_first(net, part, got)
            yield [first], 0.2
            second = rs_second(net, part, got, sl["qkv_out"], back)
            yield [second], 0.3
            y = rs_last(net, part, got, back).astype(BF)
            for n, dst in enumerate(("kt", "vt")):
                s[dst][l, :, seqs] = y[(n + 1) * width:(n + 2) * width]
            for n, dst in enumerate((kt_out, vt_out)):
                src = s[("kt", "vt")[n]]
                stores.append(net.fetch(src.at[l, :, seqs], dst.at[l, :, seqs]))
            for n, dst in enumerate(("q", "k", "v")):
                s[dst][seqs, :] = y[n * width:(n + 1) * width].astype(F32).T
            for n in range(PARTS):
                yield [], 17.0 / HALVES / PARTS + 0.2, (l * HALVES + h) * PARTS + n
                att.piece(l, h, n, PARTS)
            if l == layers - 1 and h == 0:
                loads["wu", 0] = [net.fetch(wu, s["wu"])]
            o = sl["o"]
            o[net.i] = s["att"][seqs, :].T.astype(BF)
            sib, across = gather_x(net, o)
            yield [across], 0.1
            fwd = gather_forward(net, o)
            yield [sib, fwd], 0.4
            w = once("wo", l)
            act = o[...].reshape(-1, hb)
            summed = send_half(net, w, act, sl["ypart1"], sl["ygot1"])
            mine = own_half(net, w, act, blk)
            yield [summed], 0.3
            h_own = (h_own.astype(F32) + (mine + sl["ygot1"][...].astype(F32))).astype(BF)
            stats, near, _ = norm_send(net, h_own, sl["hx_m"], sl["ssq_m"])
            yield stats + [near], 0.7
            w = once("win", l)
            inv = norm_scale(sl["ssq_m"], model_dim)
            xn = normed(sl["hx_m"].at[0], inv, columns(gx, layers + l))
            r = w.shape[1] // 4
            y = tdot(w[...], xn).astype(BF)
            part, got, back = sl["upart"], sl["ugot"], sl["uback"]
            for d in range(4):
                part[slot_of(d)] = y[d * r:(d + 1) * r]
            first = rs_first(net, part, got)
            yield [first], 0.2
            second = rs_second(net, part, got, sl["uout"], back)
            yield [second], 0.4
            up = rs_last(net, part, got, back).astype(BF)
            u = sl["u"]
            u[net.i] = jax.nn.gelu(up.astype(F32)).astype(BF)
            sib, across = gather_x(net, u)
            yield [across], 0.1
            fwd = gather_forward(net, u)
            yield [sib, fwd], 0.5
            w = once("wout", l)
            act = u[...].reshape(-1, hb)
            summed = send_half(net, w, act, sl["ypart2"], sl["ygot2"])
            mine = own_half(net, w, act, blk)
            yield [summed], 0.3
            h_own = (h_own.astype(F32) + (mine + sl["ygot2"][...].astype(F32))).astype(BF)
            stats, near, fars = norm_send(net, h_own, s[f"hx_a{l + 1}{h}"], s[f"ssq_a{l + 1}{h}"], far=l == layers - 1)
        s["h"][seqs, :] = h_own.astype(F32).T.astype(BF)
        final.append((stats + [near], fars))

    interleave(net, [chain(h) for h in range(HALVES)], fill)
    while len(early) < 2 * MOVED // PIECE:
        cross()
    stores.append(net.fetch(s["h"], h_out))
    waits = [m for f in final for m in f[0]]
    fars = [m for f in final for m in f[1]]
    unembed(net, s, model_dim, layers, waits, fars + g_fars + early, loads["wu", 0][0], p_own, p_other, stores)
    for c in stores:
        c.wait()
    net.finish()


def unembed(net, s, model_dim, layers, waits, late, wu_load, p_own, p_other, stores):
    v_loc = p_own.shape[0]
    moved = MOVED
    left = v_loc - moved
    wu, wm, own = s["wu"], s["wm"], s["own"]
    for c in waits:
        c.wait_recv()

    def acts(side, gains):
        return jnp.concatenate(
            [normed(s[f"hx_a{layers}{h}"].at[side], norm_scale(s[f"ssq_a{layers}{h}"], model_dim), columns(gains, 2 * layers))
             for h in range(HALVES)], axis=1)

    xn = acts(0, s["gx"])
    wu_load.wait()
    far_chip = 1 - net.chip
    send_a, got_a, send_b = s["send_a"], s["got_a"], s["send_b"]

    def rows(chip, core, a, n):
        return wu[pl.ds(pl.multiple_of((2 * chip + core) * v_loc + a, 16), n), :]

    def product(chip, core, a, n):
        return jnp.dot(rows(chip, core, moved + a, n), xn, preferred_element_type=F32)

    spans = [(a, min(512, left - a)) for a in range(0, left, 512)]
    first, arrivals = [], []

    def stage1(a, n):
        for chip in range(2):
            send_a[chip, pl.ds(a, n)] = product(chip, 1 - net.core, a, n).astype(BF)
        first.append(net.put(send_a.at[:, pl.ds(a, n)], got_a.at[:, pl.ds(a, n)], net.sib))

    def stage2(r, a, n):
        y = product(far_chip, net.core, a, n)
        first[r].wait_recv()
        send_b[pl.ds(a, n)] = (y + got_a[far_chip, pl.ds(a, n)].astype(F32)).astype(BF)
        arrivals.append(net.put(send_b.at[pl.ds(a, n)], p_other.at[pl.ds(moved + a, n)], net.across))

    stage1(*spans[0])
    for r in range(len(spans)):
        if r + 1 < len(spans):
            stage1(*spans[r + 1])
        stage2(r, *spans[r])

    def store(a, n):
        stores.append(net.fetch(own.at[pl.ds(a, n)], p_own.at[pl.ds(a, n)]))

    for c in late:
        c.wait_recv()
    xf = acts(1, s["gfar"])
    x2 = jnp.concatenate([xn, xf], axis=0)
    mspans = [(a, min(512, moved - a)) for a in range(0, moved, 512)]
    send_m = s["send_m"]

    def both(core, a, n):
        w2 = jnp.concatenate([rows(net.chip, core, a, n), wm[core, pl.ds(a, n), :]], axis=1)
        return jnp.dot(w2, x2, preferred_element_type=F32)

    for a, n in mspans:
        send_m[pl.ds(a, n)] = both(1 - net.core, a, n).astype(BF)
        arrivals.append(net.put(send_m.at[pl.ds(a, n)], p_other.at[pl.ds(a, n)], net.sib))
    for a, n in mspans:
        own[pl.ds(a, n)] = both(net.core, a, n).astype(BF)
        store(a, n)
    for a, n in spans:
        y = product(net.chip, net.core, a, n) + got_a[net.chip, pl.ds(a, n)].astype(F32)
        own[pl.ds(moved + a, n)] = y.astype(BF)
        store(moved + a, n)
    for c in arrivals:
        c.wait_recv()


def output_kernel(p_own, p_other, h, kt, vt, logits, h_out, kt_out, vt_out, own, other, total, hb, kb, vb, in_sems, out_sems):
    small = [(h, hb, h_out), (kt, kb, kt_out), (vt, vb, vt_out)]
    spans = [pl.ds(a, min(OUT_ROWS, total.shape[0] - a)) for a in range(0, total.shape[0], OUT_ROWS)]
    ins = [[pltpu.make_async_copy(p.at[d], buf.at[d], in_sems.at[2 * n + m]) for m, (p, buf) in enumerate(((p_own, own), (p_other, other)))]
           for n, d in enumerate(spans)]
    ins += [[pltpu.make_async_copy(src, buf, in_sems.at[2 * len(spans) + n])] for n, (src, buf, dst) in enumerate(small)]
    outs = [pltpu.make_async_copy(total.at[d], logits.at[d], out_sems.at[n]) for n, d in enumerate(spans)]
    outs += [pltpu.make_async_copy(buf, dst, out_sems.at[len(spans) + n]) for n, (src, buf, dst) in enumerate(small)]
    for group in ins:
        for c in group:
            c.start()
    for n, d in enumerate(spans):
        for c in ins[n]:
            c.wait()
        total[d] = own[d].astype(F32) + other[d].astype(F32)
        outs[n].start()
    for n in range(len(small)):
        ins[len(spans) + n][0].wait()
        outs[len(spans) + n].start()
    for c in outs:
        c.wait()


def scratch(layers, blk, batch, k_o, f_loc, n_qkv, v_loc, width, heads, dh, cache_len):
    r = f_loc // 4
    moved = MOVED
    left = v_loc - moved
    t = {}
    hb = batch // HALVES
    for l in range(layers):
        t.update({
            f"wqkv{l}": ((3, 2 * blk, n_qkv), BF), f"wo{l}": ((k_o, 2 * blk), BF),
            f"win{l}": ((2 * blk, f_loc), BF), f"wout{l}": ((f_loc, 2 * blk), BF)})
    for h in range(HALVES):
        for l in range(layers + 1):
            t[f"hx_a{l}{h}"] = ((2 if l == layers else 1, 2, blk, hb), BF)
            t[f"ssq_a{l}{h}"] = ((8, 1, hb), F32)
        for l in range(layers):
            e = f"{l}{h}"
            t.update({
                "qkv_part" + e: ((4, 3 * width, hb), BF), "qkv_got" + e: ((2, 3 * width, hb), BF),
                "qkv_out" + e: ((3 * width, hb), BF), "qkv_back" + e: ((3 * width, hb), BF),
                "o" + e: ((4, width, hb), BF),
                "ypart1" + e: ((blk, hb), BF), "ygot1" + e: ((blk, hb), BF),
                "hx_m" + e: ((1, 2, blk, hb), BF), "ssq_m" + e: ((8, 1, hb), F32),
                "upart" + e: ((4, r, hb), BF), "ugot" + e: ((2, r, hb), BF),
                "uout" + e: ((r, hb), BF), "uback" + e: ((r, hb), BF), "u" + e: ((4, r, hb), BF),
                "ypart2" + e: ((blk, hb), BF), "ygot2" + e: ((blk, hb), BF),
            })
    t.update({
        "gx": ((2, 8, blk), F32), "gfar": ((2, 8, blk), F32),
        "q": ((batch, width), F32), "k": ((batch, width), F32), "v": ((batch, width), F32), "att": ((batch, width), F32),
        "kbuf": ((SLOTS, SEQ_STEP, heads, dh, cache_len), BF), "vbuf": ((SLOTS, SEQ_STEP, heads, dh, cache_len), BF),
        "pbuf": ((SEQ_STEP // 8, 16, cache_len), BF), "pnew": ((SEQ_STEP // 8, 16, width), F32),
        "wu": ((4 * v_loc, 2 * blk), BF), "wm": ((2, moved, 2 * blk), BF),
        "send_a": ((2, left, batch), BF), "got_a": ((2, left, batch), BF),
        "send_b": ((left, batch), BF), "send_m": ((moved, batch), BF), "own": ((v_loc, batch), BF),
        "kt": ((layers, width, batch), BF), "vt": ((layers, width, batch), BF), "h": ((batch, blk), BF),
    })
    return t


def sds(shape, dtype):
    return jax.ShapeDtypeStruct(shape, dtype)


def solution(mesh):
    def decode_step(h_loc, seq_lens, k_cache, v_cache, g_attn, w_q, w_k, w_v, w_o, g_mlp, w_in, w_out, g_final, w_unemb):
        batch, blk = h_loc.shape
        layers = w_q.shape[0]
        heads, dh, cache_len = k_cache.shape[2], k_cache.shape[4], k_cache.shape[3]
        v_loc = w_unemb.shape[1] // 4
        width = heads * dh
        kc = jnp.swapaxes(k_cache, 3, 4)
        vc = jnp.swapaxes(v_cache, 3, 4)
        names = scratch(layers, blk, batch, w_o.shape[1], w_in.shape[2], w_q.shape[2], v_loc, width, heads, dh, cache_len)
        h_out, p_own, p_other, kt, vt = pl.pallas_call(
            functools.partial(kernel, tuple(names), 8 * blk),
            name="decode",
            out_shape=[sds((batch, blk), BF), sds((v_loc, batch), BF), sds((v_loc, batch), BF)] + [sds((layers, width, batch), BF)] * 2,
            in_specs=[VM, pl.BlockSpec(memory_space=pltpu.SMEM), ANY, ANY, VM, VM, VM] + [ANY] * 7,
            out_specs=[ANY] * 5,
            scratch_shapes=[pltpu.VMEM(shape, dtype) for shape, dtype in names.values()] + [
                pltpu.SemaphoreType.DMA((SLOTS, 2)),
                pltpu.SemaphoreType.DMA((COPIES,)), pltpu.SemaphoreType.DMA((COPIES,)), pltpu.SemaphoreType.DMA((40,))],
            compiler_params=pltpu.CompilerParams(collective_id=0, has_side_effects=True, vmem_limit_bytes=67043328),
        )(h_loc, seq_lens, kc, vc, g_attn, g_mlp, g_final[None], w_q, w_k, w_v, w_o, w_in, w_out, w_unemb.T)

        parts = -(-v_loc // OUT_ROWS)
        logits_t, h_out, kt, vt = pl.pallas_call(
            output_kernel,
            name="outputs",
            out_shape=[sds((v_loc, batch), F32), sds(h_out.shape, BF), sds(kt.shape, BF), sds(vt.shape, BF)],
            in_specs=[ANY] * 5,
            out_specs=[ANY] * 4,
            scratch_shapes=[pltpu.VMEM((v_loc, batch), BF), pltpu.VMEM((v_loc, batch), BF), pltpu.VMEM((v_loc, batch), F32),
                            pltpu.VMEM(h_out.shape, BF), pltpu.VMEM(kt.shape, BF), pltpu.VMEM(vt.shape, BF),
                            pltpu.SemaphoreType.DMA((2 * parts + 3,)), pltpu.SemaphoreType.DMA((parts + 3,))],
            compiler_params=pltpu.CompilerParams(vmem_limit_bytes=56 * 2**20),
        )(p_own, p_other, h_out, kt, vt)

        def entries(t):
            return jnp.transpose(t.reshape(layers, heads, dh, batch), (0, 3, 1, 2))

        return h_out, logits_t.T, entries(kt), entries(vt)

    emb_spec = P('dp', ('x', 'yz'))
    gain_spec = P(None, ('x', 'yz'))
    cache_spec = P(None, 'dp', ('yz', 'x'), None, None)
    in_rows = P(None, 'x', 'yz')
    out_rows = P(None, 'yz', 'x')
    new_spec = P(None, 'dp', ('yz', 'x'), None)
    in_specs = (emb_spec, P('dp'), cache_spec, cache_spec, gain_spec, in_rows, in_rows, in_rows, out_rows, gain_spec, in_rows, out_rows, P(('x', 'yz')), P('x', 'yz'))
    out_specs = (emb_spec, P('dp', ('yz', 'x')), new_spec, new_spec)
    return jax.shard_map(decode_step, mesh=mesh, in_specs=in_specs, out_specs=out_specs, check_vma=False)
```

```python
import functools

import jax
import jax.numpy as jnp
from jax import lax
from jax.experimental import pallas as pl
from jax.experimental.pallas import tpu as pltpu
from jax.sharding import PartitionSpec as P

NORM_EPS = 1e-6
MESH = pl.DeviceIdType.MESH
BF = jnp.bfloat16
F32 = jnp.float32
ANY = pl.BlockSpec(memory_space=pl.ANY)
VM = pl.BlockSpec(memory_space=pltpu.VMEM)
SEQ_STEP = 16
SLOTS = 5
HALVES = 2
PARTS = 4
MOVED = 3024
PIECE = 48
SLACK = 0.3
COPIES = 300
OUT_ROWS = 512


def tdot(w, act):
    return lax.dot_general(w, act, (((0,), (0,)), ((), ())), preferred_element_type=F32)


class Attention:
    def __init__(self, lens_ref, kc_ref, vc_ref, q_ref, k_ref, v_ref, o_ref, kbuf, vbuf, pbuf, pnew, sems):
        self.lens, self.kc, self.vc = lens_ref, kc_ref, vc_ref
        self.q, self.k, self.v, self.o = q_ref, k_ref, v_ref, o_ref
        self.kbuf, self.vbuf, self.pbuf, self.pnew, self.sems = kbuf, vbuf, pbuf, pnew, sems
        self.layers = kc_ref.shape[0]
        self.batch, self.width = q_ref.shape
        self.dh, self.cache_len = kc_ref.shape[3], kc_ref.shape[4]
        self.steps = self.batch // SEQ_STEP
        self.groups = range(SEQ_STEP // 8)
        self.row = lax.broadcasted_iota(jnp.int32, (16, self.width), 0) % 8
        self.pos = lax.broadcasted_iota(jnp.int32, (16, self.cache_len), 1)
        self.row8 = lax.broadcasted_iota(jnp.int32, (8, self.width), 0)
        self.first_head = lax.broadcasted_iota(jnp.int32, (8, self.width), 1) < self.dh

    def copy(self, g, n):
        slot = lax.rem(g, SLOTS)
        src, buf = ((self.kc, self.kbuf), (self.vc, self.vbuf))[n]
        block = src.at[g // self.steps, pl.ds(lax.rem(g, self.steps) * SEQ_STEP, SEQ_STEP)]
        return pltpu.make_async_copy(block, buf.at[slot], self.sems.at[slot, n])

    def issue(self, g):
        for n in range(2):
            self.copy(g, n).start()

    def start(self):
        for g in range(SLOTS):
            self.issue(jnp.int32(g))

    def base(self, step, g):
        return pl.multiple_of(step * SEQ_STEP + 8 * g, 8)

    def score(self, step, slot):
        q2s, scores = [], []
        for g in self.groups:
            q8 = self.q[pl.ds(self.base(step, g), 8), :]
            q2 = jnp.concatenate([jnp.where(self.first_head, q8, 0.0), jnp.where(self.first_head, 0.0, q8)], axis=0)
            qbd = jnp.concatenate([jnp.where(self.row == n, q2, 0.0) for n in range(8)], axis=1).astype(BF)
            kb = self.kbuf[slot, 8 * g:8 * g + 8].reshape(8 * self.width, self.cache_len)
            scores.append(jnp.dot(qbd, kb, preferred_element_type=F32))
            q2s.append(q2)
        return q2s, scores

    def softmax(self, step, q2s, scores):
        for g in self.groups:
            k8 = self.k[pl.ds(self.base(step, g), 8), :]
            k2 = jnp.concatenate([k8, k8], axis=0)
            s_new = jnp.sum(q2s[g] * k2, axis=1, keepdims=True) * (self.dh ** -0.5)
            lens8 = jnp.zeros((8, self.width), jnp.int32)
            for n in range(8):
                lens8 = jnp.where(self.row8 == n, self.lens[self.base(step, g) + n], lens8)
            lens16 = jnp.concatenate([lens8, lens8], axis=0)
            lens_full = jnp.concatenate([lens16] * (self.cache_len // self.width), axis=1)
            s = jnp.where(self.pos < lens_full, scores[g] * (self.dh ** -0.5), -1e30)
            top = jnp.maximum(jnp.max(s, axis=1, keepdims=True), s_new)
            e = jnp.exp(s - top)
            e_new = jnp.exp(s_new - top)
            inv = 1.0 / (jnp.sum(e, axis=1, keepdims=True) + e_new)
            self.pbuf[g] = (e * inv).astype(BF)
            self.pnew[g] = jnp.broadcast_to((e_new * inv).astype(BF).astype(F32), (16, self.width))

    def mix(self, step, slot):
        w = self.width
        for g in self.groups:
            vb = self.vbuf[slot, 8 * g:8 * g + 8].reshape(8 * w, self.cache_len)
            mixed = lax.dot_general(self.pbuf[g], vb, (((1,), (1,)), ((), ())), preferred_element_type=F32)
            o2 = jnp.zeros((16, w), F32)
            for n in range(8):
                o2 = jnp.where(self.row == n, mixed[:, n * w:(n + 1) * w], o2)
            v8 = self.v[pl.ds(self.base(step, g), 8), :]
            o2 = o2 + self.pnew[g] * jnp.concatenate([v8, v8], axis=0)
            self.o[pl.ds(self.base(step, g), 8), :] = jnp.where(self.first_head, o2[:8], o2[8:])

    def fetched(self, g, n):
        self.copy(g, n).wait()
        return lax.rem(g, SLOTS)

    def refill(self, g):
        nxt = g - 2 + SLOTS

        @pl.when((g >= 2) & (nxt < self.layers * self.steps))
        def _():
            self.issue(nxt)

    def piece(self, layer, half, n, count):
        first = layer * self.steps
        per = self.steps // HALVES
        lo = half * per
        begin, end = lo + n * per // count, lo + (n + 1) * per // count

        def body(step, carry):
            self.refill(first + step)
            k_slot = self.fetched(first + step, 0)
            v_slot = self.fetched(first + step - 1, 1)
            q2s, scores = self.score(step, k_slot)
            self.mix(step - 1, v_slot)
            self.softmax(step, q2s, scores)
            return carry

        if n == 0:
            self.refill(jnp.int32(first + begin))
            self.softmax(begin, *self.score(begin, self.fetched(jnp.int32(first + begin), 0)))
            begin += 1
        lax.fori_loop(begin, end, body, 0)
        if n == count - 1:
            self.mix(end - 1, self.fetched(jnp.int32(first + end - 1), 1))


class Message:
    def __init__(self, copy, arrives):
        self.copy, self.arrives = copy, arrives

    def wait_recv(self):
        self.copy.wait_recv()


class Net:
    def __init__(self, send, recv, local):
        self.i = lax.axis_index("x")
        self.j = lax.axis_index("yz")
        self.chip = self.i // 2
        self.core = lax.rem(self.i, 2)
        self.sib = {"x": 2 * self.chip + 1 - self.core}
        self.across = {"x": lax.rem(self.i + 2, 4)}
        self.yother = {"yz": 1 - self.j}
        self.send, self.recv, self.local = send, recv, local
        self.n = 0
        self.m = 0
        self.sent = []
        self.now = 0.0
        self.free = {"x": 0.0, "y": 0.0, "d": 0.0}

    def greet(self):
        self.barrier = pltpu.get_barrier_semaphore()
        for dx in range(4):
            for dy in range(2):
                if dx or dy:
                    pl.semaphore_signal(self.barrier, inc=1, device_id=self.peer(dx, dy), device_id_type=MESH)

    def met(self):
        pl.semaphore_wait(self.barrier, 7)

    def peer(self, dx, dy):
        return {"x": lax.rem(self.i + dx, 4), "yz": lax.rem(self.j + dy, 2)}

    def put(self, src, dst, to):
        c = pltpu.make_async_remote_copy(
            src_ref=src, dst_ref=dst, send_sem=self.send.at[self.n], recv_sem=self.recv.at[self.n],
            device_id=to, device_id_type=MESH)
        self.n += 1
        c.start()
        self.sent.append(c)
        size = src.dtype.itemsize
        for d in src.shape:
            size *= d
        if to is self.sib:
            link, rate, latency = "d", 600e3, 1.0
        elif to is self.yother:
            link, rate, latency = "y", 46e3, 1.8
        else:
            link, rate, latency = "x", 46e3, 1.8
        begin = max(self.now, self.free[link])
        self.free[link] = begin + size / rate
        return Message(c, self.free[link] + latency)

    def fetch(self, src, dst):
        c = pltpu.make_async_copy(src, dst, self.local.at[self.m])
        self.m += 1
        c.start()
        return c

    def finish(self):
        for c in self.sent:
            c.wait_send()


def interleave(net, chains, fill):
    state = []
    for c in chains:
        state.append([net.now, 0.0, [], c, None])
    turn = 0
    while state:
        best = min((e for e in state if e[4] in (None, turn)), key=lambda e: (max(net.now, e[0]), e[0]))
        turn += best[4] is not None
        begin = max(net.now, best[0])
        fill(begin + best[1])
        for m in best[2]:
            m.wait_recv()
        net.now = begin + best[1]
        try:
            best[2], best[1], *tail = next(best[3])
            best[4] = tail[0] if tail else None
            best[0] = max([net.now] + [m.arrives for m in best[2]])
        except StopIteration:
            state.remove(best)


def slot_of(d):
    return 2 * (d % 2) + d // 2


def rs_first(net, part, got):
    return net.put(part.at[pl.ds(2 * (1 - net.core), 2)], got, net.sib)


def rs_second(net, part, got, out, back):
    far = 1 - net.chip
    out[...] = (part[2 * net.core + far].astype(F32) + got[far].astype(F32)).astype(BF)
    return net.put(out, back, net.across)


def rs_last(net, part, got, back):
    return part[2 * net.core + net.chip].astype(F32) + got[net.chip].astype(F32) + back[...].astype(F32)


def gather_x(net, buf):
    me = buf.at[net.i]
    across = net.put(me, me, net.across)
    sib = net.put(me, me, net.sib)
    return sib, across


def gather_forward(net, buf):
    far = buf.at[lax.rem(net.i + 2, 4)]
    return net.put(far, far, net.sib)


def send_half(net, w, act, part, got):
    r = got.shape[0]
    part[...] = tdot(w[:, pl.ds(pl.multiple_of((1 - net.j) * r, r), r)], act).astype(BF)
    return net.put(part, got, net.yother)


def own_half(net, w, act, r):
    return tdot(w[:, pl.ds(pl.multiple_of(net.j * r, r), r)], act)


def norm_send(net, h_own, hx, ssq, far=False):
    hf = h_own.astype(F32)
    me = 2 * net.i + net.j
    hx[0, net.j] = h_own
    ssq[me] = jnp.sum(hf * hf, axis=0, keepdims=True)
    mine = hx.at[0, net.j]
    stats = []
    for dx in range(4):
        for dy in range(2):
            if dx or dy:
                stats.append(net.put(ssq.at[me], ssq.at[me], net.peer(dx, dy)))
    near = net.put(mine, hx.at[0, net.j], net.yother)
    fars = [net.put(mine, hx.at[1, net.j], to) for to in (net.across, net.peer(2, 1))] if far else []
    return stats, near, fars


def norm_scale(ssq, model_dim):
    total = ssq[0]
    for n in range(1, 8):
        total = total + ssq[n]
    return lax.rsqrt(total / model_dim + NORM_EPS)


def normed(hx, inv, gain):
    rows = hx.shape[0] * hx.shape[1]
    return (hx[...].reshape(rows, hx.shape[2]).astype(F32) * inv * gain).astype(BF)


def columns(gx, n):
    return jnp.concatenate([gx[0].T[:, n:n + 1], gx[1].T[:, n:n + 1]], axis=0)


def kernel(names, model_dim, h_ref, lens_ref, kc, vc, ga, gm, gf, wq, wk, wv, wo, win, wout, wu, h_out, p_own, p_other, kt_out, vt_out, *rest):
    s = dict(zip(names, rest))
    kv_sems, send, recv, local = rest[len(names):]
    layers = wq.shape[0]
    net = Net(send, recv, local)
    net.greet()
    mats = (("wo", wo), ("win", win), ("wout", wout))
    loads = {("wqkv", 0): [net.fetch(w.at[0], s["wqkv0"].at[n]) for n, w in enumerate((wq, wk, wv))]}
    att = Attention(lens_ref, kc, vc, s["q"], s["k"], s["v"], s["att"], s["kbuf"], s["vbuf"], s["pbuf"], s["pnew"], kv_sems)
    for l in range(layers):
        if l:
            loads["wqkv", l] = [net.fetch(w.at[l], s[f"wqkv{l}"].at[n]) for n, w in enumerate((wq, wk, wv))]
        for name, w in mats:
            loads[name, l] = [net.fetch(w.at[l], s[f"{name}{l}"])]
    att.start()

    v_loc = p_own.shape[0]
    early = []
    far_chip = 1 - net.chip

    def cross():
        core, a = len(early) % 2, len(early) // 2 * PIECE
        src = wu.at[pl.ds(pl.multiple_of((2 * far_chip + core) * v_loc + a, 16), PIECE)]
        early.append(net.put(src, s["wm"].at[core, pl.ds(a, PIECE)], net.across))

    cost = PIECE * 512 / 46e3

    def fill(until):
        while len(early) < 2 * MOVED // PIECE and max(net.free["x"], net.now) + cost <= until + SLACK:
            cross()

    gx, gfar = s["gx"], s["gfar"]
    for n, g in enumerate((ga, gm, gf)):
        gx[net.j, pl.ds(n * layers, g.shape[0])] = g[...].astype(F32)
    rest_rows = gx.shape[1] - 2 * layers - 1
    gx[net.j, pl.ds(2 * layers + 1, rest_rows)] = jnp.zeros((rest_rows, gx.shape[2]), F32)
    h_in = h_ref[...].astype(F32).T.astype(BF)
    net.met()
    g_near = net.put(gx.at[net.j], gx.at[net.j], net.yother)
    g_fars = []
    stores = []
    h_last = [None] * HALVES
    final = []
    hb = s["ssq_a00"].shape[2]
    blk = h_in.shape[0]
    width = s["q"].shape[1]
    waited = {}

    def once(name, l):
        if (name, l) not in waited:
            for c in loads[name, l]:
                c.wait()
            waited[name, l] = s[f"{name}{l}"]
        return waited[name, l]

    def chain(h):
        lanes = slice(h * hb, (h + 1) * hb)
        seqs = pl.ds(h * hb, hb)
        h_own = h_in[:, lanes]
        stats, near, _ = norm_send(net, h_own, s[f"hx_a0{h}"], s[f"ssq_a0{h}"])
        head = [g_near] if h == 0 else []
        if h == 0:
            g_fars.extend([net.put(gx.at[net.j], gfar.at[net.j], to) for to in (net.across, net.peer(2, 1))])
        for l in range(layers):
            sl = {k[:-2]: s[k] for k in s if k.endswith(f"{l}{h}")}
            yield stats + [near] + head, 0.9
            head = []
            inv = norm_scale(sl["ssq_a"], model_dim)
            xn = normed(sl["hx_a"].at[0], inv, columns(gx, l))
            w = once("wqkv", l)
            part, got, back = sl["qkv_part"], sl["qkv_got"], sl["qkv_back"]
            for n in range(3):
                y = tdot(w[n], xn).astype(BF)
                for d in range(4):
                    part[slot_of(d), n * width:(n + 1) * width] = y[d * width:(d + 1) * width]
            first = rs_first(net, part, got)
            yield [first], 0.2
            second = rs_second(net, part, got, sl["qkv_out"], back)
            yield [second], 0.3
            y = rs_last(net, part, got, back).astype(BF)
            for n, dst in enumerate(("kt", "vt")):
                s[dst][l, :, seqs] = y[(n + 1) * width:(n + 2) * width]
            for n, dst in enumerate((kt_out, vt_out)):
                src = s[("kt", "vt")[n]]
                stores.append(net.fetch(src.at[l, :, seqs], dst.at[l, :, seqs]))
            for n, dst in enumerate(("q", "k", "v")):
                s[dst][seqs, :] = y[n * width:(n + 1) * width].astype(F32).T
            for n in range(PARTS):
                yield [], 17.0 / HALVES / PARTS + 0.2, (l * HALVES + h) * PARTS + n
                att.piece(l, h, n, PARTS)
            if l == layers - 1 and h == 0:
                loads["wu", 0] = [net.fetch(wu, s["wu"])]
            o = sl["o"]
            o[net.i] = s["att"][seqs, :].T.astype(BF)
            sib, across = gather_x(net, o)
            yield [across], 0.1
            fwd = gather_forward(net, o)
            yield [sib, fwd], 0.4
            w = once("wo", l)
            act = o[...].reshape(-1, hb)
            summed = send_half(net, w, act, sl["ypart1"], sl["ygot1"])
            mine = own_half(net, w, act, blk)
            yield [summed], 0.3
            h_own = (h_own.astype(F32) + (mine + sl["ygot1"][...].astype(F32))).astype(BF)
            stats, near, _ = norm_send(net, h_own, sl["hx_m"], sl["ssq_m"])
            yield stats + [near], 0.7
            w = once("win", l)
            inv = norm_scale(sl["ssq_m"], model_dim)
            xn = normed(sl["hx_m"].at[0], inv, columns(gx, layers + l))
            r = w.shape[1] // 4
            y = tdot(w[...], xn).astype(BF)
            part, got, back = sl["upart"], sl["ugot"], sl["uback"]
            for d in range(4):
                part[slot_of(d)] = y[d * r:(d + 1) * r]
            first = rs_first(net, part, got)
            yield [first], 0.2
            second = rs_second(net, part, got, sl["uout"], back)
            yield [second], 0.4
            up = rs_last(net, part, got, back).astype(BF)
            u = sl["u"]
            u[net.i] = jax.nn.gelu(up.astype(F32)).astype(BF)
            sib, across = gather_x(net, u)
            yield [across], 0.1
            fwd = gather_forward(net, u)
            yield [sib, fwd], 0.5
            w = once("wout", l)
            act = u[...].reshape(-1, hb)
            summed = send_half(net, w, act, sl["ypart2"], sl["ygot2"])
            mine = own_half(net, w, act, blk)
            yield [summed], 0.3
            h_own = (h_own.astype(F32) + (mine + sl["ygot2"][...].astype(F32))).astype(BF)
            stats, near, fars = norm_send(net, h_own, s[f"hx_a{l + 1}{h}"], s[f"ssq_a{l + 1}{h}"], far=l == layers - 1)
        s["h"][seqs, :] = h_own.astype(F32).T.astype(BF)
        final.append((stats + [near], fars))

    interleave(net, [chain(h) for h in range(HALVES)], fill)
    while len(early) < 2 * MOVED // PIECE:
        cross()
    stores.append(net.fetch(s["h"], h_out))
    waits = [m for f in final for m in f[0]]
    fars = [m for f in final for m in f[1]]
    unembed(net, s, model_dim, layers, waits, fars + g_fars + early, loads["wu", 0][0], p_own, p_other, stores)
    for c in stores:
        c.wait()
    net.finish()


def unembed(net, s, model_dim, layers, waits, late, wu_load, p_own, p_other, stores):
    v_loc = p_own.shape[0]
    moved = MOVED
    left = v_loc - moved
    wu, wm, own = s["wu"], s["wm"], s["own"]
    for c in waits:
        c.wait_recv()

    def acts(side, gains):
        return jnp.concatenate(
            [normed(s[f"hx_a{layers}{h}"].at[side], norm_scale(s[f"ssq_a{layers}{h}"], model_dim), columns(gains, 2 * layers))
             for h in range(HALVES)], axis=1)

    xn = acts(0, s["gx"])
    wu_load.wait()
    far_chip = 1 - net.chip
    send_a, got_a, send_b = s["send_a"], s["got_a"], s["send_b"]

    def rows(chip, core, a, n):
        return wu[pl.ds(pl.multiple_of((2 * chip + core) * v_loc + a, 16), n), :]

    def product(chip, core, a, n):
        return jnp.dot(rows(chip, core, moved + a, n), xn, preferred_element_type=F32)

    spans = [(a, min(512, left - a)) for a in range(0, left, 512)]
    first, arrivals = [], []

    def stage1(a, n):
        for chip in range(2):
            send_a[chip, pl.ds(a, n)] = product(chip, 1 - net.core, a, n).astype(BF)
        first.append(net.put(send_a.at[:, pl.ds(a, n)], got_a.at[:, pl.ds(a, n)], net.sib))

    def stage2(r, a, n):
        y = product(far_chip, net.core, a, n)
        first[r].wait_recv()
        send_b[pl.ds(a, n)] = (y + got_a[far_chip, pl.ds(a, n)].astype(F32)).astype(BF)
        arrivals.append(net.put(send_b.at[pl.ds(a, n)], p_other.at[pl.ds(moved + a, n)], net.across))

    stage1(*spans[0])
    for r in range(len(spans)):
        if r + 1 < len(spans):
            stage1(*spans[r + 1])
        stage2(r, *spans[r])

    def store(a, n):
        stores.append(net.fetch(own.at[pl.ds(a, n)], p_own.at[pl.ds(a, n)]))

    for c in late:
        c.wait_recv()
    xf = acts(1, s["gfar"])
    x2 = jnp.concatenate([xn, xf], axis=0)
    mspans = [(a, min(512, moved - a)) for a in range(0, moved, 512)]
    send_m = s["send_m"]

    def both(core, a, n):
        w2 = jnp.concatenate([rows(net.chip, core, a, n), wm[core, pl.ds(a, n), :]], axis=1)
        return jnp.dot(w2, x2, preferred_element_type=F32)

    for a, n in mspans:
        send_m[pl.ds(a, n)] = both(1 - net.core, a, n).astype(BF)
        arrivals.append(net.put(send_m.at[pl.ds(a, n)], p_other.at[pl.ds(a, n)], net.sib))
    for a, n in mspans:
        own[pl.ds(a, n)] = both(net.core, a, n).astype(BF)
        store(a, n)
    for a, n in spans:
        y = product(net.chip, net.core, a, n) + got_a[net.chip, pl.ds(a, n)].astype(F32)
        own[pl.ds(moved + a, n)] = y.astype(BF)
        store(moved + a, n)
    for c in arrivals:
        c.wait_recv()


def output_kernel(p_own, p_other, h, kt, vt, logits, h_out, kt_out, vt_out, own, other, total, hb, kb, vb, in_sems, out_sems):
    small = [(h, hb, h_out), (kt, kb, kt_out), (vt, vb, vt_out)]
    spans = [pl.ds(a, min(OUT_ROWS, total.shape[0] - a)) for a in range(0, total.shape[0], OUT_ROWS)]
    ins = [[pltpu.make_async_copy(p.at[d], buf.at[d], in_sems.at[2 * n + m]) for m, (p, buf) in enumerate(((p_own, own), (p_other, other)))]
           for n, d in enumerate(spans)]
    ins += [[pltpu.make_async_copy(src, buf, in_sems.at[2 * len(spans) + n])] for n, (src, buf, dst) in enumerate(small)]
    outs = [pltpu.make_async_copy(total.at[d], logits.at[d], out_sems.at[n]) for n, d in enumerate(spans)]
    outs += [pltpu.make_async_copy(buf, dst, out_sems.at[len(spans) + n]) for n, (src, buf, dst) in enumerate(small)]
    for group in ins:
        for c in group:
            c.start()
    for n, d in enumerate(spans):
        for c in ins[n]:
            c.wait()
        total[d] = own[d].astype(F32) + other[d].astype(F32)
        outs[n].start()
    for n in range(len(small)):
        ins[len(spans) + n][0].wait()
        outs[len(spans) + n].start()
    for c in outs:
        c.wait()


def scratch(layers, blk, batch, k_o, f_loc, n_qkv, v_loc, width, heads, dh, cache_len):
    r = f_loc // 4
    moved = MOVED
    left = v_loc - moved
    t = {}
    hb = batch // HALVES
    for l in range(layers):
        t.update({
            f"wqkv{l}": ((3, 2 * blk, n_qkv), BF), f"wo{l}": ((k_o, 2 * blk), BF),
            f"win{l}": ((2 * blk, f_loc), BF), f"wout{l}": ((f_loc, 2 * blk), BF)})
    for h in range(HALVES):
        for l in range(layers + 1):
            t[f"hx_a{l}{h}"] = ((2 if l == layers else 1, 2, blk, hb), BF)
            t[f"ssq_a{l}{h}"] = ((8, 1, hb), F32)
        for l in range(layers):
            e = f"{l}{h}"
            t.update({
                "qkv_part" + e: ((4, 3 * width, hb), BF), "qkv_got" + e: ((2, 3 * width, hb), BF),
                "qkv_out" + e: ((3 * width, hb), BF), "qkv_back" + e: ((3 * width, hb), BF),
                "o" + e: ((4, width, hb), BF),
                "ypart1" + e: ((blk, hb), BF), "ygot1" + e: ((blk, hb), BF),
                "hx_m" + e: ((1, 2, blk, hb), BF), "ssq_m" + e: ((8, 1, hb), F32),
                "upart" + e: ((4, r, hb), BF), "ugot" + e: ((2, r, hb), BF),
                "uout" + e: ((r, hb), BF), "uback" + e: ((r, hb), BF), "u" + e: ((4, r, hb), BF),
                "ypart2" + e: ((blk, hb), BF), "ygot2" + e: ((blk, hb), BF),
            })
    t.update({
        "gx": ((2, 8, blk), F32), "gfar": ((2, 8, blk), F32),
        "q": ((batch, width), F32), "k": ((batch, width), F32), "v": ((batch, width), F32), "att": ((batch, width), F32),
        "kbuf": ((SLOTS, SEQ_STEP, heads, dh, cache_len), BF), "vbuf": ((SLOTS, SEQ_STEP, heads, dh, cache_len), BF),
        "pbuf": ((SEQ_STEP // 8, 16, cache_len), BF), "pnew": ((SEQ_STEP // 8, 16, width), F32),
        "wu": ((4 * v_loc, 2 * blk), BF), "wm": ((2, moved, 2 * blk), BF),
        "send_a": ((2, left, batch), BF), "got_a": ((2, left, batch), BF),
        "send_b": ((left, batch), BF), "send_m": ((moved, batch), BF), "own": ((v_loc, batch), BF),
        "kt": ((layers, width, batch), BF), "vt": ((layers, width, batch), BF), "h": ((batch, blk), BF),
    })
    return t


def sds(shape, dtype):
    return jax.ShapeDtypeStruct(shape, dtype)


def solution(mesh):
    def decode_step(h_loc, seq_lens, k_cache, v_cache, g_attn, w_q, w_k, w_v, w_o, g_mlp, w_in, w_out, g_final, w_unemb):
        batch, blk = h_loc.shape
        layers = w_q.shape[0]
        heads, dh, cache_len = k_cache.shape[2], k_cache.shape[4], k_cache.shape[3]
        v_loc = w_unemb.shape[1] // 4
        width = heads * dh
        kc = jnp.swapaxes(k_cache, 3, 4)
        vc = jnp.swapaxes(v_cache, 3, 4)
        names = scratch(layers, blk, batch, w_o.shape[1], w_in.shape[2], w_q.shape[2], v_loc, width, heads, dh, cache_len)
        h_out, p_own, p_other, kt, vt = pl.pallas_call(
            functools.partial(kernel, tuple(names), 8 * blk),
            name="decode",
            out_shape=[sds((batch, blk), BF), sds((v_loc, batch), BF), sds((v_loc, batch), BF)] + [sds((layers, width, batch), BF)] * 2,
            in_specs=[VM, pl.BlockSpec(memory_space=pltpu.SMEM), ANY, ANY, VM, VM, VM] + [ANY] * 7,
            out_specs=[ANY] * 5,
            scratch_shapes=[pltpu.VMEM(shape, dtype) for shape, dtype in names.values()] + [
                pltpu.SemaphoreType.DMA((SLOTS, 2)),
                pltpu.SemaphoreType.DMA((COPIES,)), pltpu.SemaphoreType.DMA((COPIES,)), pltpu.SemaphoreType.DMA((40,))],
            compiler_params=pltpu.CompilerParams(collective_id=0, has_side_effects=True, vmem_limit_bytes=67043328),
        )(h_loc, seq_lens, kc, vc, g_attn, g_mlp, g_final[None], w_q, w_k, w_v, w_o, w_in, w_out, w_unemb.T)

        parts = -(-v_loc // OUT_ROWS)
        logits_t, h_out, kt, vt = pl.pallas_call(
            output_kernel,
            name="outputs",
            out_shape=[sds((v_loc, batch), F32), sds(h_out.shape, BF), sds(kt.shape, BF), sds(vt.shape, BF)],
            in_specs=[ANY] * 5,
            out_specs=[ANY] * 4,
            scratch_shapes=[pltpu.VMEM((v_loc, batch), BF), pltpu.VMEM((v_loc, batch), BF), pltpu.VMEM((v_loc, batch), F32),
                            pltpu.VMEM(h_out.shape, BF), pltpu.VMEM(kt.shape, BF), pltpu.VMEM(vt.shape, BF),
                            pltpu.SemaphoreType.DMA((2 * parts + 3,)), pltpu.SemaphoreType.DMA((parts + 3,))],
            compiler_params=pltpu.CompilerParams(vmem_limit_bytes=56 * 2**20),
        )(p_own, p_other, h_out, kt, vt)

        def entries(t):
            return jnp.transpose(t.reshape(layers, heads, dh, batch), (0, 3, 1, 2))

        return h_out, logits_t.T, entries(kt), entries(vt)

    emb_spec = P('dp', ('x', 'yz'))
    gain_spec = P(None, ('x', 'yz'))
    cache_spec = P(None, 'dp', ('yz', 'x'), None, None)
    in_rows = P(None, 'x', 'yz')
    out_rows = P(None, 'yz', 'x')
    new_spec = P(None, 'dp', ('yz', 'x'), None)
    in_specs = (emb_spec, P('dp'), cache_spec, cache_spec, gain_spec, in_rows, in_rows, in_rows, out_rows, gain_spec, in_rows, out_rows, P(('x', 'yz')), P('x', 'yz'))
    out_specs = (emb_spec, P('dp', ('yz', 'x')), new_spec, new_spec)
    return jax.shard_map(decode_step, mesh=mesh, in_specs=in_specs, out_specs=out_specs, check_vma=False)
```

```python
import functools

import jax
import jax.numpy as jnp
from jax import lax
from jax.experimental import pallas as pl
from jax.experimental.pallas import tpu as pltpu
from jax.sharding import PartitionSpec as P

NORM_EPS = 1e-6
MESH = pl.DeviceIdType.MESH
BF = jnp.bfloat16
F32 = jnp.float32
ANY = pl.BlockSpec(memory_space=pl.ANY)
VM = pl.BlockSpec(memory_space=pltpu.VMEM)
SEQ_STEP = 16
SLOTS = 5
HALVES = 2
PARTS = 4
MOVED = 3024
PIECE = 48
SLACK = 0.3
COPIES = 320
OUT_ROWS = 512


def tdot(w, act):
    return lax.dot_general(w, act, (((0,), (0,)), ((), ())), preferred_element_type=F32)


class Attention:
    def __init__(self, lens_ref, kc_ref, vc_ref, q_ref, k_ref, v_ref, o_ref, kbuf, vbuf, pbuf, pnew, sems):
        self.lens, self.kc, self.vc = lens_ref, kc_ref, vc_ref
        self.q, self.k, self.v, self.o = q_ref, k_ref, v_ref, o_ref
        self.kbuf, self.vbuf, self.pbuf, self.pnew, self.sems = kbuf, vbuf, pbuf, pnew, sems
        self.layers = kc_ref.shape[0]
        self.batch, self.width = q_ref.shape
        self.dh, self.cache_len = kc_ref.shape[3], kc_ref.shape[4]
        self.steps = self.batch // SEQ_STEP
        self.groups = range(SEQ_STEP // 8)
        self.row = lax.broadcasted_iota(jnp.int32, (16, self.width), 0) % 8
        self.pos = lax.broadcasted_iota(jnp.int32, (16, self.cache_len), 1)
        self.row8 = lax.broadcasted_iota(jnp.int32, (8, self.width), 0)
        self.first_head = lax.broadcasted_iota(jnp.int32, (8, self.width), 1) < self.dh

    def copy(self, g, n):
        slot = lax.rem(g, SLOTS)
        src, buf = ((self.kc, self.kbuf), (self.vc, self.vbuf))[n]
        block = src.at[g // self.steps, pl.ds(lax.rem(g, self.steps) * SEQ_STEP, SEQ_STEP)]
        return pltpu.make_async_copy(block, buf.at[slot], self.sems.at[slot, n])

    def issue(self, g):
        for n in range(2):
            self.copy(g, n).start()

    def start(self):
        for g in range(SLOTS):
            self.issue(jnp.int32(g))

    def base(self, step, g):
        return pl.multiple_of(step * SEQ_STEP + 8 * g, 8)

    def score(self, step, slot):
        q2s, scores = [], []
        for g in self.groups:
            q8 = self.q[pl.ds(self.base(step, g), 8), :]
            q2 = jnp.concatenate([jnp.where(self.first_head, q8, 0.0), jnp.where(self.first_head, 0.0, q8)], axis=0)
            qbd = jnp.concatenate([jnp.where(self.row == n, q2, 0.0) for n in range(8)], axis=1).astype(BF)
            kb = self.kbuf[slot, 8 * g:8 * g + 8].reshape(8 * self.width, self.cache_len)
            scores.append(jnp.dot(qbd, kb, preferred_element_type=F32))
            q2s.append(q2)
        return q2s, scores

    def softmax(self, step, q2s, scores):
        for g in self.groups:
            k8 = self.k[pl.ds(self.base(step, g), 8), :]
            k2 = jnp.concatenate([k8, k8], axis=0)
            s_new = jnp.sum(q2s[g] * k2, axis=1, keepdims=True) * (self.dh ** -0.5)
            lens8 = jnp.zeros((8, self.width), jnp.int32)
            for n in range(8):
                lens8 = jnp.where(self.row8 == n, self.lens[self.base(step, g) + n], lens8)
            lens16 = jnp.concatenate([lens8, lens8], axis=0)
            lens_full = jnp.concatenate([lens16] * (self.cache_len // self.width), axis=1)
            s = jnp.where(self.pos < lens_full, scores[g] * (self.dh ** -0.5), -1e30)
            top = jnp.maximum(jnp.max(s, axis=1, keepdims=True), s_new)
            e = jnp.exp(s - top)
            e_new = jnp.exp(s_new - top)
            inv = 1.0 / (jnp.sum(e, axis=1, keepdims=True) + e_new)
            self.pbuf[g] = (e * inv).astype(BF)
            self.pnew[g] = jnp.broadcast_to((e_new * inv).astype(BF).astype(F32), (16, self.width))

    def mix(self, step, slot):
        w = self.width
        for g in self.groups:
            vb = self.vbuf[slot, 8 * g:8 * g + 8].reshape(8 * w, self.cache_len)
            mixed = lax.dot_general(self.pbuf[g], vb, (((1,), (1,)), ((), ())), preferred_element_type=F32)
            o2 = jnp.zeros((16, w), F32)
            for n in range(8):
                o2 = jnp.where(self.row == n, mixed[:, n * w:(n + 1) * w], o2)
            v8 = self.v[pl.ds(self.base(step, g), 8), :]
            o2 = o2 + self.pnew[g] * jnp.concatenate([v8, v8], axis=0)
            self.o[pl.ds(self.base(step, g), 8), :] = jnp.where(self.first_head, o2[:8], o2[8:])

    def fetched(self, g, n):
        self.copy(g, n).wait()
        return lax.rem(g, SLOTS)

    def refill(self, g):
        nxt = g - 2 + SLOTS

        @pl.when((g >= 2) & (nxt < self.layers * self.steps))
        def _():
            self.issue(nxt)

    def piece(self, layer, half, n, count):
        first = layer * self.steps
        per = self.steps // HALVES
        lo = half * per
        begin, end = lo + n * per // count, lo + (n + 1) * per // count

        def body(step, carry):
            self.refill(first + step)
            k_slot = self.fetched(first + step, 0)
            v_slot = self.fetched(first + step - 1, 1)
            q2s, scores = self.score(step, k_slot)
            self.mix(step - 1, v_slot)
            self.softmax(step, q2s, scores)
            return carry

        if n == 0:
            self.refill(jnp.int32(first + begin))
            self.softmax(begin, *self.score(begin, self.fetched(jnp.int32(first + begin), 0)))
            begin += 1
        lax.fori_loop(begin, end, body, 0)
        if n == count - 1:
            self.mix(end - 1, self.fetched(jnp.int32(first + end - 1), 1))


class Message:
    def __init__(self, copy, arrives):
        self.copy, self.arrives = copy, arrives

    def wait_recv(self):
        self.copy.wait_recv()


class Net:
    def __init__(self, send, recv, local):
        self.i = lax.axis_index("x")
        self.j = lax.axis_index("yz")
        self.chip = self.i // 2
        self.core = lax.rem(self.i, 2)
        self.sib = {"x": 2 * self.chip + 1 - self.core}
        self.across = {"x": lax.rem(self.i + 2, 4)}
        self.yother = {"yz": 1 - self.j}
        self.send, self.recv, self.local = send, recv, local
        self.n = 0
        self.m = 0
        self.sent = []
        self.now = 0.0
        self.free = {"x": 0.0, "y": 0.0, "d": 0.0}

    def greet(self):
        self.barrier = pltpu.get_barrier_semaphore()
        for dx in range(4):
            for dy in range(2):
                if dx or dy:
                    pl.semaphore_signal(self.barrier, inc=1, device_id=self.peer(dx, dy), device_id_type=MESH)

    def met(self):
        pl.semaphore_wait(self.barrier, 7)

    def peer(self, dx, dy):
        return {"x": lax.rem(self.i + dx, 4), "yz": lax.rem(self.j + dy, 2)}

    def put(self, src, dst, to):
        c = pltpu.make_async_remote_copy(
            src_ref=src, dst_ref=dst, send_sem=self.send.at[self.n], recv_sem=self.recv.at[self.n],
            device_id=to, device_id_type=MESH)
        self.n += 1
        c.start()
        self.sent.append(c)
        size = src.dtype.itemsize
        for d in src.shape:
            size *= d
        if to is self.sib:
            link, rate, latency = "d", 600e3, 1.0
        elif to is self.yother:
            link, rate, latency = "y", 46e3, 1.8
        else:
            link, rate, latency = "x", 46e3, 1.8
        begin = max(self.now, self.free[link])
        self.free[link] = begin + size / rate
        return Message(c, self.free[link] + latency)

    def fetch(self, src, dst):
        c = pltpu.make_async_copy(src, dst, self.local.at[self.m])
        self.m += 1
        c.start()
        return c

    def finish(self):
        for c in self.sent:
            c.wait_send()


def interleave(net, chains, fill):
    state = []
    for c in chains:
        state.append([net.now, 0.0, [], c, None])
    turn = 0
    while state:
        best = min((e for e in state if e[4] in (None, turn)), key=lambda e: (max(net.now, e[0]), e[0]))
        turn += best[4] is not None
        begin = max(net.now, best[0])
        fill(begin + best[1])
        for m in best[2]:
            m.wait_recv()
        net.now = begin + best[1]
        try:
            best[2], best[1], *tail = next(best[3])
            best[4] = tail[0] if tail else None
            best[0] = max([net.now] + [m.arrives for m in best[2]])
        except StopIteration:
            state.remove(best)


def slot_of(d):
    return 2 * (d % 2) + d // 2


def rs_first(net, part, got):
    return net.put(part.at[pl.ds(2 * (1 - net.core), 2)], got, net.sib)


def rs_second(net, part, got, out, back):
    far = 1 - net.chip
    out[...] = (part[2 * net.core + far].astype(F32) + got[far].astype(F32)).astype(BF)
    return net.put(out, back, net.across)


def rs_last(net, part, got, back):
    return part[2 * net.core + net.chip].astype(F32) + got[net.chip].astype(F32) + back[...].astype(F32)


def gather_x(net, buf):
    me = buf.at[net.i]
    across = net.put(me, me, net.across)
    sib = net.put(me, me, net.sib)
    return sib, across


def gather_forward(net, buf):
    far = buf.at[lax.rem(net.i + 2, 4)]
    return net.put(far, far, net.sib)


def send_half(net, w, act, part, got):
    r = got.shape[0]
    part[...] = tdot(w[:, pl.ds(pl.multiple_of((1 - net.j) * r, r), r)], act).astype(BF)
    return net.put(part, got, net.yother)


def own_half(net, w, act, r):
    return tdot(w[:, pl.ds(pl.multiple_of(net.j * r, r), r)], act)


def norm_send(net, h_own, hx, ssq, far=False):
    hf = h_own.astype(F32)
    me = 2 * net.i + net.j
    hx[0, net.j] = h_own
    ssq[me] = jnp.sum(hf * hf, axis=0, keepdims=True)
    mine = hx.at[0, net.j]
    stats = []
    for dx in range(4):
        for dy in range(2):
            if dx or dy:
                stats.append(net.put(ssq.at[me], ssq.at[me], net.peer(dx, dy)))
    near = net.put(mine, hx.at[0, net.j], net.yother)
    fars = [net.put(mine, hx.at[1, net.j], to) for to in (net.across, net.peer(2, 1))] if far else []
    return stats, near, fars


def norm_scale(ssq, model_dim):
    total = ssq[0]
    for n in range(1, 8):
        total = total + ssq[n]
    return lax.rsqrt(total / model_dim + NORM_EPS)


def normed(hx, inv, gain):
    rows = hx.shape[0] * hx.shape[1]
    return (hx[...].reshape(rows, hx.shape[2]).astype(F32) * inv * gain).astype(BF)


def columns(gx, n):
    return jnp.concatenate([gx[0].T[:, n:n + 1], gx[1].T[:, n:n + 1]], axis=0)


def kernel(names, model_dim, h_ref, lens_ref, kc, vc, ga, gm, gf, wq, wk, wv, wo, win, wout, wu, h_out, p_own, p_other, kt_out, vt_out, *rest):
    s = dict(zip(names, rest))
    kv_sems, send, recv, local = rest[len(names):]
    layers = wq.shape[0]
    net = Net(send, recv, local)
    net.greet()
    mats = (("wo", wo), ("win", win), ("wout", wout))
    loads = {("wqkv", 0): [net.fetch(w.at[0], s["wqkv0"].at[n]) for n, w in enumerate((wq, wk, wv))]}
    att = Attention(lens_ref, kc, vc, s["q"], s["k"], s["v"], s["att"], s["kbuf"], s["vbuf"], s["pbuf"], s["pnew"], kv_sems)
    for l in range(layers):
        if l:
            loads["wqkv", l] = [net.fetch(w.at[l], s[f"wqkv{l}"].at[n]) for n, w in enumerate((wq, wk, wv))]
        for name, w in mats:
            loads[name, l] = [net.fetch(w.at[l], s[f"{name}{l}"])]
    att.start()

    v_loc = p_own.shape[0]
    early, pending, arrivals = [], [], []
    far_chip = 1 - net.chip

    def cross():
        core, a = len(early) % 2, len(early) // 2 * PIECE
        src = wu.at[pl.ds(pl.multiple_of((2 * far_chip + core) * v_loc + a, 16), PIECE)]
        early.append(net.put(src, s["wm"].at[core, pl.ds(a, PIECE)], net.across))

    cost = PIECE * 512 / 46e3

    def fill(until):
        while max(net.free["x"], net.now) + cost <= until + SLACK:
            if len(early) < 2 * MOVED // PIECE:
                cross()
            elif pending:
                pending.pop(0)()
            else:
                break

    gx, gfar = s["gx"], s["gfar"]
    for n, g in enumerate((ga, gm, gf)):
        gx[net.j, pl.ds(n * layers, g.shape[0])] = g[...].astype(F32)
    rest_rows = gx.shape[1] - 2 * layers - 1
    gx[net.j, pl.ds(2 * layers + 1, rest_rows)] = jnp.zeros((rest_rows, gx.shape[2]), F32)
    h_in = h_ref[...].astype(F32).T.astype(BF)
    net.met()
    g_near = net.put(gx.at[net.j], gx.at[net.j], net.yother)
    g_fars = []
    stores = []
    late, done = [], [False] * HALVES
    hb = s["ssq_a00"].shape[2]
    blk = h_in.shape[0]
    width = s["q"].shape[1]
    waited = {}

    def once(name, l):
        if (name, l) not in waited:
            for c in loads[name, l]:
                c.wait()
            waited[name, l] = s[f"{name}{l}"]
        return waited[name, l]

    def chain(h):
        lanes = slice(h * hb, (h + 1) * hb)
        seqs = pl.ds(h * hb, hb)
        h_own = h_in[:, lanes]
        stats, near, _ = norm_send(net, h_own, s[f"hx_a0{h}"], s[f"ssq_a0{h}"])
        head = [g_near] if h == 0 else []
        if h == 0:
            g_fars.extend([net.put(gx.at[net.j], gfar.at[net.j], to) for to in (net.across, net.peer(2, 1))])
        for l in range(layers):
            sl = {k[:-2]: s[k] for k in s if k.endswith(f"{l}{h}")}
            yield stats + [near] + head, 0.9
            head = []
            inv = norm_scale(sl["ssq_a"], model_dim)
            xn = normed(sl["hx_a"].at[0], inv, columns(gx, l))
            w = once("wqkv", l)
            part, got, back = sl["qkv_part"], sl["qkv_got"], sl["qkv_back"]
            for n in range(3):
                y = tdot(w[n], xn).astype(BF)
                for d in range(4):
                    part[slot_of(d), n * width:(n + 1) * width] = y[d * width:(d + 1) * width]
            first = rs_first(net, part, got)
            yield [first], 0.2
            second = rs_second(net, part, got, sl["qkv_out"], back)
            yield [second], 0.3
            y = rs_last(net, part, got, back).astype(BF)
            for n, dst in enumerate(("kt", "vt")):
                s[dst][l, :, seqs] = y[(n + 1) * width:(n + 2) * width]
            for n, dst in enumerate((kt_out, vt_out)):
                src = s[("kt", "vt")[n]]
                stores.append(net.fetch(src.at[l, :, seqs], dst.at[l, :, seqs]))
            for n, dst in enumerate(("q", "k", "v")):
                s[dst][seqs, :] = y[n * width:(n + 1) * width].astype(F32).T
            for n in range(PARTS):
                yield [], 17.0 / HALVES / PARTS + 0.2, (l * HALVES + h) * PARTS + n
                att.piece(l, h, n, PARTS)
            if l == layers - 1 and h == 0:
                loads["wu", 0] = [net.fetch(wu, s["wu"])]
            o = sl["o"]
            o[net.i] = s["att"][seqs, :].T.astype(BF)
            sib, across = gather_x(net, o)
            yield [across], 0.1
            fwd = gather_forward(net, o)
            yield [sib, fwd], 0.4
            w = once("wo", l)
            act = o[...].reshape(-1, hb)
            summed = send_half(net, w, act, sl["ypart1"], sl["ygot1"])
            mine = own_half(net, w, act, blk)
            yield [summed], 0.3
            h_own = (h_own.astype(F32) + (mine + sl["ygot1"][...].astype(F32))).astype(BF)
            stats, near, _ = norm_send(net, h_own, sl["hx_m"], sl["ssq_m"])
            yield stats + [near], 0.7
            w = once("win", l)
            inv = norm_scale(sl["ssq_m"], model_dim)
            xn = normed(sl["hx_m"].at[0], inv, columns(gx, layers + l))
            r = w.shape[1] // 4
            y = tdot(w[...], xn).astype(BF)
            part, got, back = sl["upart"], sl["ugot"], sl["uback"]
            for d in range(4):
                part[slot_of(d)] = y[d * r:(d + 1) * r]
            first = rs_first(net, part, got)
            yield [first], 0.2
            second = rs_second(net, part, got, sl["uout"], back)
            yield [second], 0.4
            up = rs_last(net, part, got, back).astype(BF)
            u = sl["u"]
            u[net.i] = jax.nn.gelu(up.astype(F32)).astype(BF)
            sib, across = gather_x(net, u)
            yield [across], 0.1
            fwd = gather_forward(net, u)
            yield [sib, fwd], 0.5
            w = once("wout", l)
            act = u[...].reshape(-1, hb)
            summed = send_half(net, w, act, sl["ypart2"], sl["ygot2"])
            mine = own_half(net, w, act, blk)
            yield [summed], 0.3
            h_own = (h_own.astype(F32) + (mine + sl["ygot2"][...].astype(F32))).astype(BF)
            stats, near, fars = norm_send(net, h_own, s[f"hx_a{l + 1}{h}"], s[f"ssq_a{l + 1}{h}"], far=l == layers - 1)
        s["h"][seqs, :] = h_own.astype(F32).T.astype(BF)
        late.extend(fars)
        yield stats + [near], 0.7
        xn = normed(s[f"hx_a{layers}{h}"].at[0], norm_scale(s[f"ssq_a{layers}{h}"], model_dim), columns(gx, 2 * layers))
        s["xn"][:, seqs] = xn
        if "wu" not in waited:
            loads["wu", 0][0].wait()
            waited["wu"] = True
        left = v_loc - MOVED
        send_a, got_a, send_b = s[f"send_a{h}"], s[f"got_a{h}"], s[f"send_b{h}"]
        spans = [(a, min(512, left - a)) for a in range(0, left, 512)]
        first = []
        for a, n in spans:
            for chip in range(2):
                send_a[chip, pl.ds(a, n)] = product(net, s["wu"], xn, chip, 1 - net.core, v_loc, a, n).astype(BF)
            first.append(net.put(send_a.at[:, pl.ds(a, n)], got_a.at[:, pl.ds(a, n)], net.sib))
        for r, (a, n) in enumerate(spans):
            yield [first[r]], 0.3
            y = product(net, s["wu"], xn, far_chip, net.core, v_loc, a, n)
            send_b[pl.ds(a, n)] = (y + got_a[far_chip, pl.ds(a, n)].astype(F32)).astype(BF)
            for b in range(a, a + n, 128):
                rows = min(128, a + n - b)

                def leave(b=b, rows=rows):
                    arrivals.append(net.put(send_b.at[pl.ds(b, rows)], p_other.at[pl.ds(MOVED + b, rows), seqs], net.across))

                pending.append(leave)
            done[h] = r == len(spans) - 1
            if all(done):
                while pending:
                    pending.pop(0)()

    interleave(net, [chain(h) for h in range(HALVES)], fill)
    while len(early) < 2 * MOVED // PIECE:
        cross()
    stores.append(net.fetch(s["h"], h_out))
    unembed(net, s, model_dim, layers, late + g_fars + early, arrivals, p_own, p_other, stores)
    for c in stores:
        c.wait()
    net.finish()


def wu_rows(net, wu, chip, core, v_loc, a, n):
    return wu[pl.ds(pl.multiple_of((2 * chip + core) * v_loc + a, 16), n), :]


def product(net, wu, xn, chip, core, v_loc, a, n):
    return jnp.dot(wu_rows(net, wu, chip, core, v_loc, MOVED + a, n), xn, preferred_element_type=F32)


def unembed(net, s, model_dim, layers, late, arrivals, p_own, p_other, stores):
    v_loc = p_own.shape[0]
    moved = MOVED
    left = v_loc - moved
    wu, wm, own = s["wu"], s["wm"], s["own"]
    xn = s["xn"][...]

    def store(a, n):
        stores.append(net.fetch(own.at[pl.ds(a, n)], p_own.at[pl.ds(a, n)]))

    for c in late:
        c.wait_recv()
    xf = jnp.concatenate(
        [normed(s[f"hx_a{layers}{h}"].at[1], norm_scale(s[f"ssq_a{layers}{h}"], model_dim), columns(s["gfar"], 2 * layers))
         for h in range(HALVES)], axis=1)
    x2 = jnp.concatenate([xn, xf], axis=0)
    mspans = [(a, min(512, moved - a)) for a in range(0, moved, 512)]
    send_m = s["send_m"]

    def both(core, a, n):
        w2 = jnp.concatenate([wu_rows(net, wu, net.chip, core, v_loc, a, n), wm[core, pl.ds(a, n), :]], axis=1)
        return jnp.dot(w2, x2, preferred_element_type=F32)

    for a, n in mspans:
        send_m[pl.ds(a, n)] = both(1 - net.core, a, n).astype(BF)
        arrivals.append(net.put(send_m.at[pl.ds(a, n)], p_other.at[pl.ds(a, n)], net.sib))
    for a, n in mspans:
        own[pl.ds(a, n)] = both(net.core, a, n).astype(BF)
        store(a, n)
    for a in range(0, left, 512):
        n = min(512, left - a)
        got = jnp.concatenate([s[f"got_a{h}"][net.chip, pl.ds(a, n)] for h in range(HALVES)], axis=1)
        y = product(net, wu, xn, net.chip, net.core, v_loc, a, n) + got.astype(F32)
        own[pl.ds(moved + a, n)] = y.astype(BF)
        store(moved + a, n)
    for c in arrivals:
        c.wait_recv()


def output_kernel(p_own, p_other, h, kt, vt, logits, h_out, kt_out, vt_out, own, other, total, hb, kb, vb, in_sems, out_sems):
    small = [(h, hb, h_out), (kt, kb, kt_out), (vt, vb, vt_out)]
    spans = [pl.ds(a, min(OUT_ROWS, total.shape[0] - a)) for a in range(0, total.shape[0], OUT_ROWS)]
    ins = [[pltpu.make_async_copy(p.at[d], buf.at[d], in_sems.at[2 * n + m]) for m, (p, buf) in enumerate(((p_own, own), (p_other, other)))]
           for n, d in enumerate(spans)]
    ins += [[pltpu.make_async_copy(src, buf, in_sems.at[2 * len(spans) + n])] for n, (src, buf, dst) in enumerate(small)]
    outs = [pltpu.make_async_copy(total.at[d], logits.at[d], out_sems.at[n]) for n, d in enumerate(spans)]
    outs += [pltpu.make_async_copy(buf, dst, out_sems.at[len(spans) + n]) for n, (src, buf, dst) in enumerate(small)]
    for group in ins:
        for c in group:
            c.start()
    for n, d in enumerate(spans):
        for c in ins[n]:
            c.wait()
        total[d] = own[d].astype(F32) + other[d].astype(F32)
        outs[n].start()
    for n in range(len(small)):
        ins[len(spans) + n][0].wait()
        outs[len(spans) + n].start()
    for c in outs:
        c.wait()


def scratch(layers, blk, batch, k_o, f_loc, n_qkv, v_loc, width, heads, dh, cache_len):
    r = f_loc // 4
    moved = MOVED
    left = v_loc - moved
    t = {}
    hb = batch // HALVES
    for l in range(layers):
        t.update({
            f"wqkv{l}": ((3, 2 * blk, n_qkv), BF), f"wo{l}": ((k_o, 2 * blk), BF),
            f"win{l}": ((2 * blk, f_loc), BF), f"wout{l}": ((f_loc, 2 * blk), BF)})
    for h in range(HALVES):
        t.update({f"send_a{h}": ((2, left, hb), BF), f"got_a{h}": ((2, left, hb), BF), f"send_b{h}": ((left, hb), BF)})
        for l in range(layers + 1):
            t[f"hx_a{l}{h}"] = ((2 if l == layers else 1, 2, blk, hb), BF)
            t[f"ssq_a{l}{h}"] = ((8, 1, hb), F32)
        for l in range(layers):
            e = f"{l}{h}"
            t.update({
                "qkv_part" + e: ((4, 3 * width, hb), BF), "qkv_got" + e: ((2, 3 * width, hb), BF),
                "qkv_out" + e: ((3 * width, hb), BF), "qkv_back" + e: ((3 * width, hb), BF),
                "o" + e: ((4, width, hb), BF),
                "ypart1" + e: ((blk, hb), BF), "ygot1" + e: ((blk, hb), BF),
                "hx_m" + e: ((1, 2, blk, hb), BF), "ssq_m" + e: ((8, 1, hb), F32),
                "upart" + e: ((4, r, hb), BF), "ugot" + e: ((2, r, hb), BF),
                "uout" + e: ((r, hb), BF), "uback" + e: ((r, hb), BF), "u" + e: ((4, r, hb), BF),
                "ypart2" + e: ((blk, hb), BF), "ygot2" + e: ((blk, hb), BF),
            })
    t.update({
        "gx": ((2, 8, blk), F32), "gfar": ((2, 8, blk), F32),
        "q": ((batch, width), F32), "k": ((batch, width), F32), "v": ((batch, width), F32), "att": ((batch, width), F32),
        "kbuf": ((SLOTS, SEQ_STEP, heads, dh, cache_len), BF), "vbuf": ((SLOTS, SEQ_STEP, heads, dh, cache_len), BF),
        "pbuf": ((SEQ_STEP // 8, 16, cache_len), BF), "pnew": ((SEQ_STEP // 8, 16, width), F32),
        "wu": ((4 * v_loc, 2 * blk), BF), "wm": ((2, moved, 2 * blk), BF),
        "xn": ((2 * blk, batch), BF), "send_m": ((moved, batch), BF), "own": ((v_loc, batch), BF),
        "kt": ((layers, width, batch), BF), "vt": ((layers, width, batch), BF), "h": ((batch, blk), BF),
    })
    return t


def sds(shape, dtype):
    return jax.ShapeDtypeStruct(shape, dtype)


def solution(mesh):
    def decode_step(h_loc, seq_lens, k_cache, v_cache, g_attn, w_q, w_k, w_v, w_o, g_mlp, w_in, w_out, g_final, w_unemb):
        batch, blk = h_loc.shape
        layers = w_q.shape[0]
        heads, dh, cache_len = k_cache.shape[2], k_cache.shape[4], k_cache.shape[3]
        v_loc = w_unemb.shape[1] // 4
        width = heads * dh
        kc = jnp.swapaxes(k_cache, 3, 4)
        vc = jnp.swapaxes(v_cache, 3, 4)
        names = scratch(layers, blk, batch, w_o.shape[1], w_in.shape[2], w_q.shape[2], v_loc, width, heads, dh, cache_len)
        h_out, p_own, p_other, kt, vt = pl.pallas_call(
            functools.partial(kernel, tuple(names), 8 * blk),
            name="decode",
            out_shape=[sds((batch, blk), BF), sds((v_loc, batch), BF), sds((v_loc, batch), BF)] + [sds((layers, width, batch), BF)] * 2,
            in_specs=[VM, pl.BlockSpec(memory_space=pltpu.SMEM), ANY, ANY, VM, VM, VM] + [ANY] * 7,
            out_specs=[ANY] * 5,
            scratch_shapes=[pltpu.VMEM(shape, dtype) for shape, dtype in names.values()] + [
                pltpu.SemaphoreType.DMA((SLOTS, 2)),
                pltpu.SemaphoreType.DMA((COPIES,)), pltpu.SemaphoreType.DMA((COPIES,)), pltpu.SemaphoreType.DMA((40,))],
            compiler_params=pltpu.CompilerParams(collective_id=0, has_side_effects=True, vmem_limit_bytes=67043328),
        )(h_loc, seq_lens, kc, vc, g_attn, g_mlp, g_final[None], w_q, w_k, w_v, w_o, w_in, w_out, w_unemb.T)

        parts = -(-v_loc // OUT_ROWS)
        logits_t, h_out, kt, vt = pl.pallas_call(
            output_kernel,
            name="outputs",
            out_shape=[sds((v_loc, batch), F32), sds(h_out.shape, BF), sds(kt.shape, BF), sds(vt.shape, BF)],
            in_specs=[ANY] * 5,
            out_specs=[ANY] * 4,
            scratch_shapes=[pltpu.VMEM((v_loc, batch), BF), pltpu.VMEM((v_loc, batch), BF), pltpu.VMEM((v_loc, batch), F32),
                            pltpu.VMEM(h_out.shape, BF), pltpu.VMEM(kt.shape, BF), pltpu.VMEM(vt.shape, BF),
                            pltpu.SemaphoreType.DMA((2 * parts + 3,)), pltpu.SemaphoreType.DMA((parts + 3,))],
            compiler_params=pltpu.CompilerParams(vmem_limit_bytes=56 * 2**20),
        )(p_own, p_other, h_out, kt, vt)

        def entries(t):
            return jnp.transpose(t.reshape(layers, heads, dh, batch), (0, 3, 1, 2))

        return h_out, logits_t.T, entries(kt), entries(vt)

    emb_spec = P('dp', ('x', 'yz'))
    gain_spec = P(None, ('x', 'yz'))
    cache_spec = P(None, 'dp', ('yz', 'x'), None, None)
    in_rows = P(None, 'x', 'yz')
    out_rows = P(None, 'yz', 'x')
    new_spec = P(None, 'dp', ('yz', 'x'), None)
    in_specs = (emb_spec, P('dp'), cache_spec, cache_spec, gain_spec, in_rows, in_rows, in_rows, out_rows, gain_spec, in_rows, out_rows, P(('x', 'yz')), P('x', 'yz'))
    out_specs = (emb_spec, P('dp', ('yz', 'x')), new_spec, new_spec)
    return jax.shard_map(decode_step, mesh=mesh, in_specs=in_specs, out_specs=out_specs, check_vma=False)
```

```python
import functools

import jax
import jax.numpy as jnp
from jax import lax
from jax.experimental import pallas as pl
from jax.experimental.pallas import tpu as pltpu
from jax.sharding import PartitionSpec as P

NORM_EPS = 1e-6
MESH = pl.DeviceIdType.MESH
BF = jnp.bfloat16
F32 = jnp.float32
ANY = pl.BlockSpec(memory_space=pl.ANY)
VM = pl.BlockSpec(memory_space=pltpu.VMEM)
SEQ_STEP = 16
SLOTS = 7
VT = 256
HALVES = 2
PARTS = 4
MOVED = 3024
PIECE = 48
SLACK = 0.6
COPIES = 320
OUT_ROWS = 512


def tdot(w, act):
    return lax.dot_general(w, act, (((0,), (0,)), ((), ())), preferred_element_type=F32)


class Attention:
    def __init__(self, lens_ref, kc_ref, vc_ref, q_ref, k_ref, v_ref, o_ref, kbuf, vbuf, pbuf, pnew, vt, sems):
        self.lens, self.kc, self.vc = lens_ref, kc_ref, vc_ref
        self.q, self.k, self.v, self.o = q_ref, k_ref, v_ref, o_ref
        self.kbuf, self.vbuf, self.pbuf, self.pnew, self.vt, self.sems = kbuf, vbuf, pbuf, pnew, vt, sems
        self.layers = kc_ref.shape[0]
        self.batch, self.width = q_ref.shape
        self.dh, self.cache_len = kc_ref.shape[3], kc_ref.shape[4]
        self.steps = self.batch // SEQ_STEP
        self.groups = range(SEQ_STEP // 8)
        self.row = lax.broadcasted_iota(jnp.int32, (16, self.width), 0) % 8
        self.pos = lax.broadcasted_iota(jnp.int32, (16, self.cache_len), 1)
        self.row8 = lax.broadcasted_iota(jnp.int32, (8, self.width), 0)
        self.first_head = lax.broadcasted_iota(jnp.int32, (8, self.width), 1) < self.dh

    def copy(self, g, n):
        slot = lax.rem(g, SLOTS)
        src, buf = ((self.kc, self.kbuf), (self.vc, self.vbuf))[n]
        block = src.at[g // self.steps, pl.ds(lax.rem(g, self.steps) * SEQ_STEP, SEQ_STEP)]
        return pltpu.make_async_copy(block, buf.at[slot], self.sems.at[slot, n])

    def issue(self, g):
        for n in range(2):
            self.copy(g, n).start()

    def start(self):
        for g in range(SLOTS):
            self.issue(jnp.int32(g))

    def base(self, step, g):
        return pl.multiple_of(step * SEQ_STEP + 8 * g, 8)

    def score(self, step, slot):
        q2s, scores = [], []
        for g in self.groups:
            q8 = self.q[pl.ds(self.base(step, g), 8), :]
            q2 = jnp.concatenate([jnp.where(self.first_head, q8, 0.0), jnp.where(self.first_head, 0.0, q8)], axis=0)
            qbd = jnp.concatenate([jnp.where(self.row == n, q2, 0.0) for n in range(8)], axis=1).astype(BF)
            kb = self.kbuf[slot, 8 * g:8 * g + 8].reshape(8 * self.width, self.cache_len)
            scores.append(jnp.dot(qbd, kb, preferred_element_type=F32))
            q2s.append(q2)
        return q2s, scores

    def softmax(self, step, q2s, scores):
        for g in self.groups:
            k8 = self.k[pl.ds(self.base(step, g), 8), :]
            k2 = jnp.concatenate([k8, k8], axis=0)
            s_new = jnp.sum(q2s[g] * k2, axis=1, keepdims=True) * (self.dh ** -0.5)
            lens8 = jnp.zeros((8, self.width), jnp.int32)
            for n in range(8):
                lens8 = jnp.where(self.row8 == n, self.lens[self.base(step, g) + n], lens8)
            lens16 = jnp.concatenate([lens8, lens8], axis=0)
            lens_full = jnp.concatenate([lens16] * (self.cache_len // self.width), axis=1)
            s = jnp.where(self.pos < lens_full, scores[g] * (self.dh ** -0.5), -1e30)
            top = jnp.maximum(jnp.max(s, axis=1, keepdims=True), s_new)
            e = jnp.exp(s - top)
            e_new = jnp.exp(s_new - top)
            inv = 1.0 / (jnp.sum(e, axis=1, keepdims=True) + e_new)
            self.pbuf[g] = (e * inv).astype(BF)
            self.pnew[g] = jnp.broadcast_to((e_new * inv).astype(BF).astype(F32), (16, self.width))

    def mix(self, step, slot):
        w = self.width
        for g in self.groups:
            vb = self.vbuf[slot, 8 * g:8 * g + 8].reshape(8 * w, self.cache_len)
            parts = []
            for t in range(8 * w // VT):
                self.vt[g, t] = vb[VT * t:VT * (t + 1)].T
                parts.append(jnp.dot(self.pbuf[g], self.vt[g, t], preferred_element_type=F32))
            mixed = jnp.concatenate(parts, axis=1)
            o2 = jnp.zeros((16, w), F32)
            for n in range(8):
                o2 = jnp.where(self.row == n, mixed[:, n * w:(n + 1) * w], o2)
            v8 = self.v[pl.ds(self.base(step, g), 8), :]
            o2 = o2 + self.pnew[g] * jnp.concatenate([v8, v8], axis=0)
            self.o[pl.ds(self.base(step, g), 8), :] = jnp.where(self.first_head, o2[:8], o2[8:])

    def fetched(self, g, n):
        self.copy(g, n).wait()
        return lax.rem(g, SLOTS)

    def refill(self, g):
        nxt = g - 2 + SLOTS

        @pl.when((lax.rem(g, self.steps) >= 2) & (nxt < self.layers * self.steps))
        def _():
            self.issue(nxt)

    def piece(self, layer, half, n, count):
        first = layer * self.steps
        per = self.steps // HALVES
        lo = half * per
        begin, end = lo + n * per // count, lo + (n + 1) * per // count

        def body(step, carry):
            self.refill(first + step)
            k_slot = self.fetched(first + step, 0)
            v_slot = self.fetched(first + step - 1, 1)
            q2s, scores = self.score(step, k_slot)
            self.mix(step - 1, v_slot)
            self.softmax(step, q2s, scores)
            return carry

        if n == 0:
            self.refill(jnp.int32(first + begin))
            self.softmax(begin, *self.score(begin, self.fetched(jnp.int32(first + begin), 0)))
            begin += 1
        lax.fori_loop(begin, end, body, 0)
        if n == count - 1:
            self.mix(end - 1, self.fetched(jnp.int32(first + end - 1), 1))
            if end == self.steps:
                for g in (first + end - 2 + SLOTS, first + end - 1 + SLOTS):
                    if g < self.layers * self.steps:
                        self.issue(jnp.int32(g))


class Message:
    def __init__(self, copy, arrives):
        self.copy, self.arrives = copy, arrives

    def wait_recv(self):
        self.copy.wait_recv()


class Net:
    def __init__(self, send, recv, local):
        self.i = lax.axis_index("x")
        self.j = lax.axis_index("yz")
        self.chip = self.i // 2
        self.core = lax.rem(self.i, 2)
        self.sib = {"x": 2 * self.chip + 1 - self.core}
        self.across = {"x": lax.rem(self.i + 2, 4)}
        self.yother = {"yz": 1 - self.j}
        self.send, self.recv, self.local = send, recv, local
        self.n = 0
        self.m = 0
        self.sent = []
        self.now = 0.0
        self.free = {"x": 0.0, "y": 0.0, "d": 0.0}

    def greet(self):
        self.barrier = pltpu.get_barrier_semaphore()
        for dx in range(4):
            for dy in range(2):
                if dx or dy:
                    pl.semaphore_signal(self.barrier, inc=1, device_id=self.peer(dx, dy), device_id_type=MESH)

    def met(self):
        pl.semaphore_wait(self.barrier, 7)

    def peer(self, dx, dy):
        return {"x": lax.rem(self.i + dx, 4), "yz": lax.rem(self.j + dy, 2)}

    def put(self, src, dst, to):
        c = pltpu.make_async_remote_copy(
            src_ref=src, dst_ref=dst, send_sem=self.send.at[self.n], recv_sem=self.recv.at[self.n],
            device_id=to, device_id_type=MESH)
        self.n += 1
        c.start()
        self.sent.append(c)
        size = src.dtype.itemsize
        for d in src.shape:
            size *= d
        if to is self.sib:
            link, rate, latency = "d", 600e3, 1.0
        elif to is self.yother:
            link, rate, latency = "y", 46e3, 1.8
        else:
            link, rate, latency = "x", 46e3, 1.8
        begin = max(self.now, self.free[link])
        self.free[link] = begin + size / rate
        return Message(c, self.free[link] + latency)

    def fetch(self, src, dst):
        c = pltpu.make_async_copy(src, dst, self.local.at[self.m])
        self.m += 1
        c.start()
        return c

    def finish(self):
        for c in self.sent:
            c.wait_send()


def interleave(net, chains, fill):
    state = []
    for c in chains:
        state.append([net.now, 0.0, [], c, None])
    turn = 0
    while state:
        best = min((e for e in state if e[4] in (None, turn)), key=lambda e: (max(net.now, e[0]), e[0]))
        turn += best[4] is not None
        begin = max(net.now, best[0])
        fill(begin + best[1])
        for m in best[2]:
            m.wait_recv()
        net.now = begin + best[1]
        try:
            best[2], best[1], *tail = next(best[3])
            best[4] = tail[0] if tail else None
            best[0] = max([net.now] + [m.arrives for m in best[2]])
        except StopIteration:
            state.remove(best)


def slot_of(d):
    return 2 * (d % 2) + d // 2


def rs_first(net, part, got):
    return net.put(part.at[pl.ds(2 * (1 - net.core), 2)], got, net.sib)


def rs_second(net, part, got, out, back):
    far = 1 - net.chip
    out[...] = (part[2 * net.core + far].astype(F32) + got[far].astype(F32)).astype(BF)
    return net.put(out, back, net.across)


def rs_last(net, part, got, back):
    return part[2 * net.core + net.chip].astype(F32) + got[net.chip].astype(F32) + back[...].astype(F32)


def gather_x(net, buf):
    me = buf.at[net.i]
    across = net.put(me, me, net.across)
    sib = net.put(me, me, net.sib)
    return sib, across


def gather_forward(net, buf):
    far = buf.at[lax.rem(net.i + 2, 4)]
    return net.put(far, far, net.sib)


def send_half(net, w, act, part, got):
    r = got.shape[0]
    part[...] = tdot(w[:, pl.ds(pl.multiple_of((1 - net.j) * r, r), r)], act).astype(BF)
    return net.put(part, got, net.yother)


def own_half(net, w, act, r):
    return tdot(w[:, pl.ds(pl.multiple_of(net.j * r, r), r)], act)


def norm_send(net, h_own, hx, ssq, far=False):
    hf = h_own.astype(F32)
    me = 2 * net.i + net.j
    hx[0, net.j] = h_own
    ssq[me] = jnp.sum(hf * hf, axis=0, keepdims=True)
    mine = hx.at[0, net.j]
    stats = []
    for dx in range(4):
        for dy in range(2):
            if dx or dy:
                stats.append(net.put(ssq.at[me], ssq.at[me], net.peer(dx, dy)))
    near = net.put(mine, hx.at[0, net.j], net.yother)
    fars = [net.put(mine, hx.at[1, net.j], to) for to in (net.across, net.peer(2, 1))] if far else []
    return stats, near, fars


def norm_scale(ssq, model_dim):
    total = ssq[0]
    for n in range(1, 8):
        total = total + ssq[n]
    return lax.rsqrt(total / model_dim + NORM_EPS)


def normed(hx, inv, gain):
    rows = hx.shape[0] * hx.shape[1]
    return (hx[...].reshape(rows, hx.shape[2]).astype(F32) * inv * gain).astype(BF)


def columns(gx, n):
    return jnp.concatenate([gx[0].T[:, n:n + 1], gx[1].T[:, n:n + 1]], axis=0)


def kernel(names, model_dim, h_ref, lens_ref, kc, vc, ga, gm, gf, wq, wk, wv, wo, win, wout, wu, h_out, p_own, p_other, kt_out, vt_out, *rest):
    s = dict(zip(names, rest))
    kv_sems, send, recv, local = rest[len(names):]
    layers = wq.shape[0]
    net = Net(send, recv, local)
    net.greet()
    mats = (("wo", wo), ("win", win), ("wout", wout))
    loads = {("wqkv", 0): [net.fetch(w.at[0], s["wqkv0"].at[n]) for n, w in enumerate((wq, wk, wv))]}
    att = Attention(lens_ref, kc, vc, s["q"], s["k"], s["v"], s["att"], s["kbuf"], s["vbuf"], s["pbuf"], s["pnew"], s["vturn"], kv_sems)
    for l in range(layers):
        if l:
            loads["wqkv", l] = [net.fetch(w.at[l], s[f"wqkv{l}"].at[n]) for n, w in enumerate((wq, wk, wv))]
        for name, w in mats:
            loads[name, l] = [net.fetch(w.at[l], s[f"{name}{l}"])]
    att.start()

    v_loc = p_own.shape[0]
    early, pending, arrivals = [], [], []
    far_chip = 1 - net.chip

    def cross():
        core, a = len(early) % 2, len(early) // 2 * PIECE
        src = wu.at[pl.ds(pl.multiple_of((2 * far_chip + core) * v_loc + a, 16), PIECE)]
        early.append(net.put(src, s["wm"].at[core, pl.ds(a, PIECE)], net.across))

    cost = PIECE * 512 / 46e3

    def fill(until):
        while max(net.free["x"], net.now) + cost <= until + SLACK:
            if len(early) < 2 * MOVED // PIECE:
                cross()
            elif pending:
                pending.pop(0)()
            else:
                break

    gx, gfar = s["gx"], s["gfar"]
    for n, g in enumerate((ga, gm, gf)):
        gx[net.j, pl.ds(n * layers, g.shape[0])] = g[...].astype(F32)
    rest_rows = gx.shape[1] - 2 * layers - 1
    gx[net.j, pl.ds(2 * layers + 1, rest_rows)] = jnp.zeros((rest_rows, gx.shape[2]), F32)
    h_in = h_ref[...].astype(F32).T.astype(BF)
    net.met()
    g_near = net.put(gx.at[net.j], gx.at[net.j], net.yother)
    g_fars = []
    stores = []
    late, done = [], [False] * HALVES
    hb = s["ssq_a00"].shape[2]
    blk = h_in.shape[0]
    width = s["q"].shape[1]
    waited = {}

    def once(name, l):
        if (name, l) not in waited:
            for c in loads[name, l]:
                c.wait()
            waited[name, l] = s[f"{name}{l}"]
        return waited[name, l]

    def chain(h):
        lanes = slice(h * hb, (h + 1) * hb)
        seqs = pl.ds(h * hb, hb)
        h_own = h_in[:, lanes]
        stats, near, _ = norm_send(net, h_own, s[f"hx_a0{h}"], s[f"ssq_a0{h}"])
        head = [g_near] if h == 0 else []
        if h == 0:
            g_fars.extend([net.put(gx.at[net.j], gfar.at[net.j], to) for to in (net.across, net.peer(2, 1))])
        for l in range(layers):
            sl = {k[:-2]: s[k] for k in s if k.endswith(f"{l}{h}")}
            yield stats + [near] + head, 0.9
            head = []
            inv = norm_scale(sl["ssq_a"], model_dim)
            xn = normed(sl["hx_a"].at[0], inv, columns(gx, l))
            w = once("wqkv", l)
            part, got, back = sl["qkv_part"], sl["qkv_got"], sl["qkv_back"]
            for n in range(3):
                y = tdot(w[n], xn).astype(BF)
                for d in range(4):
                    part[slot_of(d), n * width:(n + 1) * width] = y[d * width:(d + 1) * width]
            first = rs_first(net, part, got)
            yield [first], 0.2
            second = rs_second(net, part, got, sl["qkv_out"], back)
            yield [second], 0.3
            y = rs_last(net, part, got, back).astype(BF)
            for n, dst in enumerate(("kt", "vt")):
                s[dst][l, :, seqs] = y[(n + 1) * width:(n + 2) * width]
            for n, dst in enumerate((kt_out, vt_out)):
                src = s[("kt", "vt")[n]]
                stores.append(net.fetch(src.at[l, :, seqs], dst.at[l, :, seqs]))
            for n, dst in enumerate(("q", "k", "v")):
                s[dst][seqs, :] = y[n * width:(n + 1) * width].astype(F32).T
            for n in range(PARTS):
                yield [], 14.0 / HALVES / PARTS + 0.2, (l * HALVES + h) * PARTS + n
                att.piece(l, h, n, PARTS)
            if l == layers - 1 and h == 0:
                loads["wu", 0] = []
                for c in range(2):
                    mine = pl.ds(pl.multiple_of((2 * net.chip + c) * v_loc, 16), v_loc)
                    other = pl.ds(pl.multiple_of((2 * far_chip + c) * v_loc + MOVED, 16), v_loc - MOVED)
                    loads["wu", 0] += [net.fetch(wu.at[mine], s["wu"].at[c]), net.fetch(wu.at[other], s["wu_far"].at[c])]
            o = sl["o"]
            o[net.i] = s["att"][seqs, :].T.astype(BF)
            sib, across = gather_x(net, o)
            yield [across], 0.1
            fwd = gather_forward(net, o)
            yield [sib, fwd], 0.4
            w = once("wo", l)
            act = o[...].reshape(-1, hb)
            summed = send_half(net, w, act, sl["ypart1"], sl["ygot1"])
            mine = own_half(net, w, act, blk)
            yield [summed], 0.3
            h_own = (h_own.astype(F32) + (mine + sl["ygot1"][...].astype(F32))).astype(BF)
            stats, near, _ = norm_send(net, h_own, sl["hx_m"], sl["ssq_m"])
            yield stats + [near], 0.7
            w = once("win", l)
            inv = norm_scale(sl["ssq_m"], model_dim)
            xn = normed(sl["hx_m"].at[0], inv, columns(gx, layers + l))
            r = w.shape[1] // 4
            y = tdot(w[...], xn).astype(BF)
            part, got, back = sl["upart"], sl["ugot"], sl["uback"]
            for d in range(4):
                part[slot_of(d)] = y[d * r:(d + 1) * r]
            first = rs_first(net, part, got)
            yield [first], 0.2
            second = rs_second(net, part, got, sl["uout"], back)
            yield [second], 0.4
            up = rs_last(net, part, got, back).astype(BF)
            u = sl["u"]
            u[net.i] = jax.nn.gelu(up.astype(F32)).astype(BF)
            sib, across = gather_x(net, u)
            yield [across], 0.1
            fwd = gather_forward(net, u)
            yield [sib, fwd], 0.5
            w = once("wout", l)
            act = u[...].reshape(-1, hb)
            summed = send_half(net, w, act, sl["ypart2"], sl["ygot2"])
            mine = own_half(net, w, act, blk)
            yield [summed], 0.3
            h_own = (h_own.astype(F32) + (mine + sl["ygot2"][...].astype(F32))).astype(BF)
            stats, near, fars = norm_send(net, h_own, s[f"hx_a{l + 1}{h}"], s[f"ssq_a{l + 1}{h}"], far=l == layers - 1)
        s["h"][seqs, :] = h_own.astype(F32).T.astype(BF)
        late.extend(fars)
        yield stats + [near], 0.7
        xn = normed(s[f"hx_a{layers}{h}"].at[0], norm_scale(s[f"ssq_a{layers}{h}"], model_dim), columns(gx, 2 * layers))
        s["xn"][:, seqs] = xn
        if "wu" not in waited:
            for c in loads["wu", 0]:
                c.wait()
            waited["wu"] = True
        left = v_loc - MOVED
        send_a, got_a, send_b = s[f"send_a{h}"], s[f"got_a{h}"], s[f"send_b{h}"]
        spans = [(a, min(512, left - a)) for a in range(0, left, 512)]
        first = []
        for a, n in spans:
            send_a[net.chip, pl.ds(a, n)] = product(s["wu"], xn, 1 - net.core, MOVED + a, n).astype(BF)
            send_a[far_chip, pl.ds(a, n)] = product(s["wu_far"], xn, 1 - net.core, a, n).astype(BF)
            first.append(net.put(send_a.at[:, pl.ds(a, n)], got_a.at[:, pl.ds(a, n)], net.sib))
        for r, (a, n) in enumerate(spans):
            yield [first[r]], 0.3
            y = product(s["wu_far"], xn, net.core, a, n)
            send_b[pl.ds(a, n)] = (y + got_a[far_chip, pl.ds(a, n)].astype(F32)).astype(BF)
            for b in range(a, a + n, 128):
                rows = min(128, a + n - b)

                def leave(b=b, rows=rows):
                    arrivals.append(net.put(send_b.at[pl.ds(b, rows)], p_other.at[pl.ds(MOVED + b, rows), seqs], net.across))

                pending.append(leave)
            done[h] = r == len(spans) - 1
            if all(done):
                while pending:
                    pending.pop(0)()

    interleave(net, [chain(h) for h in range(HALVES)], fill)
    while len(early) < 2 * MOVED // PIECE:
        cross()
    stores.append(net.fetch(s["h"], h_out))
    unembed(net, s, model_dim, layers, late + g_fars + early, arrivals, p_own, p_other, stores)
    for c in stores:
        c.wait()
    net.finish()


def product(w, xn, core, a, n):
    return jnp.dot(w[core, pl.ds(a, n), :], xn, preferred_element_type=F32)


def unembed(net, s, model_dim, layers, late, arrivals, p_own, p_other, stores):
    v_loc = p_own.shape[0]
    moved = MOVED
    left = v_loc - moved
    wu, wm, own = s["wu"], s["wm"], s["own"]
    xn = s["xn"][...]

    def store(a, n):
        stores.append(net.fetch(own.at[pl.ds(a, n)], p_own.at[pl.ds(a, n)]))

    for c in late:
        c.wait_recv()
    xf = jnp.concatenate(
        [normed(s[f"hx_a{layers}{h}"].at[1], norm_scale(s[f"ssq_a{layers}{h}"], model_dim), columns(s["gfar"], 2 * layers))
         for h in range(HALVES)], axis=1)
    x2 = jnp.concatenate([xn, xf], axis=0)
    mspans = [(a, min(512, moved - a)) for a in range(0, moved, 512)]
    send_m = s["send_m"]

    def both(core, a, n):
        w2 = jnp.concatenate([wu[core, pl.ds(a, n), :], wm[core, pl.ds(a, n), :]], axis=1)
        return jnp.dot(w2, x2, preferred_element_type=F32)

    for a, n in mspans:
        send_m[pl.ds(a, n)] = both(1 - net.core, a, n).astype(BF)
        arrivals.append(net.put(send_m.at[pl.ds(a, n)], p_other.at[pl.ds(a, n)], net.sib))
    for a, n in mspans:
        own[pl.ds(a, n)] = both(net.core, a, n).astype(BF)
        store(a, n)
    for a in range(0, left, 512):
        n = min(512, left - a)
        got = jnp.concatenate([s[f"got_a{h}"][net.chip, pl.ds(a, n)] for h in range(HALVES)], axis=1)
        y = product(wu, xn, net.core, moved + a, n) + got.astype(F32)
        own[pl.ds(moved + a, n)] = y.astype(BF)
        store(moved + a, n)
    for c in arrivals:
        c.wait_recv()


def output_kernel(p_own, p_other, h, kt, vt, logits, h_out, kt_out, vt_out, own, other, total, hb, kb, vb, in_sems, out_sems):
    small = [(h, hb, h_out), (kt, kb, kt_out), (vt, vb, vt_out)]
    spans = [pl.ds(a, min(OUT_ROWS, total.shape[0] - a)) for a in range(0, total.shape[0], OUT_ROWS)]
    ins = [[pltpu.make_async_copy(p.at[d], buf.at[d], in_sems.at[2 * n + m]) for m, (p, buf) in enumerate(((p_own, own), (p_other, other)))]
           for n, d in enumerate(spans)]
    ins += [[pltpu.make_async_copy(src, buf, in_sems.at[2 * len(spans) + n])] for n, (src, buf, dst) in enumerate(small)]
    outs = [pltpu.make_async_copy(total.at[d], logits.at[d], out_sems.at[n]) for n, d in enumerate(spans)]
    outs += [pltpu.make_async_copy(buf, dst, out_sems.at[len(spans) + n]) for n, (src, buf, dst) in enumerate(small)]
    for group in ins:
        for c in group:
            c.start()
    for n, d in enumerate(spans):
        for c in ins[n]:
            c.wait()
        total[d] = own[d].astype(F32) + other[d].astype(F32)
        outs[n].start()
    for n in range(len(small)):
        ins[len(spans) + n][0].wait()
        outs[len(spans) + n].start()
    for c in outs:
        c.wait()


def scratch(layers, blk, batch, k_o, f_loc, n_qkv, v_loc, width, heads, dh, cache_len):
    r = f_loc // 4
    moved = MOVED
    left = v_loc - moved
    t = {}
    hb = batch // HALVES
    for l in range(layers):
        t.update({
            f"wqkv{l}": ((3, 2 * blk, n_qkv), BF), f"wo{l}": ((k_o, 2 * blk), BF),
            f"win{l}": ((2 * blk, f_loc), BF), f"wout{l}": ((f_loc, 2 * blk), BF)})
    for h in range(HALVES):
        t.update({f"send_a{h}": ((2, left, hb), BF), f"got_a{h}": ((2, left, hb), BF), f"send_b{h}": ((left, hb), BF)})
        for l in range(layers + 1):
            t[f"hx_a{l}{h}"] = ((2 if l == layers else 1, 2, blk, hb), BF)
            t[f"ssq_a{l}{h}"] = ((8, 1, hb), F32)
        for l in range(layers):
            e = f"{l}{h}"
            t.update({
                "qkv_part" + e: ((4, 3 * width, hb), BF), "qkv_got" + e: ((2, 3 * width, hb), BF),
                "qkv_out" + e: ((3 * width, hb), BF), "qkv_back" + e: ((3 * width, hb), BF),
                "o" + e: ((4, width, hb), BF),
                "ypart1" + e: ((blk, hb), BF), "ygot1" + e: ((blk, hb), BF),
                "hx_m" + e: ((1, 2, blk, hb), BF), "ssq_m" + e: ((8, 1, hb), F32),
                "upart" + e: ((4, r, hb), BF), "ugot" + e: ((2, r, hb), BF),
                "uout" + e: ((r, hb), BF), "uback" + e: ((r, hb), BF), "u" + e: ((4, r, hb), BF),
                "ypart2" + e: ((blk, hb), BF), "ygot2" + e: ((blk, hb), BF),
            })
    t.update({
        "gx": ((2, 8, blk), F32), "gfar": ((2, 8, blk), F32),
        "q": ((batch, width), F32), "k": ((batch, width), F32), "v": ((batch, width), F32), "att": ((batch, width), F32),
        "kbuf": ((SLOTS, SEQ_STEP, heads, dh, cache_len), BF), "vbuf": ((SLOTS, SEQ_STEP, heads, dh, cache_len), BF),
        "vturn": ((SEQ_STEP // 8, 8 * width // VT, cache_len, VT), BF),
        "pbuf": ((SEQ_STEP // 8, 16, cache_len), BF), "pnew": ((SEQ_STEP // 8, 16, width), F32),
        "wu": ((2, v_loc, 2 * blk), BF), "wu_far": ((2, left, 2 * blk), BF), "wm": ((2, moved, 2 * blk), BF),
        "xn": ((2 * blk, batch), BF), "send_m": ((moved, batch), BF), "own": ((v_loc, batch), BF),
        "kt": ((layers, width, batch), BF), "vt": ((layers, width, batch), BF), "h": ((batch, blk), BF),
    })
    return t


def sds(shape, dtype):
    return jax.ShapeDtypeStruct(shape, dtype)


def solution(mesh):
    def decode_step(h_loc, seq_lens, k_cache, v_cache, g_attn, w_q, w_k, w_v, w_o, g_mlp, w_in, w_out, g_final, w_unemb):
        batch, blk = h_loc.shape
        layers = w_q.shape[0]
        heads, dh, cache_len = k_cache.shape[2], k_cache.shape[4], k_cache.shape[3]
        v_loc = w_unemb.shape[1] // 4
        width = heads * dh
        kc = jnp.swapaxes(k_cache, 3, 4)
        vc = jnp.swapaxes(v_cache, 3, 4)
        names = scratch(layers, blk, batch, w_o.shape[1], w_in.shape[2], w_q.shape[2], v_loc, width, heads, dh, cache_len)
        h_out, p_own, p_other, kt, vt = pl.pallas_call(
            functools.partial(kernel, tuple(names), 8 * blk),
            name="decode",
            out_shape=[sds((batch, blk), BF), sds((v_loc, batch), BF), sds((v_loc, batch), BF)] + [sds((layers, width, batch), BF)] * 2,
            in_specs=[VM, pl.BlockSpec(memory_space=pltpu.SMEM), ANY, ANY, VM, VM, VM] + [ANY] * 7,
            out_specs=[ANY] * 5,
            scratch_shapes=[pltpu.VMEM(shape, dtype) for shape, dtype in names.values()] + [
                pltpu.SemaphoreType.DMA((SLOTS, 2)),
                pltpu.SemaphoreType.DMA((COPIES,)), pltpu.SemaphoreType.DMA((COPIES,)), pltpu.SemaphoreType.DMA((40,))],
            compiler_params=pltpu.CompilerParams(collective_id=0, has_side_effects=True, vmem_limit_bytes=67043328),
        )(h_loc, seq_lens, kc, vc, g_attn, g_mlp, g_final[None], w_q, w_k, w_v, w_o, w_in, w_out, w_unemb.T)

        parts = -(-v_loc // OUT_ROWS)
        logits_t, h_out, kt, vt = pl.pallas_call(
            output_kernel,
            name="outputs",
            out_shape=[sds((v_loc, batch), F32), sds(h_out.shape, BF), sds(kt.shape, BF), sds(vt.shape, BF)],
            in_specs=[ANY] * 5,
            out_specs=[ANY] * 4,
            scratch_shapes=[pltpu.VMEM((v_loc, batch), BF), pltpu.VMEM((v_loc, batch), BF), pltpu.VMEM((v_loc, batch), F32),
                            pltpu.VMEM(h_out.shape, BF), pltpu.VMEM(kt.shape, BF), pltpu.VMEM(vt.shape, BF),
                            pltpu.SemaphoreType.DMA((2 * parts + 3,)), pltpu.SemaphoreType.DMA((parts + 3,))],
            compiler_params=pltpu.CompilerParams(vmem_limit_bytes=56 * 2**20),
        )(p_own, p_other, h_out, kt, vt)

        def entries(t):
            return jnp.transpose(t.reshape(layers, heads, dh, batch), (0, 3, 1, 2))

        return h_out, logits_t.T, entries(kt), entries(vt)

    emb_spec = P('dp', ('x', 'yz'))
    gain_spec = P(None, ('x', 'yz'))
    cache_spec = P(None, 'dp', ('yz', 'x'), None, None)
    in_rows = P(None, 'x', 'yz')
    out_rows = P(None, 'yz', 'x')
    new_spec = P(None, 'dp', ('yz', 'x'), None)
    in_specs = (emb_spec, P('dp'), cache_spec, cache_spec, gain_spec, in_rows, in_rows, in_rows, out_rows, gain_spec, in_rows, out_rows, P(('x', 'yz')), P('x', 'yz'))
    out_specs = (emb_spec, P('dp', ('yz', 'x')), new_spec, new_spec)
    return jax.shard_map(decode_step, mesh=mesh, in_specs=in_specs, out_specs=out_specs, check_vma=False)
```

```python
import functools

import jax
import jax.numpy as jnp
from jax import lax
from jax.experimental import pallas as pl
from jax.experimental.pallas import tpu as pltpu
from jax.sharding import PartitionSpec as P

NORM_EPS = 1e-6
MESH = pl.DeviceIdType.MESH
BF = jnp.bfloat16
F32 = jnp.float32
ANY = pl.BlockSpec(memory_space=pl.ANY)
VM = pl.BlockSpec(memory_space=pltpu.VMEM)
SEQ_STEP = 16
SLOTS = 7
VT = 256
HALVES = 2
PARTS = 4
MOVED = 3024
PIECE = 48
SLACK = 0.6
COPIES = 320
OUT_ROWS = 512


def tdot(w, act):
    return lax.dot_general(w, act, (((0,), (0,)), ((), ())), preferred_element_type=F32)


class Attention:
    def __init__(self, lens_ref, kc_ref, vc_ref, q_ref, k_ref, v_ref, o_ref, kbuf, vbuf, pbuf, pnew, vt, sems):
        self.lens, self.kc, self.vc = lens_ref, kc_ref, vc_ref
        self.q, self.k, self.v, self.o = q_ref, k_ref, v_ref, o_ref
        self.kbuf, self.vbuf, self.pbuf, self.pnew, self.vt, self.sems = kbuf, vbuf, pbuf, pnew, vt, sems
        self.layers = kc_ref.shape[0]
        self.batch, self.width = q_ref.shape
        self.dh, self.cache_len = kc_ref.shape[3], kc_ref.shape[4]
        self.steps = self.batch // SEQ_STEP
        self.groups = range(SEQ_STEP // 8)
        self.row = lax.broadcasted_iota(jnp.int32, (16, self.width), 0) % 8
        self.pos = lax.broadcasted_iota(jnp.int32, (16, self.cache_len), 1)
        self.row8 = lax.broadcasted_iota(jnp.int32, (8, self.width), 0)
        self.first_head = lax.broadcasted_iota(jnp.int32, (8, self.width), 1) < self.dh

    def copy(self, g, n):
        slot = lax.rem(g, SLOTS)
        src, buf = ((self.kc, self.kbuf), (self.vc, self.vbuf))[n]
        block = src.at[g // self.steps, pl.ds(lax.rem(g, self.steps) * SEQ_STEP, SEQ_STEP)]
        return pltpu.make_async_copy(block, buf.at[slot], self.sems.at[slot, n])

    def issue(self, g):
        for n in range(2):
            self.copy(g, n).start()

    def start(self):
        for g in range(SLOTS):
            self.issue(jnp.int32(g))

    def base(self, step, g):
        return pl.multiple_of(step * SEQ_STEP + 8 * g, 8)

    def score(self, step, slot):
        q2s, scores = [], []
        for g in self.groups:
            q8 = self.q[pl.ds(self.base(step, g), 8), :]
            q2 = jnp.concatenate([jnp.where(self.first_head, q8, 0.0), jnp.where(self.first_head, 0.0, q8)], axis=0)
            qbd = jnp.concatenate([jnp.where(self.row == n, q2, 0.0) for n in range(8)], axis=1).astype(BF)
            kb = self.kbuf[slot, 8 * g:8 * g + 8].reshape(8 * self.width, self.cache_len)
            scores.append(jnp.dot(qbd, kb, preferred_element_type=F32))
            q2s.append(q2)
        return q2s, scores

    def softmax(self, step, q2s, scores):
        for g in self.groups:
            k8 = self.k[pl.ds(self.base(step, g), 8), :]
            k2 = jnp.concatenate([k8, k8], axis=0)
            s_new = jnp.sum(q2s[g] * k2, axis=1, keepdims=True) * (self.dh ** -0.5)
            lens8 = jnp.zeros((8, self.width), jnp.int32)
            for n in range(8):
                lens8 = jnp.where(self.row8 == n, self.lens[self.base(step, g) + n], lens8)
            lens16 = jnp.concatenate([lens8, lens8], axis=0)
            lens_full = jnp.concatenate([lens16] * (self.cache_len // self.width), axis=1)
            s = jnp.where(self.pos < lens_full, scores[g] * (self.dh ** -0.5), -1e30)
            top = jnp.maximum(jnp.max(s, axis=1, keepdims=True), s_new)
            e = jnp.exp(s - top)
            e_new = jnp.exp(s_new - top)
            inv = 1.0 / (jnp.sum(e, axis=1, keepdims=True) + e_new)
            self.pbuf[g] = (e * inv).astype(BF)
            self.pnew[g] = jnp.broadcast_to((e_new * inv).astype(BF).astype(F32), (16, self.width))

    def mix(self, step, slot):
        w = self.width
        for g in self.groups:
            vb = self.vbuf[slot, 8 * g:8 * g + 8].reshape(8 * w, self.cache_len)
            parts = []
            for t in range(8 * w // VT):
                self.vt[g, t] = vb[VT * t:VT * (t + 1)].T
                parts.append(jnp.dot(self.pbuf[g], self.vt[g, t], preferred_element_type=F32))
            mixed = jnp.concatenate(parts, axis=1)
            o2 = jnp.zeros((16, w), F32)
            for n in range(8):
                o2 = jnp.where(self.row == n, mixed[:, n * w:(n + 1) * w], o2)
            v8 = self.v[pl.ds(self.base(step, g), 8), :]
            o2 = o2 + self.pnew[g] * jnp.concatenate([v8, v8], axis=0)
            self.o[pl.ds(self.base(step, g), 8), :] = jnp.where(self.first_head, o2[:8], o2[8:])

    def fetched(self, g, n):
        self.copy(g, n).wait()
        return lax.rem(g, SLOTS)

    def refill(self, g):
        nxt = g - 2 + SLOTS

        @pl.when((lax.rem(g, self.steps) >= 2) & (nxt < self.layers * self.steps))
        def _():
            self.issue(nxt)

    def piece(self, layer, half, n, count):
        first = layer * self.steps
        per = self.steps // HALVES
        lo = half * per
        begin, end = lo + n * per // count, lo + (n + 1) * per // count

        def body(step, carry):
            self.refill(first + step)
            k_slot = self.fetched(first + step, 0)
            v_slot = self.fetched(first + step - 1, 1)
            q2s, scores = self.score(step, k_slot)
            self.mix(step - 1, v_slot)
            self.softmax(step, q2s, scores)
            return carry

        if n == 0:
            self.refill(jnp.int32(first + begin))
            self.softmax(begin, *self.score(begin, self.fetched(jnp.int32(first + begin), 0)))
            begin += 1
        lax.fori_loop(begin, end, body, 0)
        if n == count - 1:
            self.mix(end - 1, self.fetched(jnp.int32(first + end - 1), 1))
            if end == self.steps:
                for g in (first + end - 2 + SLOTS, first + end - 1 + SLOTS):
                    if g < self.layers * self.steps:
                        self.issue(jnp.int32(g))


class Message:
    def __init__(self, copy, arrives):
        self.copy, self.arrives = copy, arrives

    def wait_recv(self):
        self.copy.wait_recv()


class Net:
    def __init__(self, send, recv, local):
        self.i = lax.axis_index("x")
        self.j = lax.axis_index("yz")
        self.chip = self.i // 2
        self.core = lax.rem(self.i, 2)
        self.sib = {"x": 2 * self.chip + 1 - self.core}
        self.across = {"x": lax.rem(self.i + 2, 4)}
        self.yother = {"yz": 1 - self.j}
        self.send, self.recv, self.local = send, recv, local
        self.n = 0
        self.m = 0
        self.sent = []
        self.now = 0.0
        self.free = {"x": 0.0, "y": 0.0, "d": 0.0}

    def greet(self):
        self.barrier = pltpu.get_barrier_semaphore()
        for dx in range(4):
            for dy in range(2):
                if dx or dy:
                    pl.semaphore_signal(self.barrier, inc=1, device_id=self.peer(dx, dy), device_id_type=MESH)

    def met(self):
        pl.semaphore_wait(self.barrier, 7)

    def peer(self, dx, dy):
        return {"x": lax.rem(self.i + dx, 4), "yz": lax.rem(self.j + dy, 2)}

    def put(self, src, dst, to):
        c = pltpu.make_async_remote_copy(
            src_ref=src, dst_ref=dst, send_sem=self.send.at[self.n], recv_sem=self.recv.at[self.n],
            device_id=to, device_id_type=MESH)
        self.n += 1
        c.start()
        self.sent.append(c)
        size = src.dtype.itemsize
        for d in src.shape:
            size *= d
        if to is self.sib:
            link, rate, latency = "d", 600e3, 1.0
        elif to is self.yother:
            link, rate, latency = "y", 46e3, 1.8
        else:
            link, rate, latency = "x", 46e3, 1.8
        begin = max(self.now, self.free[link])
        self.free[link] = begin + size / rate
        return Message(c, self.free[link] + latency)

    def fetch(self, src, dst):
        c = pltpu.make_async_copy(src, dst, self.local.at[self.m])
        self.m += 1
        c.start()
        return c

    def finish(self):
        for c in self.sent:
            c.wait_send()


def interleave(net, chains, fill):
    state = []
    for c in chains:
        state.append([net.now, 0.0, [], c, None])
    turn = 0
    while state:
        best = min((e for e in state if e[4] in (None, turn)), key=lambda e: (max(net.now, e[0]), e[0]))
        turn += best[4] is not None
        begin = max(net.now, best[0])
        fill(begin + best[1])
        for m in best[2]:
            m.wait_recv()
        net.now = begin + best[1]
        try:
            best[2], best[1], *tail = next(best[3])
            best[4] = tail[0] if tail else None
            best[0] = max([net.now] + [m.arrives for m in best[2]])
        except StopIteration:
            state.remove(best)


def slot_of(d):
    return 2 * (d % 2) + d // 2


def rs_first(net, part, got):
    return net.put(part.at[pl.ds(2 * (1 - net.core), 2)], got, net.sib)


def rs_second(net, part, got, out, back):
    far = 1 - net.chip
    out[...] = (part[2 * net.core + far].astype(F32) + got[far].astype(F32)).astype(BF)
    return net.put(out, back, net.across)


def rs_last(net, part, got, back):
    return part[2 * net.core + net.chip].astype(F32) + got[net.chip].astype(F32) + back[...].astype(F32)


def gather_x(net, buf):
    me = buf.at[net.i]
    across = net.put(me, me, net.across)
    sib = net.put(me, me, net.sib)
    return sib, across


def gather_forward(net, buf):
    far = buf.at[lax.rem(net.i + 2, 4)]
    return net.put(far, far, net.sib)


def send_half(net, w, act, part, got):
    r = got.shape[0]
    part[...] = tdot(w[:, pl.ds(pl.multiple_of((1 - net.j) * r, r), r)], act).astype(BF)
    return net.put(part, got, net.yother)


def own_half(net, w, act, r):
    return tdot(w[:, pl.ds(pl.multiple_of(net.j * r, r), r)], act)


def norm_send(net, h_own, hx, ssq, far=False):
    hf = h_own.astype(F32)
    me = 2 * net.i + net.j
    hx[0, net.j] = h_own
    ssq[me] = jnp.sum(hf * hf, axis=0, keepdims=True)
    mine = hx.at[0, net.j]
    stats = []
    for dx in range(4):
        for dy in range(2):
            if dx or dy:
                stats.append(net.put(ssq.at[me], ssq.at[me], net.peer(dx, dy)))
    near = net.put(mine, hx.at[0, net.j], net.yother)
    fars = [net.put(mine, hx.at[1, net.j], net.across)] if far else []
    return stats, near, fars


def norm_scale(ssq, model_dim):
    total = ssq[0]
    for n in range(1, 8):
        total = total + ssq[n]
    return lax.rsqrt(total / model_dim + NORM_EPS)


def normed(hx, inv, gain):
    rows = hx.shape[0] * hx.shape[1]
    return (hx[...].reshape(rows, hx.shape[2]).astype(F32) * inv * gain).astype(BF)


def columns(gx, n):
    return jnp.concatenate([gx[0].T[:, n:n + 1], gx[1].T[:, n:n + 1]], axis=0)


def kernel(names, model_dim, h_ref, lens_ref, kc, vc, ga, gm, gf, wq, wk, wv, wo, win, wout, wu, h_out, p_own, p_other, kt_out, vt_out, *rest):
    s = dict(zip(names, rest))
    kv_sems, send, recv, local = rest[len(names):]
    layers = wq.shape[0]
    net = Net(send, recv, local)
    net.greet()
    mats = (("wo", wo), ("win", win), ("wout", wout))
    loads = {("wqkv", 0): [net.fetch(w.at[0], s["wqkv0"].at[n]) for n, w in enumerate((wq, wk, wv))]}
    att = Attention(lens_ref, kc, vc, s["q"], s["k"], s["v"], s["att"], s["kbuf"], s["vbuf"], s["pbuf"], s["pnew"], s["vturn"], kv_sems)
    for l in range(layers):
        if l:
            loads["wqkv", l] = [net.fetch(w.at[l], s[f"wqkv{l}"].at[n]) for n, w in enumerate((wq, wk, wv))]
        for name, w in mats:
            loads[name, l] = [net.fetch(w.at[l], s[f"{name}{l}"])]
    att.start()

    v_loc = p_own.shape[0]
    early, pending, arrivals = [], [], []
    far_chip = 1 - net.chip

    def cross():
        core, a = len(early) % 2, len(early) // 2 * PIECE
        src = wu.at[pl.ds(pl.multiple_of((2 * far_chip + core) * v_loc + a, 16), PIECE)]
        early.append(net.put(src, s["wm"].at[core, pl.ds(a, PIECE)], net.across))

    cost = PIECE * 512 / 46e3

    def fill(until):
        while max(net.free["x"], net.now) + cost <= until + SLACK:
            if len(early) < 2 * MOVED // PIECE:
                cross()
            elif pending:
                pending.pop(0)()
            else:
                break

    gx, gfar = s["gx"], s["gfar"]
    for n, g in enumerate((ga, gm, gf)):
        gx[net.j, pl.ds(n * layers, g.shape[0])] = g[...].astype(F32)
    rest_rows = gx.shape[1] - 2 * layers - 1
    gx[net.j, pl.ds(2 * layers + 1, rest_rows)] = jnp.zeros((rest_rows, gx.shape[2]), F32)
    h_in = h_ref[...].astype(F32).T.astype(BF)
    net.met()
    g_near = net.put(gx.at[net.j], gx.at[net.j], net.yother)
    g_fars = []
    stores = []
    late, done = [], [False] * HALVES
    hb = s["ssq_a00"].shape[2]
    blk = h_in.shape[0]
    width = s["q"].shape[1]
    waited = {}

    def once(name, l):
        if (name, l) not in waited:
            for c in loads[name, l]:
                c.wait()
            waited[name, l] = s[f"{name}{l}"]
        return waited[name, l]

    def chain(h):
        lanes = slice(h * hb, (h + 1) * hb)
        seqs = pl.ds(h * hb, hb)
        h_own = h_in[:, lanes]
        stats, near, _ = norm_send(net, h_own, s[f"hx_a0{h}"], s[f"ssq_a0{h}"])
        head = [g_near] if h == 0 else []
        if h == 0:
            g_fars.extend([net.put(gx.at[net.j], gfar.at[net.j], to) for to in (net.across, net.peer(2, 1))])
        for l in range(layers):
            sl = {k[:-2]: s[k] for k in s if k.endswith(f"{l}{h}")}
            yield stats + [near] + head, 0.9
            head = []
            inv = norm_scale(sl["ssq_a"], model_dim)
            xn = normed(sl["hx_a"].at[0], inv, columns(gx, l))
            w = once("wqkv", l)
            part, got, back = sl["qkv_part"], sl["qkv_got"], sl["qkv_back"]
            for n in range(3):
                y = tdot(w[n], xn).astype(BF)
                for d in range(4):
                    part[slot_of(d), n * width:(n + 1) * width] = y[d * width:(d + 1) * width]
            first = rs_first(net, part, got)
            yield [first], 0.2
            second = rs_second(net, part, got, sl["qkv_out"], back)
            yield [second], 0.3
            y = rs_last(net, part, got, back).astype(BF)
            for n, dst in enumerate(("kt", "vt")):
                s[dst][l, :, seqs] = y[(n + 1) * width:(n + 2) * width]
            for n, dst in enumerate((kt_out, vt_out)):
                src = s[("kt", "vt")[n]]
                stores.append(net.fetch(src.at[l, :, seqs], dst.at[l, :, seqs]))
            for n, dst in enumerate(("q", "k", "v")):
                s[dst][seqs, :] = y[n * width:(n + 1) * width].astype(F32).T
            for n in range(PARTS):
                yield [], 14.0 / HALVES / PARTS + 0.2, (l * HALVES + h) * PARTS + n
                att.piece(l, h, n, PARTS)
            if l == layers - 1 and h == 0:
                loads["wu", 0] = []
                for c in range(2):
                    mine = pl.ds(pl.multiple_of((2 * net.chip + c) * v_loc, 16), v_loc)
                    other = pl.ds(pl.multiple_of((2 * far_chip + c) * v_loc + MOVED, 16), v_loc - MOVED)
                    loads["wu", 0] += [net.fetch(wu.at[mine], s["wu"].at[c]), net.fetch(wu.at[other], s["wu_far"].at[c])]
            o = sl["o"]
            o[net.i] = s["att"][seqs, :].T.astype(BF)
            sib, across = gather_x(net, o)
            yield [across], 0.1
            fwd = gather_forward(net, o)
            yield [sib, fwd], 0.4
            w = once("wo", l)
            act = o[...].reshape(-1, hb)
            summed = send_half(net, w, act, sl["ypart1"], sl["ygot1"])
            mine = own_half(net, w, act, blk)
            yield [summed], 0.3
            h_own = (h_own.astype(F32) + (mine + sl["ygot1"][...].astype(F32))).astype(BF)
            stats, near, _ = norm_send(net, h_own, sl["hx_m"], sl["ssq_m"])
            yield stats + [near], 0.7
            w = once("win", l)
            inv = norm_scale(sl["ssq_m"], model_dim)
            xn = normed(sl["hx_m"].at[0], inv, columns(gx, layers + l))
            r = w.shape[1] // 4
            y = tdot(w[...], xn).astype(BF)
            part, got, back = sl["upart"], sl["ugot"], sl["uback"]
            for d in range(4):
                part[slot_of(d)] = y[d * r:(d + 1) * r]
            first = rs_first(net, part, got)
            yield [first], 0.2
            second = rs_second(net, part, got, sl["uout"], back)
            yield [second], 0.4
            up = rs_last(net, part, got, back).astype(BF)
            u = sl["u"]
            u[net.i] = jax.nn.gelu(up.astype(F32)).astype(BF)
            sib, across = gather_x(net, u)
            yield [across], 0.1
            fwd = gather_forward(net, u)
            yield [sib, fwd], 0.5
            w = once("wout", l)
            act = u[...].reshape(-1, hb)
            summed = send_half(net, w, act, sl["ypart2"], sl["ygot2"])
            mine = own_half(net, w, act, blk)
            yield [summed], 0.3
            h_own = (h_own.astype(F32) + (mine + sl["ygot2"][...].astype(F32))).astype(BF)
            stats, near, fars = norm_send(net, h_own, s[f"hx_a{l + 1}{h}"], s[f"ssq_a{l + 1}{h}"], far=l == layers - 1)
        s["h"][seqs, :] = h_own.astype(F32).T.astype(BF)
        yield stats + [near], 0.7
        xn = normed(s[f"hx_a{layers}{h}"].at[0], norm_scale(s[f"ssq_a{layers}{h}"], model_dim), columns(gx, 2 * layers))
        s["xn"][:, seqs] = xn
        if "wu" not in waited:
            for c in loads["wu", 0]:
                c.wait()
            waited["wu"] = True
        left = v_loc - MOVED
        send_a, got_a, send_b = s[f"send_a{h}"], s[f"got_a{h}"], s[f"send_b{h}"]
        spans = [(a, min(512, left - a)) for a in range(0, left, 512)]
        first = []
        for a, n in spans:
            send_a[net.chip, pl.ds(a, n)] = product(s["wu"], xn, 1 - net.core, MOVED + a, n).astype(BF)
            send_a[far_chip, pl.ds(a, n)] = product(s["wu_far"], xn, 1 - net.core, a, n).astype(BF)
            first.append(net.put(send_a.at[:, pl.ds(a, n)], got_a.at[:, pl.ds(a, n)], net.sib))
        fars[0].wait_recv()
        block = s[f"hx_a{layers}{h}"].at[1, net.j]
        late.append(net.put(block, block, net.yother))
        for r, (a, n) in enumerate(spans):
            yield [first[r]], 0.3
            y = product(s["wu_far"], xn, net.core, a, n)
            send_b[pl.ds(a, n)] = (y + got_a[far_chip, pl.ds(a, n)].astype(F32)).astype(BF)
            for b in range(a, a + n, 128):
                rows = min(128, a + n - b)

                def leave(b=b, rows=rows):
                    arrivals.append(net.put(send_b.at[pl.ds(b, rows)], p_other.at[pl.ds(MOVED + b, rows), seqs], net.across))

                pending.append(leave)
            done[h] = r == len(spans) - 1
            if all(done):
                while pending:
                    pending.pop(0)()

    interleave(net, [chain(h) for h in range(HALVES)], fill)
    while len(early) < 2 * MOVED // PIECE:
        cross()
    stores.append(net.fetch(s["h"], h_out))
    unembed(net, s, model_dim, layers, late + g_fars + early, arrivals, p_own, p_other, stores)
    for c in stores:
        c.wait()
    net.finish()


def product(w, xn, core, a, n):
    return jnp.dot(w[core, pl.ds(a, n), :], xn, preferred_element_type=F32)


def unembed(net, s, model_dim, layers, late, arrivals, p_own, p_other, stores):
    v_loc = p_own.shape[0]
    moved = MOVED
    left = v_loc - moved
    wu, wm, own = s["wu"], s["wm"], s["own"]
    xn = s["xn"][...]

    def store(a, n):
        stores.append(net.fetch(own.at[pl.ds(a, n)], p_own.at[pl.ds(a, n)]))

    for c in late:
        c.wait_recv()
    xf = jnp.concatenate(
        [normed(s[f"hx_a{layers}{h}"].at[1], norm_scale(s[f"ssq_a{layers}{h}"], model_dim), columns(s["gfar"], 2 * layers))
         for h in range(HALVES)], axis=1)
    x2 = jnp.concatenate([xn, xf], axis=0)
    mspans = [(a, min(512, moved - a)) for a in range(0, moved, 512)]
    send_m = s["send_m"]

    def both(core, a, n):
        w2 = jnp.concatenate([wu[core, pl.ds(a, n), :], wm[core, pl.ds(a, n), :]], axis=1)
        return jnp.dot(w2, x2, preferred_element_type=F32)

    for a, n in mspans:
        send_m[pl.ds(a, n)] = both(1 - net.core, a, n).astype(BF)
        arrivals.append(net.put(send_m.at[pl.ds(a, n)], p_other.at[pl.ds(a, n)], net.sib))
    for a, n in mspans:
        own[pl.ds(a, n)] = both(net.core, a, n).astype(BF)
        store(a, n)
    for a in range(0, left, 512):
        n = min(512, left - a)
        got = jnp.concatenate([s[f"got_a{h}"][net.chip, pl.ds(a, n)] for h in range(HALVES)], axis=1)
        y = product(wu, xn, net.core, moved + a, n) + got.astype(F32)
        own[pl.ds(moved + a, n)] = y.astype(BF)
        store(moved + a, n)
    for c in arrivals:
        c.wait_recv()


def output_kernel(p_own, p_other, h, kt, vt, logits, h_out, kt_out, vt_out, own, other, total, hb, kb, vb, in_sems, out_sems):
    small = [(h, hb, h_out), (kt, kb, kt_out), (vt, vb, vt_out)]
    spans = [pl.ds(a, min(OUT_ROWS, total.shape[0] - a)) for a in range(0, total.shape[0], OUT_ROWS)]
    ins = [[pltpu.make_async_copy(p.at[d], buf.at[d], in_sems.at[2 * n + m]) for m, (p, buf) in enumerate(((p_own, own), (p_other, other)))]
           for n, d in enumerate(spans)]
    ins += [[pltpu.make_async_copy(src, buf, in_sems.at[2 * len(spans) + n])] for n, (src, buf, dst) in enumerate(small)]
    outs = [pltpu.make_async_copy(total.at[d], logits.at[d], out_sems.at[n]) for n, d in enumerate(spans)]
    outs += [pltpu.make_async_copy(buf, dst, out_sems.at[len(spans) + n]) for n, (src, buf, dst) in enumerate(small)]
    for group in ins:
        for c in group:
            c.start()
    for n, d in enumerate(spans):
        for c in ins[n]:
            c.wait()
        total[d] = own[d].astype(F32) + other[d].astype(F32)
        outs[n].start()
    for n in range(len(small)):
        ins[len(spans) + n][0].wait()
        outs[len(spans) + n].start()
    for c in outs:
        c.wait()


def scratch(layers, blk, batch, k_o, f_loc, n_qkv, v_loc, width, heads, dh, cache_len):
    r = f_loc // 4
    moved = MOVED
    left = v_loc - moved
    t = {}
    hb = batch // HALVES
    for l in range(layers):
        t.update({
            f"wqkv{l}": ((3, 2 * blk, n_qkv), BF), f"wo{l}": ((k_o, 2 * blk), BF),
            f"win{l}": ((2 * blk, f_loc), BF), f"wout{l}": ((f_loc, 2 * blk), BF)})
    for h in range(HALVES):
        t.update({f"send_a{h}": ((2, left, hb), BF), f"got_a{h}": ((2, left, hb), BF), f"send_b{h}": ((left, hb), BF)})
        for l in range(layers + 1):
            t[f"hx_a{l}{h}"] = ((2 if l == layers else 1, 2, blk, hb), BF)
            t[f"ssq_a{l}{h}"] = ((8, 1, hb), F32)
        for l in range(layers):
            e = f"{l}{h}"
            t.update({
                "qkv_part" + e: ((4, 3 * width, hb), BF), "qkv_got" + e: ((2, 3 * width, hb), BF),
                "qkv_out" + e: ((3 * width, hb), BF), "qkv_back" + e: ((3 * width, hb), BF),
                "o" + e: ((4, width, hb), BF),
                "ypart1" + e: ((blk, hb), BF), "ygot1" + e: ((blk, hb), BF),
                "hx_m" + e: ((1, 2, blk, hb), BF), "ssq_m" + e: ((8, 1, hb), F32),
                "upart" + e: ((4, r, hb), BF), "ugot" + e: ((2, r, hb), BF),
                "uout" + e: ((r, hb), BF), "uback" + e: ((r, hb), BF), "u" + e: ((4, r, hb), BF),
                "ypart2" + e: ((blk, hb), BF), "ygot2" + e: ((blk, hb), BF),
            })
    t.update({
        "gx": ((2, 8, blk), F32), "gfar": ((2, 8, blk), F32),
        "q": ((batch, width), F32), "k": ((batch, width), F32), "v": ((batch, width), F32), "att": ((batch, width), F32),
        "kbuf": ((SLOTS, SEQ_STEP, heads, dh, cache_len), BF), "vbuf": ((SLOTS, SEQ_STEP, heads, dh, cache_len), BF),
        "vturn": ((SEQ_STEP // 8, 8 * width // VT, cache_len, VT), BF),
        "pbuf": ((SEQ_STEP // 8, 16, cache_len), BF), "pnew": ((SEQ_STEP // 8, 16, width), F32),
        "wu": ((2, v_loc, 2 * blk), BF), "wu_far": ((2, left, 2 * blk), BF), "wm": ((2, moved, 2 * blk), BF),
        "xn": ((2 * blk, batch), BF), "send_m": ((moved, batch), BF), "own": ((v_loc, batch), BF),
        "kt": ((layers, width, batch), BF), "vt": ((layers, width, batch), BF), "h": ((batch, blk), BF),
    })
    return t


def sds(shape, dtype):
    return jax.ShapeDtypeStruct(shape, dtype)


def solution(mesh):
    def decode_step(h_loc, seq_lens, k_cache, v_cache, g_attn, w_q, w_k, w_v, w_o, g_mlp, w_in, w_out, g_final, w_unemb):
        batch, blk = h_loc.shape
        layers = w_q.shape[0]
        heads, dh, cache_len = k_cache.shape[2], k_cache.shape[4], k_cache.shape[3]
        v_loc = w_unemb.shape[1] // 4
        width = heads * dh
        kc = jnp.swapaxes(k_cache, 3, 4)
        vc = jnp.swapaxes(v_cache, 3, 4)
        names = scratch(layers, blk, batch, w_o.shape[1], w_in.shape[2], w_q.shape[2], v_loc, width, heads, dh, cache_len)
        h_out, p_own, p_other, kt, vt = pl.pallas_call(
            functools.partial(kernel, tuple(names), 8 * blk),
            name="decode",
            out_shape=[sds((batch, blk), BF), sds((v_loc, batch), BF), sds((v_loc, batch), BF)] + [sds((layers, width, batch), BF)] * 2,
            in_specs=[VM, pl.BlockSpec(memory_space=pltpu.SMEM), ANY, ANY, VM, VM, VM] + [ANY] * 7,
            out_specs=[ANY] * 5,
            scratch_shapes=[pltpu.VMEM(shape, dtype) for shape, dtype in names.values()] + [
                pltpu.SemaphoreType.DMA((SLOTS, 2)),
                pltpu.SemaphoreType.DMA((COPIES,)), pltpu.SemaphoreType.DMA((COPIES,)), pltpu.SemaphoreType.DMA((40,))],
            compiler_params=pltpu.CompilerParams(collective_id=0, has_side_effects=True, vmem_limit_bytes=67043328),
        )(h_loc, seq_lens, kc, vc, g_attn, g_mlp, g_final[None], w_q, w_k, w_v, w_o, w_in, w_out, w_unemb.T)

        parts = -(-v_loc // OUT_ROWS)
        logits_t, h_out, kt, vt = pl.pallas_call(
            output_kernel,
            name="outputs",
            out_shape=[sds((v_loc, batch), F32), sds(h_out.shape, BF), sds(kt.shape, BF), sds(vt.shape, BF)],
            in_specs=[ANY] * 5,
            out_specs=[ANY] * 4,
            scratch_shapes=[pltpu.VMEM((v_loc, batch), BF), pltpu.VMEM((v_loc, batch), BF), pltpu.VMEM((v_loc, batch), F32),
                            pltpu.VMEM(h_out.shape, BF), pltpu.VMEM(kt.shape, BF), pltpu.VMEM(vt.shape, BF),
                            pltpu.SemaphoreType.DMA((2 * parts + 3,)), pltpu.SemaphoreType.DMA((parts + 3,))],
            compiler_params=pltpu.CompilerParams(vmem_limit_bytes=56 * 2**20),
        )(p_own, p_other, h_out, kt, vt)

        def entries(t):
            return jnp.transpose(t.reshape(layers, heads, dh, batch), (0, 3, 1, 2))

        return h_out, logits_t.T, entries(kt), entries(vt)

    emb_spec = P('dp', ('x', 'yz'))
    gain_spec = P(None, ('x', 'yz'))
    cache_spec = P(None, 'dp', ('yz', 'x'), None, None)
    in_rows = P(None, 'x', 'yz')
    out_rows = P(None, 'yz', 'x')
    new_spec = P(None, 'dp', ('yz', 'x'), None)
    in_specs = (emb_spec, P('dp'), cache_spec, cache_spec, gain_spec, in_rows, in_rows, in_rows, out_rows, gain_spec, in_rows, out_rows, P(('x', 'yz')), P('x', 'yz'))
    out_specs = (emb_spec, P('dp', ('yz', 'x')), new_spec, new_spec)
    return jax.shard_map(decode_step, mesh=mesh, in_specs=in_specs, out_specs=out_specs, check_vma=False)
```
